32 devices in a mesh: gx: 4 (over y, x), gy: 4 (over z), gz: 2 (over core).
Axes of the slice: x: 2, y: 2, z: 4, core: 2. Of those that a mesh axis runs over, the one named last changes fastest.
Arguments:
- ref_image: bfloat16 [1024, 64, 256], P('gx', 'gy', 'gz'), may hold values from -6 to 6
- def_image: bfloat16 [1024, 64, 256], P('gx', 'gy', 'gz'), may hold values from -6 to 6
- displacement: float32 [3, 128, 8, 32], P(None, 'gx', 'gy', 'gz'), may hold values from -3 to 3
Outputs:
- new_displacement: float32 [3, 128, 8, 32], P(None, 'gx', 'gy', 'gz')
- fine_residual: bfloat16 [1024, 64, 256], P('gx', 'gy', 'gz')
The draws below stay inside these ranges and needn't reach their ends.
All inputs are finite; a program needn't handle non-finite values.
Results may differ from the reference program's by a relative error of at most 0.0022.
Values may be sent and summed in bfloat16 or wider, within the bound.
A program may use at most 64 MiB of HBM per device.

```python
import jax
import jax.numpy as jnp
from jax import lax

NX = 1024
NY = 64
NZ = 256
MX = 128
MY = 8
MZ = 32


def steps_of(stream_key, dims, pieces, low, high):
    def one(position, parts):
        draws = jax.random.uniform(jax.random.fold_in(jax.random.fold_in(stream_key, 6), position), (parts,), jnp.float32, low / len(pieces), high / len(pieces))
        return jnp.repeat(jnp.exp(draws), dims[position] // parts).reshape((-1,) + (1,) * (len(dims) - position - 1))

    factor_of = one(*pieces[0])
    for cut in pieces[1:]:
        factor_of = factor_of * one(*cut)
    return factor_of


def noise(rng, extent, width, most, pieces=(), kind=jnp.bfloat16):
    values = jax.random.normal(rng, extent, jnp.float32) * width
    if len(pieces) > 0:
        values = steps_of(rng, extent, pieces, -0.22, 0.18) * values
    return jnp.clip(values, min=-most, max=most).astype(kind)


def setup_inputs(seed: int = 0) -> dict:
    key_list = jax.random.split(jax.random.key(seed), 4)
    return {
        "ref_image": noise(key_list[0], (NX, NY, NZ), 1.0, 6.0, ((0, 4), (1, 4), (2, 2))),
        "def_image": noise(key_list[1], (NX, NY, NZ), 1.0, 6.0, ((0, 4), (1, 4), (2, 2))),
        "displacement": noise(key_list[2], (3, MX, MY, MZ), 0.5, 3.0, ((1, 4), (2, 4), (3, 2)), jnp.float32),
    }


stiffness = 64.0

def bin_level(image):
    values = image.astype(jnp.float32)
    sizex, sizey, sizez = values.shape
    return values.reshape(sizex // 8, 8, sizey // 8, 8, sizez // 8, 8).sum((1, 3, 5)) / 32.0

def central(padded):
    slope_x = (padded[2:, 1:-1, 1:-1] - padded[:-2, 1:-1, 1:-1]) / 2.0
    slope_y = (padded[1:-1, 2:, 1:-1] - padded[1:-1, :-2, 1:-1]) / 2.0
    slope_z = (padded[1:-1, 1:-1, 2:] - padded[1:-1, 1:-1, :-2]) / 2.0
    return (slope_x, slope_y, slope_z)

def line_matrix(count):
    return jnp.eye(count, dtype=jnp.float32) * (1.0 + 2.0 * stiffness) - stiffness * (jnp.eye(count, k=1, dtype=jnp.float32) + jnp.eye(count, k=-1, dtype=jnp.float32))

def prolong_table(fine_count, coarse_count):
    index = jnp.arange(fine_count)
    center = index // 8 + 1
    offset = ((index % 8).astype(jnp.float32) + 0.5) / 8.0 - 0.5
    column = jnp.arange(coarse_count + 2)[None, :]
    weight = jnp.where(column == center[:, None], 1.0 - jnp.abs(offset)[:, None], 0.0)
    weight = weight + jnp.where((offset[:, None] >= 0.0) & (column == center[:, None] + 1), offset[:, None], 0.0)
    weight = weight + jnp.where((offset[:, None] < 0.0) & (column == center[:, None] - 1), -offset[:, None], 0.0)
    return weight.astype(jnp.float32)

def reference(ref_image, def_image, displacement):
    coarse_ref = bin_level(ref_image)
    coarse_def = bin_level(def_image)
    slopes = central(jnp.pad(coarse_ref, 1))
    mismatch = coarse_def - coarse_ref - (slopes[0] * displacement[0] + slopes[1] * displacement[1] + slopes[2] * displacement[2])
    rhs = jnp.stack([slope * mismatch for slope in slopes])
    lines = rhs.shape[1]
    factor = jnp.linalg.cholesky(line_matrix(lines))
    flat = jnp.moveaxis(rhs, 1, 0).reshape(lines, -1)
    solved = jax.scipy.linalg.cho_solve((factor, True), flat)
    step = jnp.moveaxis(solved.reshape(lines, 3, rhs.shape[2], rhs.shape[3]), 0, 1)
    new_displacement = displacement + step
    padded = jnp.pad(new_displacement, ((0, 0), (1, 1), (1, 1), (1, 1)))
    table_x = prolong_table(ref_image.shape[0], rhs.shape[1])
    table_y = prolong_table(ref_image.shape[1], rhs.shape[2])
    table_z = prolong_table(ref_image.shape[2], rhs.shape[3])
    grads = central(jnp.pad(ref_image.astype(jnp.float32), 1))
    total = def_image.astype(jnp.float32) - ref_image.astype(jnp.float32)
    for component in range(3):
        field = jnp.einsum('ia,abc->ibc', table_x, padded[component], precision=lax.Precision.HIGHEST)
        field = jnp.einsum('jb,ibc->ijc', table_y, field, precision=lax.Precision.HIGHEST)
        field = jnp.einsum('ijc,kc->ijk', field, table_z, precision=lax.Precision.HIGHEST)
        total = total - grads[component] * field
    return (new_displacement, total.astype(jnp.bfloat16))
```

```python
import functools

import jax
import jax.numpy as jnp
import numpy as np
from jax import lax
from jax.experimental import pallas as pl
from jax.experimental.pallas import tpu as pltpu
from jax.sharding import PartitionSpec as P

stiffness = 64.0
BIN = 8
SLOT = 32
MESH = pl.DeviceIdType.MESH
HIGHEST = lax.Precision.HIGHEST


def inverse_table(devices, cells):
    lines = devices * cells
    theta = np.arccosh((1.0 + 2.0 * stiffness) / (2.0 * stiffness))
    index = np.arange(lines)
    low = np.minimum(index[:, None], index[None, :])
    high = np.maximum(index[:, None], index[None, :])
    a, b, c = (low + 1) * theta, (lines - high) * theta, (lines + 1) * theta
    inverse = (
        np.exp(a + b - c) * (1 - np.exp(-2 * a)) * (1 - np.exp(-2 * b)) / (1 - np.exp(-2 * c))
        / (2.0 * stiffness * np.sinh(theta))
    )
    table = np.zeros((devices, 3, cells + 16, cells + 8 * devices))
    sums = np.zeros((devices, 8, 3 * cells))
    for me in range(devices):
        first, last = me * cells, (me + 1) * cells - 1
        own = index[first : last + 1]
        up = np.exp((own - last) * theta) * (1 - np.exp(-2 * (own + 1) * theta)) / (1 - np.exp(-2 * (last + 1) * theta))
        down = (
            np.exp((first - own) * theta)
            * (1 - np.exp(-2 * (lines - own) * theta))
            / (1 - np.exp(-2 * (lines - first) * theta))
        )
        for k in range(3):
            sums[me, 2 * k, k * cells : (k + 1) * cells] = up
            sums[me, 2 * k + 1, k * cells : (k + 1) * cells] = down
            for row in range(7, cells + 9):
                x = first + row - 8
                if x < 0 or x >= lines:
                    continue
                table[me, k, row, :cells] = inverse[x, first : last + 1]
                for peer in range(devices):
                    if peer < me:
                        table[me, k, row, cells + 8 * peer + 2 * k] = inverse[x, (peer + 1) * cells - 1]
                    if peer > me:
                        table[me, k, row, cells + 8 * peer + 2 * k + 1] = inverse[x, peer * cells]
    return table.astype(np.float32), sums.astype(np.float32)


def lane_tables(cells_z, size_z, slots):
    place = np.zeros((cells_z, 3 * 128), np.float32)
    for variant in range(3):
        for z in range(cells_z):
            lane = z + 2 - (variant - 1) * cells_z
            if 0 <= lane < cells_z + 4:
                place[z, variant * 128 + lane] = 1.0
    binning = np.repeat(place, BIN, axis=0) / 32.0
    prolong = np.zeros((128, slots * size_z), np.float32)
    for slot in range(slots):
        for fine in range(size_z):
            lane, offset = slot * SLOT + fine // BIN + 2, (fine % BIN + 0.5) / BIN - 0.5
            prolong[lane, slot * size_z + fine] = 1.0 - abs(offset)
            prolong[lane + (1 if offset >= 0 else -1), slot * size_z + fine] = abs(offset)
    return place, binning, prolong


def exchange(
    counts,
    ref_hbm, def_hbm, disp_hbm, table_hbm, sums_hbm, place_hbm, bin_hbm, prolong_hbm,
    new_ref, lines, base, grad_x, grad_y, grad_z,
    zhalo, ref_ref, def_ref, disp_ref, table_ref, sums_ref, place_ref, bin_ref, prolong_ref,
    binned, packed, halo, mine, theirs, xhalo, yrows, ysend, yhalo,
    load_sem,
    near_send, near_recv, peer_send, peer_recv, x_send, x_recv, y_send, y_recv, z_send, z_recv,
):
    nx, ny, nz = counts
    sizex, sizey, sizez = def_ref.shape
    cells_x, cells_z = sizex // BIN, sizez // BIN
    me = (lax.axis_index("gx"), lax.axis_index("gy"), lax.axis_index("gz"))

    def inside(offset):
        good = None
        for at, step, count in zip(me, offset, counts):
            if step:
                test = at > 0 if step < 0 else at < count - 1
                good = test if good is None else jnp.logical_and(good, test)
        return good

    def device(offset):
        return {"gx": me[0] + offset[0], "gy": me[1] + offset[1], "gz": me[2] + offset[2]}

    def peer(j):
        return {"gx": lax.rem(me[0] + j, nx), "gy": me[1], "gz": me[2]}

    steps = (-1, 0, 1)
    offsets = [(i, j, k) for i in steps for j in steps for k in steps if (i, j, k) != (0, 0, 0)]

    loads = [
        pltpu.make_async_copy(hbm, held, load_sem.at[i])
        for i, (hbm, held) in enumerate(
            (
                (disp_hbm, disp_ref), (place_hbm, place_ref), (ref_hbm, ref_ref), (def_hbm, def_ref),
                (bin_hbm, bin_ref), (sums_hbm.at[me[0]], sums_ref),
                (table_hbm.at[me[0]], table_ref), (prolong_hbm, prolong_ref),
            )
        )
    ]
    for load in loads:
        load.start()
    halo[...] = jnp.zeros_like(halo)
    theirs[...] = jnp.zeros_like(theirs)
    xhalo[...] = jnp.zeros_like(xhalo)
    yhalo[...] = jnp.zeros_like(yhalo)

    z_steps = (1,) if nz == 2 else (1, nz - 1)

    def z_device(step):
        return {"gx": me[0], "gy": me[1], "gz": lax.rem(me[2] + step, nz)}

    barrier = pltpu.get_barrier_semaphore()
    for j in range(1, nx):
        pl.semaphore_signal(barrier, inc=1, device_id=peer(j), device_id_type=MESH)
    expect = jnp.int32(nx - 1)
    for offset in offsets:
        if offset[1:] == (0, 0):
            continue

        @pl.when(inside(offset))
        def _():
            pl.semaphore_signal(barrier, inc=1, device_id=device(offset), device_id_type=MESH)

    reach = [
        1 + (at > 0).astype(jnp.int32) + (at < count - 1).astype(jnp.int32)
        for at, count in zip(me, counts)
    ]
    expect = expect + reach[0] * (reach[1] * reach[2] - 1)
    if nz > 2:
        ends = jnp.logical_or(me[2] == 0, me[2] == nz - 1)

        @pl.when(ends)
        def _():
            other = {"gx": me[0], "gy": me[1], "gz": nz - 1 - me[2]}
            pl.semaphore_signal(barrier, inc=1, device_id=other, device_id_type=MESH)

        expect = expect + ends.astype(jnp.int32)
    z_copies = [
        pltpu.make_async_remote_copy(
            src_ref=ref_ref, dst_ref=zhalo.at[i], send_sem=z_send.at[i], recv_sem=z_recv.at[i],
            device_id=z_device(step), device_id_type=MESH,
        )
        for i, step in enumerate(z_steps)
    ]

    source_rows = {-1: (0, 8), 0: (0, cells_x), 1: (cells_x - 8, 8)}
    target_rows = {-1: (0, 8), 0: (8, cells_x), 1: (cells_x + 8, 8)}

    def number(offset):
        return (offset[0] + 1) * 9 + (offset[1] + 1) * 3 + offset[2] + 1

    def blocks_of(step, part):
        return pl.ds(0, 1) if part == 0 else {-1: pl.ds(1, 1), 0: pl.ds(1, 2), 1: pl.ds(2, 1)}[step]

    def near_copy(offset, part):
        blocks = blocks_of(offset[1], part)
        back = tuple(-step for step in offset)
        start, rows = source_rows[offset[0]]
        goal = target_rows[back[0]][0]
        return pltpu.make_async_remote_copy(
            src_ref=packed.at[offset[2] + 1, blocks, pl.ds(start, rows), :],
            dst_ref=halo.at[back[1] + 1, back[2] + 1, blocks, pl.ds(goal, rows), :],
            send_sem=near_send.at[number(offset), part],
            recv_sem=near_recv.at[number(back), part],
            device_id=device(offset), device_id_type=MESH,
        )

    def near_arrival(offset, part):
        blocks = blocks_of(-offset[1], part)
        goal, rows = target_rows[offset[0]]
        where = halo.at[offset[1] + 1, offset[2] + 1, blocks, pl.ds(goal, rows), :]
        return pltpu.make_async_remote_copy(
            src_ref=where, dst_ref=where,
            send_sem=near_send.at[number(offset), part],
            recv_sem=near_recv.at[number(offset), part],
            device_id=device(offset), device_id_type=MESH,
        )

    for load in loads[:2]:
        load.wait()

    def pack(lines_of):
        total = None
        for q, line in enumerate(lines_of):
            spread = lax.dot_general(
                line, place_ref[...], (((0,), (0,)), ((), ())),
                precision=HIGHEST, preferred_element_type=jnp.float32,
            )
            spread = [spread[:, 128 * v : 128 * (v + 1)] for v in range(3)]
            if q:
                spread = [pltpu.roll(s, SLOT * q, 1) for s in spread]
            total = spread if total is None else [t + s for t, s in zip(total, spread)]
        return total

    for block in (1, 2):
        spread = pack([disp_ref[k, block - 1] for k in range(3)])
        for v in range(3):
            packed[v, block] = spread[v]
        halo[1, 1, block, pl.ds(8, cells_x), :] = spread[1]
    pl.semaphore_wait(barrier, expect)
    for offset in offsets:

        @pl.when(inside(offset))
        def _():
            near_copy(offset, 1).start()

    def x_copy(step):
        return pltpu.make_async_remote_copy(
            src_ref=ref_ref.at[pl.ds(sizex - 1 if step > 0 else 0, 1)],
            dst_ref=xhalo.at[pl.ds(0 if step > 0 else 1, 1)],
            send_sem=x_send.at[0 if step > 0 else 1], recv_sem=x_recv.at[0 if step > 0 else 1],
            device_id=device((step, 0, 0)), device_id_type=MESH,
        )

    for load in loads[2:4]:
        load.wait()
    for step in (-1, 1):

        @pl.when(inside((step, 0, 0)))
        def _():
            x_copy(step).start()

    for copy in z_copies:
        copy.start()

    def bin_cell(cell, carry):
        rows = pl.multiple_of(cell * 8, 8)
        total = [None, None]
        for i in range(BIN):
            x = cell * BIN + i
            slabs = (ref_ref[x].astype(jnp.float32), def_ref[x].astype(jnp.float32))
            yrows[0, pl.ds(x, 1), :] = slabs[0][:1]
            yrows[1, pl.ds(x, 1), :] = slabs[0][sizey - 1 :]
            total = [s if t is None else t + s for t, s in zip(total, slabs)]
        for image in range(2):
            for y in range(2):
                binned[2 * image + y, pl.ds(rows, 8), :] = total[image][8 * y : 8 * y + 8]
        return carry

    lax.fori_loop(0, cells_x, bin_cell, 0)
    for load in loads[4:]:
        load.wait()
    spread = None
    for q in range(4):
        line = binned[q, pl.ds(0, cells_x, stride=8), :]
        for s in range(1, 8):
            line = line + binned[q, pl.ds(s, cells_x, stride=8), :]
        part = jnp.dot(line, bin_ref[...], precision=HIGHEST, preferred_element_type=jnp.float32)
        part = [part[:, 128 * v : 128 * (v + 1)] for v in range(3)]
        if q:
            part = [pltpu.roll(p, SLOT * q, 1) for p in part]
        spread = part if spread is None else [a + b for a, b in zip(spread, part)]
    for v in range(3):
        packed[v, 0] = spread[v]
    halo[1, 1, 0, pl.ds(8, cells_x), :] = spread[1]
    for offset in offsets:

        @pl.when(inside(offset))
        def _():
            near_copy(offset, 0).start()

    def y_copy(step):
        side = 1 if step > 0 else 0
        return pltpu.make_async_remote_copy(
            src_ref=ysend.at[side], dst_ref=yhalo.at[1 - side],
            send_sem=y_send.at[side], recv_sem=y_recv.at[1 - side],
            device_id=device((0, step, 0)), device_id_type=MESH,
        )

    ysend[...] = yrows[...].astype(jnp.bfloat16)
    for step in (-1, 1):

        @pl.when(inside((0, step, 0)))
        def _():
            y_copy(step).start()

    rows_in = BIN * sizey

    def prepare(cell, carry):
        start = pl.multiple_of(cell * BIN, BIN)
        first = jnp.maximum(start - 1, 0)
        last = jnp.minimum(start + BIN, sizex - 1)
        slabs = [ref_ref[first].astype(jnp.float32)]
        slabs += [ref_ref[start + i].astype(jnp.float32) for i in range(BIN)]
        slabs += [ref_ref[last].astype(jnp.float32)]
        for i in range(BIN):
            base[start + i] = def_ref[start + i].astype(jnp.float32) - slabs[i + 1]
            grad_x[start + i] = slabs[i + 2] - slabs[i]
        return carry

    lax.fori_loop(0, cells_x, prepare, 0)

    for copy in z_copies:
        copy.wait_recv()

    at_z = me[2]
    row = lax.broadcasted_iota(jnp.int32, (sizez, sizez), 0)
    column = lax.broadcasted_iota(jnp.int32, (sizez, sizez), 1)
    inner = jnp.where(row == column + 1, 1.0, 0.0) - jnp.where(row + 1 == column, 1.0, 0.0)
    from_low = jnp.where(
        jnp.logical_and(jnp.logical_and(row == sizez - 1, column == 0), at_z > 0), -1.0, 0.0
    )
    from_high = jnp.where(
        jnp.logical_and(jnp.logical_and(row == 0, column == sizez - 1), at_z < nz - 1), 1.0, 0.0
    )
    outer = [from_low + from_high] if nz == 2 else [from_low, from_high]
    across = jnp.concatenate([inner] + outer, axis=0).astype(jnp.bfloat16)

    def slope_z(cell, carry):
        start = pl.multiple_of(cell * BIN, BIN)
        sideways = [ref_ref[pl.ds(start, BIN)].reshape(rows_in, sizez)]
        sideways += [zhalo[i, pl.ds(start, BIN)].reshape(rows_in, sizez) for i in range(len(z_steps))]
        slope = jnp.dot(jnp.concatenate(sideways, axis=1), across, preferred_element_type=jnp.float32)
        grad_z[pl.ds(start, BIN)] = slope.reshape(BIN, sizey, sizez)
        return carry

    lax.fori_loop(0, cells_x, slope_z, 0)

    for part in (1, 0):
        for offset in offsets:

            @pl.when(inside(offset))
            def _():
                near_arrival(offset, part).wait_recv()

    summed = [[halo[y, 0, b] + halo[y, 1, b] + halo[y, 2, b] for b in range(3)] for y in range(3)]
    rows = cells_x + 16
    lane = lax.broadcasted_iota(jnp.int32, (rows, 128), 1)
    slot = lane // SLOT

    def centred(b, upper):
        one, two = (SLOT, 128 - SLOT) if upper else (128 - SLOT, SLOT)
        ends = jnp.where(slot == 0, pltpu.roll(summed[0][b], one, 1), pltpu.roll(summed[2][b], one, 1))
        return jnp.where(jnp.logical_or(slot == 0, slot == 3), ends, pltpu.roll(summed[1][b], two, 1))

    coarse = centred(0, False)
    deformed = centred(0, True)
    displacement = []
    for k in range(3):
        parts = [
            pltpu.roll(block, SLOT * ((s - k) % 4), 1) if s != k else block
            for s, block in enumerate((summed[0][2], summed[1][1], summed[1][2], summed[2][1]))
        ]
        displacement.append(
            jnp.where(slot < 2, jnp.where(slot == 0, parts[0], parts[1]), jnp.where(slot == 2, parts[2], parts[3]))
        )
    before = jnp.where(slot < 2, summed[0][0], pltpu.roll(summed[1][0], 64, 1))
    after = jnp.where(slot < 2, summed[1][0], pltpu.roll(summed[2][0], 64, 1))
    slopes = [
        (pltpu.roll(coarse, rows - 1, 0) - pltpu.roll(coarse, 1, 0)) * 0.5,
        (after - before) * 0.5,
        (pltpu.roll(coarse, 127, 1) - pltpu.roll(coarse, 1, 1)) * 0.5,
    ]
    mismatch = deformed - coarse - (
        slopes[0] * displacement[0] + slopes[1] * displacement[1] + slopes[2] * displacement[2]
    )
    place = lane - slot * SLOT
    low = jnp.where(me[2] > 0, 1, 2)
    high = jnp.where(me[2] < nz - 1, cells_z + 2, cells_z + 1)
    keep = jnp.logical_and(place >= low, place <= high)
    keep = jnp.logical_and(keep, slot >= jnp.where(me[1] > 0, 0, 1))
    keep = jnp.logical_and(keep, slot <= jnp.where(me[1] < ny - 1, 3, 2))
    rhs = [jnp.where(keep, s * mismatch, 0.0)[8 : 8 + cells_x] for s in slopes]

    mine[...] = jnp.dot(
        sums_ref[...], jnp.concatenate(rhs, axis=0), precision=HIGHEST, preferred_element_type=jnp.float32
    )

    def peer_copy(j):
        return pltpu.make_async_remote_copy(
            src_ref=mine, dst_ref=theirs.at[me[0]],
            send_sem=peer_send.at[j], recv_sem=peer_recv.at[j],
            device_id=peer(j), device_id_type=MESH,
        )

    for j in range(1, nx):
        peer_copy(j).start()

    for step in (-1, 1):

        @pl.when(inside((step, 0, 0)))
        def _():
            x_copy(-step).wait_recv()

        @pl.when(inside((0, step, 0)))
        def _():
            y_copy(-step).wait_recv()

    grad_x[0] = ref_ref[1].astype(jnp.float32) - xhalo[0].astype(jnp.float32)
    grad_x[sizex - 1] = xhalo[1].astype(jnp.float32) - ref_ref[sizex - 2].astype(jnp.float32)
    yrows[...] = yhalo[...].astype(jnp.float32)
    slab_row = lax.broadcasted_iota(jnp.int32, (sizey, sizez), 0)

    def slope_y(cell, carry):
        start = pl.multiple_of(cell * BIN, BIN)
        for i in range(BIN):
            x = start + i
            slab = ref_ref[x].astype(jnp.float32)
            above = jnp.where(slab_row == sizey - 1, yrows[1, pl.ds(x, 1), :], pltpu.roll(slab, sizey - 1, 0))
            below = jnp.where(slab_row == 0, yrows[0, pl.ds(x, 1), :], pltpu.roll(slab, 1, 0))
            grad_y[x] = above - below
        return carry

    lax.fori_loop(0, cells_x, slope_y, 0)

    for j in range(1, nx):
        came = pltpu.make_async_remote_copy(
            src_ref=mine, dst_ref=theirs.at[lax.rem(me[0] + nx - j, nx)],
            send_sem=peer_send.at[j], recv_sem=peer_recv.at[j],
            device_id=peer(j), device_id_type=MESH,
        )
        came.wait_recv()

    lane_of = lax.broadcasted_iota(jnp.int32, (cells_z, 128), 1)
    z_of = lax.broadcasted_iota(jnp.int32, (cells_z, 128), 0)
    sums = theirs[...].reshape(8 * nx, 128)
    for k in range(3):
        step = jnp.dot(
            table_ref[k], jnp.concatenate([rhs[k], sums], axis=0),
            precision=HIGHEST, preferred_element_type=jnp.float32,
        )
        new = displacement[k] + step
        for y in range(2):
            new_ref[k, y] = lax.dot_general(
                jnp.where(lane_of == z_of + (SLOT * (y + 1) + 2), 1.0, 0.0), new[8 : 8 + cells_x],
                (((1,), (1,)), ((), ())), precision=HIGHEST, preferred_element_type=jnp.float32,
            )
        along = jnp.dot(new, prolong_ref[...], precision=HIGHEST, preferred_element_type=jnp.float32) * 0.5
        for s in range(4):
            lines[k, s] = along[:, sizez * s : sizez * (s + 1)]

    for copy in z_copies:
        copy.wait_send()
    for j in range(1, nx):
        peer_copy(j).wait_send()
    for step in (-1, 1):

        @pl.when(inside((step, 0, 0)))
        def _():
            x_copy(step).wait_send()

        @pl.when(inside((0, step, 0)))
        def _():
            y_copy(step).wait_send()

    for offset in offsets:

        @pl.when(inside(offset))
        def _():
            for part in range(2):
                near_copy(offset, part).wait_send()


def combine(
    chunks,
    new_in, lines, base, grad_x, grad_y, grad_z,
    new_hbm, out_hbm,
    out, new_sem, out_sem,
):
    sizex, sizey, sizez = base.shape
    cells_x = sizex // BIN
    span = sizex // chunks
    keep_new = pltpu.make_async_copy(new_in, new_hbm, new_sem.at[0])
    keep_new.start()

    third = lax.broadcasted_iota(jnp.int32, (8, sizez), 0).astype(jnp.float32)
    offset_y = (third + 0.5) / 8.0 - 0.5
    weight_low = jnp.maximum(-offset_y, 0.0)
    weight_high = jnp.maximum(offset_y, 0.0)
    weight_mid = 1.0 - jnp.abs(offset_y)

    def plane(at):
        planes = []
        for k in range(3):
            row_of = [lines[k, s, pl.ds(at, 1), :] for s in range(4)]
            planes.append(
                jnp.concatenate(
                    [
                        weight_low * row_of[c] + weight_mid * row_of[c + 1] + weight_high * row_of[c + 2]
                        for c in range(2)
                    ],
                    axis=0,
                )
            )
        return planes

    grads = (grad_x, grad_y, grad_z)

    def residual(cell, carry):
        now, rise = carry
        later = plane(cell + 9)
        climb = [(b - a) * 0.125 for a, b in zip(now, later)]
        start = pl.multiple_of(cell * BIN, BIN)
        for i in range(BIN):
            if i == 0:
                field = [n - 3.5 * r for n, r in zip(now, rise)]
            elif i == BIN // 2:
                field = [n + 0.5 * c for n, c in zip(now, climb)]
            else:
                field = [f + d for f, d in zip(field, rise if i < BIN // 2 else climb)]
            total = base[start + i]
            for grad, f in zip(grads, field):
                total = total - grad[start + i] * f
            out[start + i] = total.astype(jnp.bfloat16)
        return (later, climb)

    def store(c):
        slabs = pl.ds(c * span, span)
        return pltpu.make_async_copy(out.at[slabs], out_hbm.at[slabs], out_sem.at[c])

    before, now = plane(7), plane(8)
    state = (now, [(b - a) * 0.125 for a, b in zip(before, now)])
    for c in range(chunks):
        each = cells_x // chunks
        state = lax.fori_loop(c * each, (c + 1) * each, residual, state)
        store(c).start()
    for c in range(chunks):
        store(c).wait()
    keep_new.wait()


def on_device(counts, ref_image, def_image, displacement):
    nx, ny, nz = counts
    sizex, sizey, sizez = ref_image.shape
    cells_x, cells_z = sizex // BIN, sizez // BIN
    table, sums = inverse_table(nx, cells_x)
    place, binning, prolong = lane_tables(cells_z, sizez, 4)
    sides = 1 if nz == 2 else 2
    dma = pltpu.SemaphoreType.DMA
    vmem, anywhere = pl.BlockSpec(memory_space=pltpu.VMEM), pl.BlockSpec(memory_space=pl.ANY)
    shape = jax.ShapeDtypeStruct
    image = ref_image.shape
    cells = jnp.transpose(displacement, (0, 2, 3, 1))
    constants = (table, sums, place, binning, prolong)
    held = pl.pallas_call(
        functools.partial(exchange, counts),
        out_shape=(
            shape(cells.shape, jnp.float32),
            shape((3, 4, cells_x + 16, sizez), jnp.float32),
            shape(image, jnp.float32),
            shape(image, jnp.float32),
            shape(image, jnp.float32),
            shape(image, jnp.float32),
        ),
        in_specs=[pl.BlockSpec(memory_space=pltpu.HBM)] * 8,
        out_specs=(vmem,) * 6,
        scratch_shapes=[
            pltpu.VMEM((sides,) + image, jnp.bfloat16),
            pltpu.VMEM(image, jnp.bfloat16),
            pltpu.VMEM(image, jnp.bfloat16),
            pltpu.VMEM(cells.shape, jnp.float32),
            pltpu.VMEM(table.shape[1:], jnp.float32),
            pltpu.VMEM(sums.shape[1:], jnp.float32),
            pltpu.VMEM(place.shape, jnp.float32),
            pltpu.VMEM(binning.shape, jnp.float32),
            pltpu.VMEM(prolong.shape, jnp.float32),
            pltpu.VMEM((4, cells_x * 8, sizez), jnp.float32),
            pltpu.VMEM((3, 3, cells_x, 128), jnp.float32),
            pltpu.VMEM((3, 3, 3, cells_x + 16, 128), jnp.float32),
            pltpu.VMEM((8, 128), jnp.float32),
            pltpu.VMEM((nx, 8, 128), jnp.float32),
            pltpu.VMEM((2, sizey, sizez), jnp.bfloat16),
            pltpu.VMEM((2, sizex, sizez), jnp.float32),
            pltpu.VMEM((2, sizex, sizez), jnp.bfloat16),
            pltpu.VMEM((2, sizex, sizez), jnp.bfloat16),
            dma((8,)),
            dma((27, 2)), dma((27, 2)), dma((nx,)), dma((nx,)),
            dma((2,)), dma((2,)), dma((2,)), dma((2,)), dma((sides,)), dma((sides,)),
        ],
        compiler_params=pltpu.CompilerParams(
            collective_id=0, has_side_effects=True, vmem_limit_bytes=24 << 20
        ),
    )(*[pltpu.with_memory_space_constraint(jnp.asarray(x), pltpu.HBM) for x in (ref_image, def_image, cells) + constants])
    chunks = 4
    new, residual = pl.pallas_call(
        functools.partial(combine, chunks),
        out_shape=(shape(cells.shape, jnp.float32), shape(image, jnp.bfloat16)),
        in_specs=[vmem] * 6,
        out_specs=(anywhere, anywhere),
        scratch_shapes=[pltpu.VMEM(image, jnp.bfloat16), dma((1,)), dma((chunks,))],
        compiler_params=pltpu.CompilerParams(vmem_limit_bytes=16 << 20),
    )(*held)
    return jnp.transpose(new, (0, 3, 1, 2)), residual


def solution(mesh):
    counts = tuple(mesh.shape[axis] for axis in ("gx", "gy", "gz"))
    return jax.shard_map(
        functools.partial(on_device, counts),
        mesh=mesh,
        in_specs=(P("gx", "gy", "gz"), P("gx", "gy", "gz"), P(None, "gx", "gy", "gz")),
        out_specs=(P(None, "gx", "gy", "gz"), P("gx", "gy", "gz")),
        check_vma=False,
    )
```

```python
import functools

import jax
import jax.numpy as jnp
import numpy as np
from jax import lax
from jax.experimental import pallas as pl
from jax.experimental.pallas import tpu as pltpu
from jax.sharding import PartitionSpec as P

stiffness = 64.0
BIN = 8
SLOT = 32
MESH = pl.DeviceIdType.MESH
half = jnp.bfloat16


def solve_tables(devices, cells, rows):
    lines = devices * cells
    theta = np.arccosh((1.0 + 2.0 * stiffness) / (2.0 * stiffness))
    index = np.arange(lines)
    low = np.minimum(index[:, None], index[None, :])
    high = np.maximum(index[:, None], index[None, :])
    a, b, c = (low + 1) * theta, (lines - high) * theta, (lines + 1) * theta
    inverse = (
        np.exp(a + b - c) * (1 - np.exp(-2 * a)) * (1 - np.exp(-2 * b)) / (1 - np.exp(-2 * c))
        / (2.0 * stiffness * np.sinh(theta))
    )
    solve = np.zeros((devices, 2 * rows, 2 * lines), np.float32)
    pick = np.zeros((devices, rows, 3 * lines), np.float32)
    for me in range(devices):
        first = me * cells
        for row, x in [(r, first + r) for r in range(cells + 1)] + [(rows - 1, first - 1)]:
            if x < 0 or x >= lines:
                continue
            top = inverse[x].astype(half).astype(np.float64)
            solve[me, row, :lines] = top
            solve[me, row, lines:] = top
            solve[me, rows + row, :lines] = inverse[x] - top
            pick[me, row, x::lines] = 1.0
    return solve.astype(half), pick.astype(half)


def lane_tables(cells_z, size_z, deep, slots):
    binning = np.repeat(np.eye(cells_z, dtype=np.float32), BIN, axis=1) / 32.0
    prolong = np.zeros((slots * SLOT, slots * size_z), np.float32)
    for slot in range(slots):
        for fine in range(size_z):
            cell, offset = fine // BIN, (fine % BIN + 0.5) / BIN - 0.5
            other = (cell + (1 if offset >= 0 else -1)) % deep
            prolong[slot * SLOT + cell, slot * size_z + fine] = 0.5 * (1.0 - abs(offset))
            prolong[slot * SLOT + other, slot * size_z + fine] = 0.5 * abs(offset)
    return np.tile(binning, (1, 2)).astype(half), np.tile(prolong, (2, 1)).astype(half)


def pieces(value, count):
    parts = []
    for i in range(count):
        part = value.astype(half)
        parts.append(part)
        if i < count - 1:
            value = value - part.astype(jnp.float32)
    return parts


def across_lanes(a, b):
    return lax.dot_general(a, b, (((1,), (1,)), ((), ())), preferred_element_type=jnp.float32)


def exchange(
    counts, chunks, early,
    ref_hbm, def_hbm, disp_hbm, solve_hbm, pick_hbm, bin_hbm, prolong_hbm,
    new_ref, lines, base, grad_x, grad_y, grad_z,
    zhalo, ref_ref, def_ref, disp_ref, solve_ref, pick_ref, bin_ref, prolong_ref,
    binned, stack, cells, rims, own_rim, moved, moved_rims, own_moved_rim, dline, dsplit, rsplit,
    xhalo, yrows, ysend, yhalo,
    load_sem, image_sem,
    b_send, b_recv, e_send, e_recv, d_send, d_recv, f_send, f_recv,
    x_send, x_recv, y_send, y_recv, z_send, z_recv,
):
    nx, ny, nz = counts
    sizex, sizey, sizez = def_ref.shape
    cells_x, cells_z = sizex // BIN, sizez // BIN
    groups = 128 // cells_x
    across_x = nx * cells_x
    deep = cells.shape[2]
    rows = new_ref.shape[0]
    me = (lax.axis_index("gx"), lax.axis_index("gy"), lax.axis_index("gz"))
    turn = lax.rem(me[0], groups)

    def device(j, dy, dz):
        gz = me[2] + dz if nz > 2 or dz == 0 else 1 - me[2]
        return {"gx": lax.rem(me[0] + j, nx), "gy": me[1] + dy, "gz": gz}

    def guarded(dy, dz, act):
        tests = []
        for at, step, count in ((me[1], dy, ny), (me[2], dz if nz > 2 else 0, nz)):
            if step:
                tests.append(at > 0 if step < 0 else at < count - 1)
        if tests:
            pl.when(functools.reduce(jnp.logical_and, tests))(act)
        else:
            act()

    z_steps = (1,) if nz == 2 else (1, -1)

    def side_out(dz):
        return me[2] if nz == 2 else (0 if dz > 0 else 1)

    def side_in(dz):
        return 1 - me[2] if nz == 2 else (1 if dz > 0 else 0)

    small = [
        pltpu.make_async_copy(hbm, held, load_sem.at[i])
        for i, (hbm, held) in enumerate(
            (
                (disp_hbm, disp_ref), (bin_hbm, bin_ref), (pick_hbm.at[me[0]], pick_ref),
                (solve_hbm.at[me[0]], solve_ref), (prolong_hbm, prolong_ref),
            )
        )
    ]
    span = sizex // chunks
    images = [
        [
            pltpu.make_async_copy(
                hbm.at[pl.ds(c * span, span)], held.at[pl.ds(c * span, span)], image_sem.at[i, c]
            )
            for i, (hbm, held) in enumerate(((ref_hbm, ref_ref), (def_hbm, def_ref)))
        ]
        for c in range(chunks)
    ]
    small[0].start()
    for pair in images:
        for load in pair:
            load.start()
    for load in small[1:]:
        load.start()

    for buffer in (cells, rims, moved, moved_rims, xhalo, yhalo):
        buffer[...] = jnp.zeros_like(buffer)
    if nz > 2:

        @pl.when(me[2] == 0)
        def _():
            zhalo[0] = jnp.zeros(zhalo.shape[1:], half)

        @pl.when(me[2] == nz - 1)
        def _():
            zhalo[1] = jnp.zeros(zhalo.shape[1:], half)

    barrier = pltpu.get_barrier_semaphore()
    for dy in (0, -1, 1):

        def greet(dy=dy):
            for j in range(nx):
                for dz in (0,) + z_steps:
                    if (j, dy, dz) != (0, 0, 0):

                        def hail(j=j, dz=dz):
                            pl.semaphore_signal(barrier, inc=1, device_id=device(j, dy, dz), device_id_type=MESH)

                        guarded(0, dz, hail)

        guarded(dy, 0, greet)

    reach = [
        1 + (at > 0).astype(jnp.int32) + (at < count - 1).astype(jnp.int32)
        for at, count in zip(me, counts)
    ]
    expect = nx * reach[1] * (2 if nz == 2 else reach[2]) - 1

    def remote(src, dst, send, recv, to):
        return pltpu.make_async_remote_copy(
            src_ref=src, dst_ref=dst, send_sem=send, recv_sem=recv, device_id=to, device_id_type=MESH
        )

    small[0].wait()
    for y in range(2):
        tile = jnp.concatenate(
            [disp_ref[k, y] for k in range(3)] + [jnp.zeros((cells_z, 128 - 3 * cells_x), jnp.float32)], axis=1
        )
        tile = pltpu.roll(tile, turn * cells_x, 1)
        moved[1 + y, me[0], pl.ds(0, cells_z)] = tile
        own_moved_rim[0, y] = tile[cells_z - 1 :]
        own_moved_rim[1, y] = tile[:1]

    body = pl.ds(0, cells_z)

    def moved_copy(j, dy):
        here = {0: pl.ds(1, 2), 1: pl.ds(2, 1), -1: pl.ds(1, 1)}[dy]
        there = {0: pl.ds(1, 2), 1: pl.ds(0, 1), -1: pl.ds(3, 1)}[dy]
        return remote(
            moved.at[here, me[0], body], moved.at[there, me[0], body],
            d_send.at[1 + dy], d_recv.at[1 - dy], device(j, dy, 0),
        )

    def moved_rim_copy(j, dy, dz):
        here = {0: pl.ds(0, 2), 1: pl.ds(1, 1), -1: pl.ds(0, 1)}[dy]
        there = {0: pl.ds(1, 2), 1: pl.ds(0, 1), -1: pl.ds(3, 1)}[dy]
        side = side_out(dz)
        return remote(
            own_moved_rim.at[side, here], moved_rims.at[side, there, me[0]],
            f_send.at[side, 1 + dy], f_recv.at[side, 1 - dy], device(j, dy, dz),
        )

    def cell_copy(j, dy):
        return remote(
            cells.at[1, me[0], body], cells.at[1 - dy, me[0], body],
            b_send.at[1 + dy], b_recv.at[1 - dy], device(j, dy, 0),
        )

    def rim_copy(j, dy, dz):
        side = side_out(dz)
        return remote(
            own_rim.at[side], rims.at[side, 1 - dy, me[0]],
            e_send.at[side, 1 + dy], e_recv.at[side, 1 - dy], device(j, dy, dz),
        )

    def start_all(flat, rim):
        for dy in (-1, 1, 0):

            def act(dy=dy):
                for j in list(range(nx - 1, 0, -1)) + ([0] if dy else []):
                    flat(j, dy).start()
                for j in range(nx - 1, -1, -1):
                    for dz in z_steps:
                        guarded(0, dz, lambda j=j, dz=dz: rim(j, dy, dz).start())

            guarded(dy, 0, act)

    def wait_flat(dy, flat_ref, send, recv, sent):
        count = nx if dy else nx - 1
        ref = flat_ref(dy, count)
        copy = remote(ref, ref, send.at[1 + dy], recv.at[1 + dy], device(1, 0, 0))
        copy.wait_send() if sent else copy.wait_recv()

    def wait_rim(dy, dz, rim_ref, send, recv, sent):
        ref = rim_ref(dy)
        copy = remote(
            ref, ref, send.at[side_out(dz), 1 + dy], recv.at[side_in(dz), 1 + dy], device(1, 0, 0)
        )
        copy.wait_send() if sent else copy.wait_recv()

    def wait_all(flat_ref, rim_ref, sems, sent):
        for dy in (0, -1, 1):

            def act(dy=dy):
                wait_flat(dy, flat_ref, sems[0], sems[1], sent)
                for dz in z_steps:
                    guarded(0, dz, lambda dz=dz: wait_rim(dy, dz, rim_ref, sems[2], sems[3], sent))

            guarded(dy, 0, act)

    def cell_ref(dy, count):
        return cells.at[0, pl.ds(0, count), body]

    def rim_ref(dy):
        return rims.at[0, 0]

    def moved_ref(dy, count):
        return moved.at[pl.ds(0, 1 if dy else 2), pl.ds(0, count), body]

    def moved_rim_ref(dy):
        return moved_rims.at[0, pl.ds(0, 1 if dy else 2)]

    def bin_cell(cell, carry):
        at = pl.multiple_of(cell * 8, 8)
        total = [None, None]
        for i in range(BIN):
            x = cell * BIN + i
            slabs = (ref_ref[x].astype(jnp.float32), def_ref[x].astype(jnp.float32))
            yrows[0, pl.ds(x, 1), :] = slabs[0][:1]
            yrows[1, pl.ds(x, 1), :] = slabs[0][sizey - 1 :]
            total = [s if t is None else t + s for t, s in zip(total, slabs)]
        for image in range(2):
            for y in range(2):
                binned[2 * image + y, pl.ds(at, 8), :] = total[image][8 * y : 8 * y + 8]
        return carry

    def bin_chunk(c):
        for load in images[c]:
            load.wait()
        each = cells_x // chunks
        lax.fori_loop(c * each, (c + 1) * each, bin_cell, 0)

    for c in range(early):
        bin_chunk(c)
    pl.semaphore_wait(barrier, expect)
    start_all(moved_copy, moved_rim_copy)
    for c in range(early, chunks):
        bin_chunk(c)

    small[1].wait()
    for q in range(4):
        line = binned[q, pl.ds(0, cells_x, stride=8), :]
        for s in range(1, 8):
            line = line + binned[q, pl.ds(s, cells_x, stride=8), :]
        at = pl.multiple_of(lax.rem(turn + q, groups) * cells_x, cells_x)
        for i, part in enumerate(pieces(line, 2)):
            stack[pl.ds(at, cells_x), pl.ds(i * sizez, sizez)] = part
    tile = across_lanes(bin_ref[...], stack[...])
    cells[1, me[0], body] = tile
    own_rim[0] = tile[cells_z - 2 :]
    own_rim[1] = tile[:2]
    start_all(cell_copy, rim_copy)

    def x_copy(step):
        side = 0 if step > 0 else 1
        return remote(
            ref_ref.at[pl.ds(sizex - 1 if step > 0 else 0, 1)], xhalo.at[pl.ds(side, 1)],
            x_send.at[side], x_recv.at[side],
            {"gx": me[0] + step, "gy": me[1], "gz": me[2]},
        )

    def y_copy(step):
        side = 1 if step > 0 else 0
        return remote(
            ysend.at[side], yhalo.at[1 - side], y_send.at[side], y_recv.at[1 - side], device(0, step, 0)
        )

    def z_copy(dz):
        i = 0 if dz > 0 else 1
        return remote(ref_ref, zhalo.at[i], z_send.at[i], z_recv.at[i], device(0, 0, dz))

    def at_x(step, act):
        pl.when(me[0] > 0 if step < 0 else me[0] < nx - 1)(act)

    ysend[...] = yrows[...].astype(half)
    for step in (-1, 1):
        guarded(step, 0, lambda step=step: y_copy(step).start())
        at_x(step, lambda step=step: x_copy(step).start())
    for dz in z_steps:
        guarded(0, dz, lambda dz=dz: z_copy(dz).start())

    def prepare(cell, carry):
        start = pl.multiple_of(cell * BIN, BIN)
        first = jnp.maximum(start - 1, 0)
        last = jnp.minimum(start + BIN, sizex - 1)
        slabs = [ref_ref[first].astype(jnp.float32)]
        slabs += [ref_ref[start + i].astype(jnp.float32) for i in range(BIN)]
        slabs += [ref_ref[last].astype(jnp.float32)]
        for i in range(BIN):
            base[start + i] = def_ref[start + i].astype(jnp.float32) - slabs[i + 1]
            grad_x[start + i] = slabs[i + 2] - slabs[i]
        return carry

    lax.fori_loop(0, cells_x, prepare, 0)

    group = lax.broadcasted_iota(jnp.int32, (deep, 128), 1) // cells_x

    def gather(tiles, q):
        out = []
        for t in range(nx // groups):
            value = tiles[t * groups + (-q) % groups]
            for g in range(1, groups):
                value = jnp.where(group == g, tiles[t * groups + (g - q) % groups], value)
            out.append(pltpu.roll(value, (groups - q) * cells_x, 1) if q else value)
        return out[0] if len(out) == 1 else jnp.concatenate(out, axis=1)

    blank = jnp.zeros((SLOT - deep, across_x), jnp.float32)

    def split_store(target, k, y, value, count):
        padded = jnp.concatenate([value, blank], axis=0)
        for i, part in enumerate(pieces(padded, count)):
            target[pl.ds((4 * k + y) * SLOT, SLOT), pl.ds(i * across_x, across_x)] = part

    for load in small[2:]:
        load.wait()
    wait_all(moved_ref, moved_rim_ref, (d_send, d_recv, f_send, f_recv), False)
    for y in range(4):
        for i in range(nx):
            moved[y, i, pl.ds(cells_z, 1)] = moved_rims[1, y, i]
            moved[y, i, pl.ds(deep - 1, 1)] = moved_rims[0, y, i]
    for y in range(4):
        tiles = [moved[y, i] for i in range(nx)]
        for k in range(3):
            value = gather(tiles, k)
            dline[k, y] = value
            split_store(dsplit, k, y, value, 3)
    new_ref[...] = across_lanes(pick_ref[...], dsplit[...])

    for dz in z_steps:
        guarded(0, dz, lambda dz=dz: z_copy(-dz if nz > 2 else dz).wait_recv())

    row = lax.broadcasted_iota(jnp.int32, (sizez, sizez), 0)
    column = lax.broadcasted_iota(jnp.int32, (sizez, sizez), 1)
    inner = jnp.where(row == column + 1, 1.0, 0.0) - jnp.where(row + 1 == column, 1.0, 0.0)
    from_low = jnp.where(
        jnp.logical_and(jnp.logical_and(row == sizez - 1, column == 0), me[2] > 0), -1.0, 0.0
    )
    from_high = jnp.where(
        jnp.logical_and(jnp.logical_and(row == 0, column == sizez - 1), me[2] < nz - 1), 1.0, 0.0
    )
    outer = [from_low + from_high] if nz == 2 else [from_low, from_high]
    across = jnp.concatenate([inner] + outer, axis=0).astype(half)

    def slope_z(cell, carry):
        start = pl.multiple_of(cell * BIN, BIN)
        sideways = [ref_ref[pl.ds(start, BIN)].reshape(BIN * sizey, sizez)]
        sideways += [zhalo[i, pl.ds(start, BIN)].reshape(BIN * sizey, sizez) for i in range(len(z_steps))]
        slope = jnp.dot(jnp.concatenate(sideways, axis=1), across, preferred_element_type=jnp.float32)
        grad_z[pl.ds(start, BIN)] = slope.reshape(BIN, sizey, sizez)
        return carry

    lax.fori_loop(0, cells_x, slope_z, 0)

    for step in (-1, 1):
        at_x(step, lambda step=step: x_copy(-step).wait_recv())
        guarded(step, 0, lambda step=step: y_copy(-step).wait_recv())
    grad_x[0] = ref_ref[1].astype(jnp.float32) - xhalo[0].astype(jnp.float32)
    grad_x[sizex - 1] = xhalo[1].astype(jnp.float32) - ref_ref[sizex - 2].astype(jnp.float32)
    yrows[...] = yhalo[...].astype(jnp.float32)
    slab_row = lax.broadcasted_iota(jnp.int32, (sizey, sizez), 0)

    def slope_y(cell, carry):
        start = pl.multiple_of(cell * BIN, BIN)
        for i in range(BIN):
            x = start + i
            slab = ref_ref[x].astype(jnp.float32)
            above = jnp.where(slab_row == sizey - 1, yrows[1, pl.ds(x, 1), :], pltpu.roll(slab, sizey - 1, 0))
            below = jnp.where(slab_row == 0, yrows[0, pl.ds(x, 1), :], pltpu.roll(slab, 1, 0))
            grad_y[x] = above - below
        return carry

    lax.fori_loop(0, cells_x, slope_y, 0)

    wait_all(cell_ref, rim_ref, (b_send, b_recv, e_send, e_recv), False)
    for dy in range(3):
        for i in range(nx):
            cells[dy, i, pl.ds(cells_z, 2)] = rims[1, dy, i]
            cells[dy, i, pl.ds(deep - 2, 2)] = rims[0, dy, i]
    tiles = [[cells[dy, i] for i in range(nx)] for dy in range(3)]
    coarse = [gather(tiles[dy], q) for dy in range(3) for q in range(2)]
    deformed = [gather(tiles[dy], q) for dy, q in ((0, 3), (1, 2), (1, 3), (2, 2))]
    lane = lax.broadcasted_iota(jnp.int32, (deep, across_x), 1)
    for y in range(4):
        c = coarse[y + 1]
        slopes = [
            (
                jnp.where(lane == across_x - 1, 0.0, pltpu.roll(c, across_x - 1, 1))
                - jnp.where(lane == 0, 0.0, pltpu.roll(c, 1, 1))
            ) * 0.5,
            (coarse[y + 2] - coarse[y]) * 0.5,
            (pltpu.roll(c, deep - 1, 0) - pltpu.roll(c, 1, 0)) * 0.5,
        ]
        mismatch = deformed[y] - c - (
            slopes[0] * dline[0, y] + slopes[1] * dline[1, y] + slopes[2] * dline[2, y]
        )
        for k in range(3):
            split_store(rsplit, k, y, slopes[k] * mismatch, 2)
    step = across_lanes(solve_ref[...], rsplit[...])
    new = new_ref[...] + (step[:rows] + step[rows:])
    new_ref[...] = new
    parts = [
        jnp.concatenate(pieces(new[:, 4 * SLOT * k : 4 * SLOT * (k + 1)], 2), axis=1) for k in range(3)
    ]
    along = jnp.dot(jnp.concatenate(parts, axis=0), prolong_ref[...], preferred_element_type=jnp.float32)
    for k in range(3):
        for s in range(4):
            lines[k, s] = along[rows * k : rows * (k + 1), sizez * s : sizez * (s + 1)]

    wait_all(moved_ref, moved_rim_ref, (d_send, d_recv, f_send, f_recv), True)
    wait_all(cell_ref, rim_ref, (b_send, b_recv, e_send, e_recv), True)
    for step in (-1, 1):
        guarded(step, 0, lambda step=step: y_copy(step).wait_send())
        at_x(step, lambda step=step: x_copy(step).wait_send())
    for dz in z_steps:
        guarded(0, dz, lambda dz=dz: z_copy(dz).wait_send())


def combine(
    chunks,
    new_in, lines, base, grad_x, grad_y, grad_z,
    new_hbm, out_hbm,
    out, turned, new_sem, out_sem,
):
    sizex, sizey, sizez = base.shape
    cells_x = sizex // BIN
    span = sizex // chunks
    keep_new = pltpu.make_async_copy(turned, new_hbm, new_sem.at[0])
    cells_z = sizez // BIN
    before_row = new_in.shape[0] - 1

    third = lax.broadcasted_iota(jnp.int32, (8, sizez), 0).astype(jnp.float32)
    offset_y = (third + 0.5) / 8.0 - 0.5
    weight_low = jnp.maximum(-offset_y, 0.0)
    weight_high = jnp.maximum(offset_y, 0.0)
    weight_mid = 1.0 - jnp.abs(offset_y)

    def plane(at):
        planes = []
        for k in range(3):
            row_of = [lines[k, s, pl.ds(at, 1), :] for s in range(4)]
            planes.append(
                jnp.concatenate(
                    [
                        weight_low * row_of[c] + weight_mid * row_of[c + 1] + weight_high * row_of[c + 2]
                        for c in range(2)
                    ],
                    axis=0,
                )
            )
        return planes

    grads = (grad_x, grad_y, grad_z)

    def residual(cell, carry):
        now, rise = carry
        later = plane(cell + 1)
        climb = [(b - a) * 0.125 for a, b in zip(now, later)]
        start = pl.multiple_of(cell * BIN, BIN)
        for i in range(BIN):
            if i == 0:
                field = [n - 3.5 * r for n, r in zip(now, rise)]
            elif i == BIN // 2:
                field = [n + 0.5 * c for n, c in zip(now, climb)]
            else:
                field = [f + d for f, d in zip(field, rise if i < BIN // 2 else climb)]
            total = base[start + i]
            for grad, f in zip(grads, field):
                total = total - grad[start + i] * f
            out[start + i] = total.astype(jnp.bfloat16)
        return (later, climb)

    def store(c):
        slabs = pl.ds(c * span, span)
        return pltpu.make_async_copy(out.at[slabs], out_hbm.at[slabs], out_sem.at[c])

    before, now = plane(before_row), plane(0)
    state = (now, [(b - a) * 0.125 for a, b in zip(before, now)])
    for c in range(chunks):
        each = cells_x // chunks
        state = lax.fori_loop(c * each, (c + 1) * each, residual, state)
        store(c).start()
        if c == 0:
            for k in range(3):
                flipped = new_in[:cells_x, 4 * SLOT * k : 4 * SLOT * (k + 1)].T
                for y in range(2):
                    turned[k, y] = flipped[SLOT * (y + 1) : SLOT * (y + 1) + cells_z]
            keep_new.start()
    for c in range(chunks):
        store(c).wait()
    keep_new.wait()


def on_device(counts, ref_image, def_image, displacement):
    nx, ny, nz = counts
    sizex, sizey, sizez = ref_image.shape
    cells_x, cells_z = sizex // BIN, sizez // BIN
    rows, deep, across_x = cells_x + 16, cells_z + 8, nx * cells_x
    solve, pick = solve_tables(nx, cells_x, rows)
    binning, prolong = lane_tables(cells_z, sizez, deep, 4)
    sides = 1 if nz == 2 else 2
    dma = pltpu.SemaphoreType.DMA
    vmem, anywhere = pl.BlockSpec(memory_space=pltpu.VMEM), pl.BlockSpec(memory_space=pl.ANY)
    shape = jax.ShapeDtypeStruct
    image = ref_image.shape
    coarse = jnp.transpose(displacement, (0, 2, 3, 1))
    constants = (solve, pick, binning, prolong)
    f32 = jnp.float32
    held = pl.pallas_call(
        functools.partial(exchange, counts, 4, 2),
        out_shape=(
            shape((rows, 12 * SLOT), f32),
            shape((3, 4, rows, sizez), f32),
            shape(image, f32),
            shape(image, f32),
            shape(image, f32),
            shape(image, f32),
        ),
        in_specs=[pl.BlockSpec(memory_space=pltpu.HBM)] * 7,
        out_specs=(vmem,) * 6,
        scratch_shapes=[
            pltpu.VMEM((sides,) + image, half),
            pltpu.VMEM(image, half),
            pltpu.VMEM(image, half),
            pltpu.VMEM(coarse.shape, f32),
            pltpu.VMEM(solve.shape[1:], half),
            pltpu.VMEM(pick.shape[1:], half),
            pltpu.VMEM(binning.shape, half),
            pltpu.VMEM(prolong.shape, half),
            pltpu.VMEM((4, cells_x * 8, sizez), f32),
            pltpu.VMEM((4 * cells_x, 2 * sizez), half),
            pltpu.VMEM((3, nx, deep, 128), f32),
            pltpu.VMEM((2, 3, nx, 2, 128), f32),
            pltpu.VMEM((2, 2, 128), f32),
            pltpu.VMEM((4, nx, deep, 128), f32),
            pltpu.VMEM((2, 4, nx, 1, 128), f32),
            pltpu.VMEM((2, 2, 1, 128), f32),
            pltpu.VMEM((3, 4, deep, across_x), f32),
            pltpu.VMEM((12 * SLOT, 3 * across_x), half),
            pltpu.VMEM((12 * SLOT, 2 * across_x), half),
            pltpu.VMEM((2, sizey, sizez), half),
            pltpu.VMEM((2, sizex, sizez), f32),
            pltpu.VMEM((2, sizex, sizez), half),
            pltpu.VMEM((2, sizex, sizez), half),
            dma((5,)), dma((2, 4)),
            dma((3,)), dma((3,)), dma((2, 3)), dma((2, 3)),
            dma((3,)), dma((3,)), dma((2, 3)), dma((2, 3)),
            dma((2,)), dma((2,)), dma((2,)), dma((2,)), dma((sides,)), dma((sides,)),
        ],
        compiler_params=pltpu.CompilerParams(
            collective_id=0, has_side_effects=True, vmem_limit_bytes=24 << 20
        ),
    )(*[pltpu.with_memory_space_constraint(jnp.asarray(x), pltpu.HBM) for x in (ref_image, def_image, coarse) + constants])
    chunks = 4
    new, residual = pl.pallas_call(
        functools.partial(combine, chunks),
        out_shape=(shape(coarse.shape, f32), shape(image, half)),
        in_specs=[vmem] * 6,
        out_specs=(anywhere, anywhere),
        scratch_shapes=[pltpu.VMEM(image, half), pltpu.VMEM(coarse.shape, f32), dma((1,)), dma((chunks,))],
        compiler_params=pltpu.CompilerParams(vmem_limit_bytes=16 << 20),
    )(*held)
    return jnp.transpose(new, (0, 3, 1, 2)), residual


def solution(mesh):
    counts = tuple(mesh.shape[axis] for axis in ("gx", "gy", "gz"))
    return jax.shard_map(
        functools.partial(on_device, counts),
        mesh=mesh,
        in_specs=(P("gx", "gy", "gz"), P("gx", "gy", "gz"), P(None, "gx", "gy", "gz")),
        out_specs=(P(None, "gx", "gy", "gz"), P("gx", "gy", "gz")),
        check_vma=False,
    )
```

```python
import functools

import jax
import jax.numpy as jnp
import numpy as np
from jax import lax
from jax.experimental import pallas as pl
from jax.experimental.pallas import tpu as pltpu
from jax.sharding import PartitionSpec as P

stiffness = 64.0
BIN = 8
SLOT = 32
MESH = pl.DeviceIdType.MESH
half = jnp.bfloat16


def solve_tables(devices, cells, rows):
    lines = devices * cells
    theta = np.arccosh((1.0 + 2.0 * stiffness) / (2.0 * stiffness))
    index = np.arange(lines)
    low = np.minimum(index[:, None], index[None, :])
    high = np.maximum(index[:, None], index[None, :])
    a, b, c = (low + 1) * theta, (lines - high) * theta, (lines + 1) * theta
    inverse = (
        np.exp(a + b - c) * (1 - np.exp(-2 * a)) * (1 - np.exp(-2 * b)) / (1 - np.exp(-2 * c))
        / (2.0 * stiffness * np.sinh(theta))
    )
    solve = np.zeros((devices, 2 * rows, 2 * lines), np.float32)
    pick = np.zeros((devices, rows, 3 * lines), np.float32)
    for me in range(devices):
        first = me * cells
        for row, x in [(r, first + r) for r in range(cells + 1)] + [(rows - 1, first - 1)]:
            if x < 0 or x >= lines:
                continue
            top = inverse[x].astype(half).astype(np.float64)
            solve[me, row, :lines] = top
            solve[me, row, lines:] = top
            solve[me, rows + row, :lines] = inverse[x] - top
            pick[me, row, x::lines] = 1.0
    return solve.astype(half), pick.astype(half)


def lane_tables(cells_z, size_z, deep, slots):
    binning = np.repeat(np.eye(cells_z, dtype=np.float32), BIN, axis=1) / 32.0
    prolong = np.zeros((slots * SLOT, slots * size_z), np.float32)
    for slot in range(slots):
        for fine in range(size_z):
            cell, offset = fine // BIN, (fine % BIN + 0.5) / BIN - 0.5
            other = (cell + (1 if offset >= 0 else -1)) % deep
            prolong[slot * SLOT + cell, slot * size_z + fine] = 0.5 * (1.0 - abs(offset))
            prolong[slot * SLOT + other, slot * size_z + fine] = 0.5 * abs(offset)
    return np.tile(binning, (1, 3)).astype(half), np.tile(prolong, (2, 1)).astype(half)


def pieces(value, count):
    parts = []
    for i in range(count):
        part = value.astype(half)
        parts.append(part)
        if i < count - 1:
            value = value - part.astype(jnp.float32)
    return parts


def across_lanes(a, b):
    return lax.dot_general(a, b, (((1,), (1,)), ((), ())), preferred_element_type=jnp.float32)


def exchange(
    counts, chunks, early,
    ref_hbm, def_hbm, disp_hbm, solve_hbm, pick_hbm, bin_hbm, prolong_hbm,
    new_ref, lines, base, grad_x, grad_y, grad_z,
    zhalo, ref_ref, def_ref, disp_ref, solve_ref, pick_ref, bin_ref, prolong_ref,
    binned, stack, cells, rims, own_rim, moved, moved_rims, own_moved_rim, dline, dsplit, rsplit,
    xhalo, yrows, ysend, yhalo,
    load_sem, image_sem,
    b_send, b_recv, e_send, e_recv, d_send, d_recv, f_send, f_recv,
    x_send, x_recv, y_send, y_recv, z_send, z_recv,
):
    nx, ny, nz = counts
    sizex, sizey, sizez = def_ref.shape
    cells_x, cells_z = sizex // BIN, sizez // BIN
    groups = 128 // cells_x
    across_x = nx * cells_x
    deep = cells.shape[2]
    rows = new_ref.shape[0]
    me = (lax.axis_index("gx"), lax.axis_index("gy"), lax.axis_index("gz"))
    turn = lax.rem(me[0], groups)

    def device(j, dy, dz):
        gz = me[2] + dz if nz > 2 or dz == 0 else 1 - me[2]
        return {"gx": lax.rem(me[0] + j, nx), "gy": me[1] + dy, "gz": gz}

    def guarded(dy, dz, act):
        tests = []
        for at, step, count in ((me[1], dy, ny), (me[2], dz if nz > 2 else 0, nz)):
            if step:
                tests.append(at > 0 if step < 0 else at < count - 1)
        if tests:
            pl.when(functools.reduce(jnp.logical_and, tests))(act)
        else:
            act()

    z_steps = (1,) if nz == 2 else (1, -1)

    def side_out(dz):
        return me[2] if nz == 2 else (0 if dz > 0 else 1)

    def side_in(dz):
        return 1 - me[2] if nz == 2 else (1 if dz > 0 else 0)

    barrier = pltpu.get_barrier_semaphore()
    for dy in (0, -1, 1):

        def greet(dy=dy):
            for j in range(nx):
                for dz in (0,) + z_steps:
                    if (j, dy, dz) != (0, 0, 0):

                        def hail(j=j, dz=dz):
                            pl.semaphore_signal(barrier, inc=1, device_id=device(j, dy, dz), device_id_type=MESH)

                        guarded(0, dz, hail)

        guarded(dy, 0, greet)

    small = [
        pltpu.make_async_copy(hbm, held, load_sem.at[i])
        for i, (hbm, held) in enumerate(
            (
                (disp_hbm, disp_ref), (bin_hbm, bin_ref), (pick_hbm.at[me[0]], pick_ref),
                (solve_hbm.at[me[0]], solve_ref), (prolong_hbm, prolong_ref),
            )
        )
    ]
    span = sizex // chunks
    images = [
        [
            pltpu.make_async_copy(
                hbm.at[pl.ds(c * span, span)], held.at[pl.ds(c * span, span)], image_sem.at[i, c]
            )
            for i, (hbm, held) in enumerate(((ref_hbm, ref_ref), (def_hbm, def_ref)))
        ]
        for c in range(chunks)
    ]
    small[0].start()
    for pair in images:
        for load in pair:
            load.start()
    for load in small[1:]:
        load.start()

    def clear(test, *parts):
        @pl.when(test)
        def _():
            for part in parts:
                part[...] = jnp.zeros(part.shape, part.dtype)

    low_y, high_y = me[1] == 0, me[1] == ny - 1
    low_z, high_z = me[2] == 0, me[2] == nz - 1
    clear(me[0] == 0, xhalo.at[0])
    clear(me[0] == nx - 1, xhalo.at[1])
    clear(low_y, yhalo.at[0], cells.at[0], moved.at[0], rims.at[:, 0], moved_rims.at[:, 0])
    clear(high_y, yhalo.at[1], cells.at[2], moved.at[3], rims.at[:, 2], moved_rims.at[:, 3])
    clear(low_z, rims.at[0], moved_rims.at[0])
    clear(high_z, rims.at[1], moved_rims.at[1])
    if nz > 2:
        clear(low_z, zhalo.at[0])
        clear(high_z, zhalo.at[1])
    for tiles in (cells, moved):
        for line in range(tiles.shape[0]):
            for i in range(nx):
                tiles[line, i, pl.ds(cells_z, deep - cells_z)] = jnp.zeros((deep - cells_z, 128), jnp.float32)

    reach = [
        1 + (at > 0).astype(jnp.int32) + (at < count - 1).astype(jnp.int32)
        for at, count in zip(me, counts)
    ]
    expect = nx * reach[1] * (2 if nz == 2 else reach[2]) - 1

    def remote(src, dst, send, recv, to):
        return pltpu.make_async_remote_copy(
            src_ref=src, dst_ref=dst, send_sem=send, recv_sem=recv, device_id=to, device_id_type=MESH
        )

    small[0].wait()
    for y in range(2):
        tile = jnp.concatenate(
            [disp_ref[k, y] for k in range(3)] + [jnp.zeros((cells_z, 128 - 3 * cells_x), jnp.float32)], axis=1
        )
        tile = pltpu.roll(tile, turn * cells_x, 1)
        moved[1 + y, me[0], pl.ds(0, cells_z)] = tile
        own_moved_rim[0, y] = tile[cells_z - 1 :]
        own_moved_rim[1, y] = tile[:1]

    body = pl.ds(0, cells_z)

    def moved_copy(j, dy):
        here = {0: pl.ds(1, 2), 1: pl.ds(2, 1), -1: pl.ds(1, 1)}[dy]
        there = {0: pl.ds(1, 2), 1: pl.ds(0, 1), -1: pl.ds(3, 1)}[dy]
        return remote(
            moved.at[here, me[0], body], moved.at[there, me[0], body],
            d_send.at[1 + dy], d_recv.at[1 - dy], device(j, dy, 0),
        )

    def moved_rim_copy(j, dy, dz):
        here = {0: pl.ds(0, 2), 1: pl.ds(1, 1), -1: pl.ds(0, 1)}[dy]
        there = {0: pl.ds(1, 2), 1: pl.ds(0, 1), -1: pl.ds(3, 1)}[dy]
        side = side_out(dz)
        return remote(
            own_moved_rim.at[side, here], moved_rims.at[side, there, me[0]],
            f_send.at[side, 1 + dy], f_recv.at[side, 1 - dy], device(j, dy, dz),
        )

    def cell_copy(j, dy):
        return remote(
            cells.at[1, me[0], body], cells.at[1 - dy, me[0], body],
            b_send.at[1 + dy], b_recv.at[1 - dy], device(j, dy, 0),
        )

    def rim_copy(j, dy, dz):
        side = side_out(dz)
        return remote(
            own_rim.at[side], rims.at[side, 1 - dy, me[0]],
            e_send.at[side, 1 + dy], e_recv.at[side, 1 - dy], device(j, dy, dz),
        )

    def start_all(flat, rim):
        for dy in (-1, 1, 0):

            def act(dy=dy):
                for j in list(range(nx - 1, 0, -1)) + ([0] if dy else []):
                    flat(j, dy).start()
                for j in range(nx - 1, -1, -1):
                    for dz in z_steps:
                        guarded(0, dz, lambda j=j, dz=dz: rim(j, dy, dz).start())

            guarded(dy, 0, act)

    def wait_flat(dy, flat_ref, send, recv, sent):
        count = nx if dy else nx - 1
        ref = flat_ref(dy, count)
        copy = remote(ref, ref, send.at[1 + dy], recv.at[1 + dy], device(1, 0, 0))
        copy.wait_send() if sent else copy.wait_recv()

    def wait_rim(dy, dz, rim_ref, send, recv, sent):
        ref = rim_ref(dy)
        copy = remote(
            ref, ref, send.at[side_out(dz), 1 + dy], recv.at[side_in(dz), 1 + dy], device(1, 0, 0)
        )
        copy.wait_send() if sent else copy.wait_recv()

    def wait_all(flat_ref, rim_ref, sems, sent):
        for dy in (0, -1, 1):

            def act(dy=dy):
                wait_flat(dy, flat_ref, sems[0], sems[1], sent)
                for dz in z_steps:
                    guarded(0, dz, lambda dz=dz: wait_rim(dy, dz, rim_ref, sems[2], sems[3], sent))

            guarded(dy, 0, act)

    def cell_ref(dy, count):
        return cells.at[0, pl.ds(0, count), body]

    def rim_ref(dy):
        return rims.at[0, 0]

    def moved_ref(dy, count):
        return moved.at[pl.ds(0, 1 if dy else 2), pl.ds(0, count), body]

    def moved_rim_ref(dy):
        return moved_rims.at[0, pl.ds(0, 1 if dy else 2)]

    def bin_cell(cell, carry):
        at = pl.multiple_of(cell * 8, 8)
        total = [None, None]
        for i in range(BIN):
            x = cell * BIN + i
            slabs = (ref_ref[x].astype(jnp.float32), def_ref[x].astype(jnp.float32))
            yrows[0, pl.ds(x, 1), :] = slabs[0][:1]
            yrows[1, pl.ds(x, 1), :] = slabs[0][sizey - 1 :]
            total = [s if t is None else t + s for t, s in zip(total, slabs)]
        for image in range(2):
            for y in range(2):
                binned[2 * image + y, pl.ds(at, 8), :] = total[image][8 * y : 8 * y + 8]
        return carry

    def bin_chunk(c):
        for load in images[c]:
            load.wait()
        each = cells_x // chunks
        lax.fori_loop(c * each, (c + 1) * each, bin_cell, 0)

    for c in range(early):
        bin_chunk(c)
    for c in range(early, chunks):
        bin_chunk(c)

    small[1].wait()
    for q in range(4):
        line = binned[q, pl.ds(0, cells_x, stride=8), :]
        for s in range(1, 8):
            line = line + binned[q, pl.ds(s, cells_x, stride=8), :]
        at = pl.multiple_of(lax.rem(turn + q, groups) * cells_x, cells_x)
        for i, part in enumerate(pieces(line, 3)):
            stack[pl.ds(at, cells_x), pl.ds(i * sizez, sizez)] = part
    tile = across_lanes(bin_ref[...], stack[...])
    cells[1, me[0], body] = tile
    own_rim[0] = tile[cells_z - 2 :]
    own_rim[1] = tile[:2]
    pl.semaphore_wait(barrier, expect)
    start_all(moved_copy, moved_rim_copy)
    start_all(cell_copy, rim_copy)

    def x_copy(step):
        side = 0 if step > 0 else 1
        return remote(
            ref_ref.at[pl.ds(sizex - 1 if step > 0 else 0, 1)], xhalo.at[pl.ds(side, 1)],
            x_send.at[side], x_recv.at[side],
            {"gx": me[0] + step, "gy": me[1], "gz": me[2]},
        )

    def y_copy(step):
        side = 1 if step > 0 else 0
        return remote(
            ysend.at[side], yhalo.at[1 - side], y_send.at[side], y_recv.at[1 - side], device(0, step, 0)
        )

    def z_copy(dz):
        i = 0 if dz > 0 else 1
        return remote(ref_ref, zhalo.at[i], z_send.at[i], z_recv.at[i], device(0, 0, dz))

    def at_x(step, act):
        pl.when(me[0] > 0 if step < 0 else me[0] < nx - 1)(act)

    ysend[...] = yrows[...].astype(half)
    for step in (-1, 1):
        guarded(step, 0, lambda step=step: y_copy(step).start())
        at_x(step, lambda step=step: x_copy(step).start())
    for dz in z_steps:
        guarded(0, dz, lambda dz=dz: z_copy(dz).start())

    def prepare(cell, carry):
        start = pl.multiple_of(cell * BIN, BIN)
        first = jnp.maximum(start - 1, 0)
        last = jnp.minimum(start + BIN, sizex - 1)
        slabs = [ref_ref[first].astype(jnp.float32)]
        slabs += [ref_ref[start + i].astype(jnp.float32) for i in range(BIN)]
        slabs += [ref_ref[last].astype(jnp.float32)]
        for i in range(BIN):
            base[start + i] = def_ref[start + i].astype(jnp.float32) - slabs[i + 1]
            grad_x[start + i] = slabs[i + 2] - slabs[i]
        return carry

    lax.fori_loop(0, cells_x, prepare, 0)

    for dz in z_steps:
        guarded(0, dz, lambda dz=dz: z_copy(-dz if nz > 2 else dz).wait_recv())

    row = lax.broadcasted_iota(jnp.int32, (sizez, sizez), 0)
    column = lax.broadcasted_iota(jnp.int32, (sizez, sizez), 1)
    inner = jnp.where(row == column + 1, 1.0, 0.0) - jnp.where(row + 1 == column, 1.0, 0.0)
    from_low = jnp.where(
        jnp.logical_and(jnp.logical_and(row == sizez - 1, column == 0), me[2] > 0), -1.0, 0.0
    )
    from_high = jnp.where(
        jnp.logical_and(jnp.logical_and(row == 0, column == sizez - 1), me[2] < nz - 1), 1.0, 0.0
    )
    outer = [from_low + from_high] if nz == 2 else [from_low, from_high]
    across = jnp.concatenate([inner] + outer, axis=0).astype(half)

    def slope_z(cell, carry):
        start = pl.multiple_of(cell * BIN, BIN)
        sideways = [ref_ref[pl.ds(start, BIN)].reshape(BIN * sizey, sizez)]
        sideways += [zhalo[i, pl.ds(start, BIN)].reshape(BIN * sizey, sizez) for i in range(len(z_steps))]
        slope = jnp.dot(jnp.concatenate(sideways, axis=1), across, preferred_element_type=jnp.float32)
        grad_z[pl.ds(start, BIN)] = slope.reshape(BIN, sizey, sizez)
        return carry

    lax.fori_loop(0, cells_x, slope_z, 0, unroll=8)

    for step in (-1, 1):
        at_x(step, lambda step=step: x_copy(-step).wait_recv())
        guarded(step, 0, lambda step=step: y_copy(-step).wait_recv())
    grad_x[0] = ref_ref[1].astype(jnp.float32) - xhalo[0].astype(jnp.float32)
    grad_x[sizex - 1] = xhalo[1].astype(jnp.float32) - ref_ref[sizex - 2].astype(jnp.float32)
    yrows[...] = yhalo[...].astype(jnp.float32)
    slab_row = lax.broadcasted_iota(jnp.int32, (sizey, sizez), 0)

    def slope_y(cell, carry):
        start = pl.multiple_of(cell * BIN, BIN)
        for i in range(BIN):
            x = start + i
            slab = ref_ref[x].astype(jnp.float32)
            above = jnp.where(slab_row == sizey - 1, yrows[1, pl.ds(x, 1), :], pltpu.roll(slab, sizey - 1, 0))
            below = jnp.where(slab_row == 0, yrows[0, pl.ds(x, 1), :], pltpu.roll(slab, 1, 0))
            grad_y[x] = above - below
        return carry

    lax.fori_loop(0, cells_x, slope_y, 0)

    group = lax.broadcasted_iota(jnp.int32, (deep, 128), 1) // cells_x

    def gather(tiles, q):
        out = []
        for t in range(nx // groups):
            value = tiles[t * groups + (-q) % groups]
            for g in range(1, groups):
                value = jnp.where(group == g, tiles[t * groups + (g - q) % groups], value)
            out.append(pltpu.roll(value, (groups - q) * cells_x, 1) if q else value)
        return out[0] if len(out) == 1 else jnp.concatenate(out, axis=1)

    blank = jnp.zeros((SLOT - deep, across_x), jnp.float32)

    def split_store(target, k, y, value, count):
        padded = jnp.concatenate([value, blank], axis=0)
        for i, part in enumerate(pieces(padded, count)):
            target[pl.ds((4 * k + y) * SLOT, SLOT), pl.ds(i * across_x, across_x)] = part

    for load in small[2:]:
        load.wait()
    wait_all(moved_ref, moved_rim_ref, (d_send, d_recv, f_send, f_recv), False)
    for y in range(4):
        for i in range(nx):
            moved[y, i, pl.ds(cells_z, 1)] = moved_rims[1, y, i]
            moved[y, i, pl.ds(deep - 1, 1)] = moved_rims[0, y, i]
    for y in range(4):
        tiles = [moved[y, i] for i in range(nx)]
        for k in range(3):
            value = gather(tiles, k)
            dline[k, y] = value
            split_store(dsplit, k, y, value, 3)
    new_ref[...] = across_lanes(pick_ref[...], dsplit[...])

    wait_all(cell_ref, rim_ref, (b_send, b_recv, e_send, e_recv), False)
    for dy in range(3):
        for i in range(nx):
            cells[dy, i, pl.ds(cells_z, 2)] = rims[1, dy, i]
            cells[dy, i, pl.ds(deep - 2, 2)] = rims[0, dy, i]
    tiles = [[cells[dy, i] for i in range(nx)] for dy in range(3)]
    coarse = [gather(tiles[dy], q) for dy in range(3) for q in range(2)]
    deformed = [gather(tiles[dy], q) for dy, q in ((0, 3), (1, 2), (1, 3), (2, 2))]
    lane = lax.broadcasted_iota(jnp.int32, (deep, across_x), 1)
    for y in range(4):
        c = coarse[y + 1]
        slopes = [
            (
                jnp.where(lane == across_x - 1, 0.0, pltpu.roll(c, across_x - 1, 1))
                - jnp.where(lane == 0, 0.0, pltpu.roll(c, 1, 1))
            ) * 0.5,
            (coarse[y + 2] - coarse[y]) * 0.5,
            (pltpu.roll(c, deep - 1, 0) - pltpu.roll(c, 1, 0)) * 0.5,
        ]
        mismatch = deformed[y] - c - (
            slopes[0] * dline[0, y] + slopes[1] * dline[1, y] + slopes[2] * dline[2, y]
        )
        for k in range(3):
            split_store(rsplit, k, y, slopes[k] * mismatch, 2)
    step = across_lanes(solve_ref[...], rsplit[...])
    new = new_ref[...] + (step[:rows] + step[rows:])
    new_ref[...] = new
    parts = [
        jnp.concatenate(pieces(new[:, 4 * SLOT * k : 4 * SLOT * (k + 1)], 2), axis=1) for k in range(3)
    ]
    along = jnp.dot(jnp.concatenate(parts, axis=0), prolong_ref[...], preferred_element_type=jnp.float32)
    for k in range(3):
        for s in range(4):
            lines[k, s] = along[rows * k : rows * (k + 1), sizez * s : sizez * (s + 1)]

    wait_all(moved_ref, moved_rim_ref, (d_send, d_recv, f_send, f_recv), True)
    wait_all(cell_ref, rim_ref, (b_send, b_recv, e_send, e_recv), True)
    for step in (-1, 1):
        guarded(step, 0, lambda step=step: y_copy(step).wait_send())
        at_x(step, lambda step=step: x_copy(step).wait_send())
    for dz in z_steps:
        guarded(0, dz, lambda dz=dz: z_copy(dz).wait_send())


def combine(
    chunks,
    new_in, lines, base, grad_x, grad_y, grad_z,
    new_hbm, out_hbm,
    out, turned, new_sem, out_sem,
):
    sizex, sizey, sizez = base.shape
    cells_x = sizex // BIN
    span = sizex // chunks
    keep_new = pltpu.make_async_copy(turned, new_hbm, new_sem.at[0])
    cells_z = sizez // BIN
    before_row = new_in.shape[0] - 1

    third = lax.broadcasted_iota(jnp.int32, (8, sizez), 0).astype(jnp.float32)
    offset_y = (third + 0.5) / 8.0 - 0.5
    weight_low = jnp.maximum(-offset_y, 0.0)
    weight_high = jnp.maximum(offset_y, 0.0)
    weight_mid = 1.0 - jnp.abs(offset_y)

    def plane(at):
        planes = []
        for k in range(3):
            row_of = [lines[k, s, pl.ds(at, 1), :] for s in range(4)]
            planes.append(
                jnp.concatenate(
                    [
                        weight_low * row_of[c] + weight_mid * row_of[c + 1] + weight_high * row_of[c + 2]
                        for c in range(2)
                    ],
                    axis=0,
                )
            )
        return planes

    grads = (grad_x, grad_y, grad_z)

    def residual(cell, carry):
        now, rise = carry
        later = plane(cell + 1)
        climb = [(b - a) * 0.125 for a, b in zip(now, later)]
        start = pl.multiple_of(cell * BIN, BIN)
        for i in range(BIN):
            if i == 0:
                field = [n - 3.5 * r for n, r in zip(now, rise)]
            elif i == BIN // 2:
                field = [n + 0.5 * c for n, c in zip(now, climb)]
            else:
                field = [f + d for f, d in zip(field, rise if i < BIN // 2 else climb)]
            total = base[start + i]
            for grad, f in zip(grads, field):
                total = total - grad[start + i] * f
            out[start + i] = total.astype(jnp.bfloat16)
        return (later, climb)

    def store(c):
        slabs = pl.ds(c * span, span)
        return pltpu.make_async_copy(out.at[slabs], out_hbm.at[slabs], out_sem.at[c])

    before, now = plane(before_row), plane(0)
    state = (now, [(b - a) * 0.125 for a, b in zip(before, now)])
    for c in range(chunks):
        each = cells_x // chunks
        state = lax.fori_loop(c * each, (c + 1) * each, residual, state)
        store(c).start()
        if c == 0:
            for k in range(3):
                flipped = new_in[:cells_x, 4 * SLOT * k : 4 * SLOT * (k + 1)].T
                for y in range(2):
                    turned[k, y] = flipped[SLOT * (y + 1) : SLOT * (y + 1) + cells_z]
            keep_new.start()
    for c in range(chunks):
        store(c).wait()
    keep_new.wait()


def on_device(counts, ref_image, def_image, displacement):
    nx, ny, nz = counts
    sizex, sizey, sizez = ref_image.shape
    cells_x, cells_z = sizex // BIN, sizez // BIN
    rows, deep, across_x = cells_x + 16, cells_z + 8, nx * cells_x
    solve, pick = solve_tables(nx, cells_x, rows)
    binning, prolong = lane_tables(cells_z, sizez, deep, 4)
    sides = 1 if nz == 2 else 2
    dma = pltpu.SemaphoreType.DMA
    vmem, anywhere = pl.BlockSpec(memory_space=pltpu.VMEM), pl.BlockSpec(memory_space=pl.ANY)
    shape = jax.ShapeDtypeStruct
    image = ref_image.shape
    coarse = jnp.transpose(displacement, (0, 2, 3, 1))
    constants = (solve, pick, binning, prolong)
    f32 = jnp.float32
    held = pl.pallas_call(
        functools.partial(exchange, counts, 4, 4),
        out_shape=(
            shape((rows, 12 * SLOT), f32),
            shape((3, 4, rows, sizez), f32),
            shape(image, f32),
            shape(image, f32),
            shape(image, f32),
            shape(image, f32),
        ),
        in_specs=[pl.BlockSpec(memory_space=pltpu.HBM)] * 7,
        out_specs=(vmem,) * 6,
        scratch_shapes=[
            pltpu.VMEM((sides,) + image, half),
            pltpu.VMEM(image, half),
            pltpu.VMEM(image, half),
            pltpu.VMEM(coarse.shape, f32),
            pltpu.VMEM(solve.shape[1:], half),
            pltpu.VMEM(pick.shape[1:], half),
            pltpu.VMEM(binning.shape, half),
            pltpu.VMEM(prolong.shape, half),
            pltpu.VMEM((4, cells_x * 8, sizez), f32),
            pltpu.VMEM((4 * cells_x, 3 * sizez), half),
            pltpu.VMEM((3, nx, deep, 128), f32),
            pltpu.VMEM((2, 3, nx, 2, 128), f32),
            pltpu.VMEM((2, 2, 128), f32),
            pltpu.VMEM((4, nx, deep, 128), f32),
            pltpu.VMEM((2, 4, nx, 1, 128), f32),
            pltpu.VMEM((2, 2, 1, 128), f32),
            pltpu.VMEM((3, 4, deep, across_x), f32),
            pltpu.VMEM((12 * SLOT, 3 * across_x), half),
            pltpu.VMEM((12 * SLOT, 2 * across_x), half),
            pltpu.VMEM((2, sizey, sizez), half),
            pltpu.VMEM((2, sizex, sizez), f32),
            pltpu.VMEM((2, sizex, sizez), half),
            pltpu.VMEM((2, sizex, sizez), half),
            dma((5,)), dma((2, 4)),
            dma((3,)), dma((3,)), dma((2, 3)), dma((2, 3)),
            dma((3,)), dma((3,)), dma((2, 3)), dma((2, 3)),
            dma((2,)), dma((2,)), dma((2,)), dma((2,)), dma((sides,)), dma((sides,)),
        ],
        compiler_params=pltpu.CompilerParams(
            collective_id=0, has_side_effects=True, vmem_limit_bytes=24 << 20
        ),
    )(*[pltpu.with_memory_space_constraint(jnp.asarray(x), pltpu.HBM) for x in (ref_image, def_image, coarse) + constants])
    chunks = 4
    new, residual = pl.pallas_call(
        functools.partial(combine, chunks),
        out_shape=(shape(coarse.shape, f32), shape(image, half)),
        in_specs=[vmem] * 6,
        out_specs=(anywhere, anywhere),
        scratch_shapes=[pltpu.VMEM(image, half), pltpu.VMEM(coarse.shape, f32), dma((1,)), dma((chunks,))],
        compiler_params=pltpu.CompilerParams(vmem_limit_bytes=16 << 20),
    )(*held)
    return jnp.transpose(new, (0, 3, 1, 2)), residual


def solution(mesh):
    counts = tuple(mesh.shape[axis] for axis in ("gx", "gy", "gz"))
    return jax.shard_map(
        functools.partial(on_device, counts),
        mesh=mesh,
        in_specs=(P("gx", "gy", "gz"), P("gx", "gy", "gz"), P(None, "gx", "gy", "gz")),
        out_specs=(P(None, "gx", "gy", "gz"), P("gx", "gy", "gz")),
        check_vma=False,
    )
```

```python
import functools

import jax
import jax.numpy as jnp
import numpy as np
from jax import lax
from jax.experimental import pallas as pl
from jax.experimental.pallas import tpu as pltpu
from jax.sharding import PartitionSpec as P

stiffness = 64.0
BIN = 8
SLOT = 32
MESH = pl.DeviceIdType.MESH
half = jnp.bfloat16


def solve_tables(devices, cells, rows):
    lines = devices * cells
    theta = np.arccosh((1.0 + 2.0 * stiffness) / (2.0 * stiffness))
    index = np.arange(lines)
    low = np.minimum(index[:, None], index[None, :])
    high = np.maximum(index[:, None], index[None, :])
    a, b, c = (low + 1) * theta, (lines - high) * theta, (lines + 1) * theta
    inverse = (
        np.exp(a + b - c) * (1 - np.exp(-2 * a)) * (1 - np.exp(-2 * b)) / (1 - np.exp(-2 * c))
        / (2.0 * stiffness * np.sinh(theta))
    )
    solve = np.zeros((devices, 2 * rows, 2 * lines), np.float32)
    pick = np.zeros((devices, rows, 3 * lines), np.float32)
    for me in range(devices):
        first = me * cells
        for row, x in [(r, first + r) for r in range(cells + 1)] + [(rows - 1, first - 1)]:
            if x < 0 or x >= lines:
                continue
            top = inverse[x].astype(half).astype(np.float64)
            solve[me, row, :lines] = top
            solve[me, row, lines:] = top
            solve[me, rows + row, :lines] = inverse[x] - top
            pick[me, row, x::lines] = 1.0
    return solve.astype(half), pick.astype(half)


def lane_tables(cells_z, size_z, deep, slots):
    binning = np.repeat(np.eye(cells_z, dtype=np.float32), BIN, axis=1) / 32.0
    prolong = np.zeros((slots * SLOT, slots * size_z), np.float32)
    for slot in range(slots):
        for fine in range(size_z):
            cell, offset = fine // BIN, (fine % BIN + 0.5) / BIN - 0.5
            other = (cell + (1 if offset >= 0 else -1)) % deep
            prolong[slot * SLOT + cell, slot * size_z + fine] = 0.5 * (1.0 - abs(offset))
            prolong[slot * SLOT + other, slot * size_z + fine] = 0.5 * abs(offset)
    return np.tile(binning, (1, 3)).astype(half), np.tile(prolong, (2, 1)).astype(half)


def pieces(value, count):
    parts = []
    for i in range(count):
        part = value.astype(half)
        parts.append(part)
        if i < count - 1:
            value = value - part.astype(jnp.float32)
    return parts


def across_lanes(a, b):
    return lax.dot_general(a, b, (((1,), (1,)), ((), ())), preferred_element_type=jnp.float32)


def exchange(
    counts, chunks, parts_of,
    ref_hbm, def_hbm, disp_hbm, table_hbm,
    new_ref, lines, base, grad_x, grad_y, grad_z,
    zhalo, image_ref, disp_ref, table_ref,
    binned, stack, mail, rims, own_rim, foot, dline, cline, fline, dsplit, rsplit,
    xhalo, yrows, ysend, yhalo,
    load_sem, image_sem, mail_send, mail_recv, y_recv, z_recv,
):
    nx, ny, nz = counts
    ref_ref, def_ref = image_ref.at[0], image_ref.at[1]
    sizex, sizey, sizez = def_ref.shape
    cells_x, cells_z = sizex // BIN, sizez // BIN
    groups = 128 // cells_x
    across_x = nx * cells_x
    deep = dline.shape[2]
    rows = new_ref.shape[0]
    me = (lax.axis_index("gx"), lax.axis_index("gy"), lax.axis_index("gz"))
    turn = lax.rem(me[0], groups)

    def device(j, dy, dz):
        gz = me[2] + dz if nz > 2 or dz == 0 else 1 - me[2]
        return {"gx": lax.rem(me[0] + j, nx), "gy": me[1] + dy, "gz": gz}

    def guarded(dy, dz, act):
        tests = []
        for at, step, count in ((me[1], dy, ny), (me[2], dz if nz > 2 else 0, nz)):
            if step:
                tests.append(at > 0 if step < 0 else at < count - 1)
        if tests:
            pl.when(functools.reduce(jnp.logical_and, tests))(act)
        else:
            act()

    z_steps = (1,) if nz == 2 else (1, -1)

    def side_out(dz):
        return me[2] if nz == 2 else (0 if dz > 0 else 1)

    def lane_of(dz):
        return 0 if nz == 2 or dz == 0 else (1 if dz > 0 else 2)

    barrier = pltpu.get_barrier_semaphore()
    for dy in (-1, 1, 0):

        def greet(dy=dy):
            for j in range(nx - 1, -1, -1):
                for dz in (0,) + z_steps:
                    if (j, dy, dz) != (0, 0, 0):

                        def hail(j=j, dz=dz):
                            pl.semaphore_signal(barrier, inc=1, device_id=device(j, dy, dz), device_id_type=MESH)

                        guarded(0, dz, hail)

        guarded(dy, 0, greet)

    sections = {}
    for name, (row, height, width) in parts_of.items():
        sections[name] = table_ref.at[pl.ds(row, height), pl.ds(0, width)]
    load_disp = pltpu.make_async_copy(disp_hbm, disp_ref, load_sem.at[0])
    load_table = pltpu.make_async_copy(table_hbm.at[me[0]], table_ref, load_sem.at[1])
    span = sizex // chunks
    for c in range(chunks):
        for i, hbm in enumerate((ref_hbm, def_hbm)):
            pltpu.make_async_copy(
                hbm.at[pl.ds(c * span, span)], image_ref.at[i, pl.ds(c * span, span)], image_sem.at[c]
            ).start()
    load_disp.start()
    load_table.start()

    def clear(test, *parts):
        @pl.when(test)
        def _():
            for part in parts:
                part[...] = jnp.zeros(part.shape, part.dtype)

    low_y, high_y = me[1] == 0, me[1] == ny - 1
    low_z, high_z = me[2] == 0, me[2] == nz - 1
    clear(low_y, yhalo.at[0], mail.at[0], rims.at[:, 0])
    clear(high_y, yhalo.at[1], mail.at[2], rims.at[:, 2])
    clear(low_z, rims.at[0])
    clear(high_z, rims.at[1])
    if nz > 2:
        clear(low_z, zhalo.at[0])
        clear(high_z, zhalo.at[1])
    foot[...] = jnp.zeros(foot.shape, jnp.float32)

    reach = [
        1 + (at > 0).astype(jnp.int32) + (at < count - 1).astype(jnp.int32)
        for at, count in zip(me, counts)
    ]
    expect = nx * reach[1] * (2 if nz == 2 else reach[2]) - 1

    def remote(src, dst, send, recv, to):
        return pltpu.make_async_remote_copy(
            src_ref=src, dst_ref=dst, send_sem=send, recv_sem=recv, device_id=to, device_id_type=MESH
        )

    body = pl.ds(0, cells_z)
    quarter = cells_z // 2
    part_rows = {0: (0, 5 * quarter), 1: (0, 3 * quarter), -1: (2 * quarter, 3 * quarter)}
    part_rims = {0: (0, 4), 1: (0, 3), -1: (1, 3)}

    def mail_copy(j, dy):
        where = pl.ds(*part_rows[dy])
        return remote(
            mail.at[1, me[0], where], mail.at[1 - dy, me[0], where],
            mail_send.at[1 + dy, 0], mail_recv.at[1 - dy, 0], device(j, dy, 0),
        )

    def rim_copy(j, dy, dz):
        side, where = side_out(dz), pl.ds(*part_rims[dy])
        return remote(
            own_rim.at[side, where], rims.at[side, 1 - dy, me[0], where],
            mail_send.at[1 + dy, lane_of(dz)], mail_recv.at[1 - dy, lane_of(dz)], device(j, dy, dz),
        )

    unit = 128 * 4
    plane_bytes = {"x": 2 * sizey * sizez, "y": 2 * sizex * sizez, "z": 2 * sizex * sizey * sizez}

    def settle(dy, sent):
        def one(dz_of, bytes_of):
            lane = lane_of(dz_of if sent else -dz_of)
            ref = grad_y.at[pl.ds(0, bytes_of // unit)]
            copy = remote(ref, ref, mail_send.at[1 + dy, lane], mail_recv.at[1 + dy, lane], device(1, 0, 0))
            copy.wait_send() if sent else copy.wait_recv()

        flat = (nx if dy else nx - 1) * part_rows[dy][1] * unit
        rim = nx * part_rims[dy][1] * unit
        if dy == 0:
            flat += 2 * plane_bytes["x"]
            rim += plane_bytes["z"] if sent else 0
        elif sent:
            flat += plane_bytes["y"]
        if nz == 2:
            guarded(dy, 0, lambda: one(0, flat + rim))
        else:

            def act():
                one(0, flat)
                for dz in z_steps:
                    guarded(0, dz, lambda dz=dz: one(dz, rim))

            guarded(dy, 0, act)

    def bin_cell(cell, carry):
        at = pl.multiple_of(cell * 8, 8)
        total = [None, None]
        for i in range(BIN):
            x = cell * BIN + i
            slabs = (ref_ref[x].astype(jnp.float32), def_ref[x].astype(jnp.float32))
            yrows[0, pl.ds(x, 1), :] = slabs[0][:1]
            yrows[1, pl.ds(x, 1), :] = slabs[0][sizey - 1 :]
            total = [s if t is None else t + s for t, s in zip(total, slabs)]
        for image in range(2):
            for y in range(2):
                binned[2 * image + y, pl.ds(at, 8), :] = total[image][8 * y : 8 * y + 8]
        return carry

    def bin_chunk(c):
        both = image_ref.at[:, pl.ds(c * span, span)]
        pltpu.make_async_copy(both, both, image_sem.at[c]).wait()
        each = cells_x // chunks
        lax.fori_loop(c * each, (c + 1) * each, bin_cell, 0)

    for c in range(chunks):
        bin_chunk(c)

    load_table.wait()
    for q, spots in enumerate(((0, 1), (2, 3), (4, 6), (5, 7))):
        line = binned[q, pl.ds(0, cells_x, stride=8), :]
        for s in range(1, 8):
            line = line + binned[q, pl.ds(s, cells_x, stride=8), :]
        for i, part in enumerate(pieces(line, 3)):
            for spot in spots:
                at = (lax.rem(turn + spot, groups) + spot // groups * groups) * cells_x
                stack[pl.ds(pl.multiple_of(at, cells_x), cells_x), pl.ds(i * sizez, sizez)] = part
    sums = across_lanes(sections["bin"][...], stack[...])
    load_disp.wait()
    lane = lax.broadcasted_iota(jnp.int32, (cells_z, 128), 1)
    held = lax.rem(lane // cells_x + groups - turn, groups)
    empty = jnp.zeros((cells_z, cells_x), jnp.float32)

    def turned_tile(row):
        return pltpu.roll(jnp.concatenate(row, axis=1), turn * cells_x, 1)

    upper = turned_tile([disp_ref[0, 1], disp_ref[1, 1], disp_ref[2, 1], empty])
    lower = turned_tile([disp_ref[1, 0], disp_ref[2, 0], empty, disp_ref[0, 0]])
    upper = jnp.where(held == 3, sums[:, 128:], upper)
    lower = jnp.where(held == 2, sums[:, 128:], lower)
    middle = jnp.where(held[:quarter] % 2 == 0, sums[:quarter, :128], sums[quarter:, :128])
    mail[1, me[0], pl.ds(0, cells_z)] = upper
    mail[1, me[0], pl.ds(cells_z, quarter)] = middle
    mail[1, me[0], pl.ds(cells_z + quarter, cells_z)] = lower
    for side, rows_out in (
        (0, (upper[cells_z - 1 :], middle[quarter - 2 : quarter - 1], middle[quarter - 1 :], lower[cells_z - 1 :])),
        (1, (upper[:1], middle[:1], middle[1:2], lower[:1])),
    ):
        for i, row_out in enumerate(rows_out):
            own_rim[side, i] = row_out
    pl.semaphore_wait(barrier, expect)
    for dy in (-1, 1, 0):

        def act(dy=dy):
            for j in list(range(nx - 1, 0, -1)) + ([0] if dy else []):
                mail_copy(j, dy).start()
            for j in range(nx - 1, -1, -1):
                for dz in z_steps:
                    guarded(0, dz, lambda j=j, dz=dz: rim_copy(j, dy, dz).start())

        guarded(dy, 0, act)

    def x_copy(step):
        side = 0 if step > 0 else 1
        return remote(
            ref_ref.at[pl.ds(sizex - 1 if step > 0 else 0, 1)], xhalo.at[pl.ds(side, 1)],
            mail_send.at[1, 0], mail_recv.at[1, 0], device(1 if step > 0 else nx - 1, 0, 0),
        )

    def y_copy(step):
        side = 1 if step > 0 else 0
        return remote(
            ysend.at[side], yhalo.at[1 - side], mail_send.at[1 + step, 0], y_recv.at[1 - side], device(0, step, 0)
        )

    def z_copy(dz):
        i = 0 if dz > 0 else 1
        return remote(ref_ref, zhalo.at[i], mail_send.at[1, lane_of(dz)], z_recv.at[i], device(0, 0, dz))

    ysend[...] = yrows[...].astype(half)
    for step in (-1, 1):
        guarded(step, 0, lambda step=step: y_copy(step).start())
        x_copy(step).start()
    for dz in z_steps:
        guarded(0, dz, lambda dz=dz: z_copy(dz).start())

    def prepare(cell, carry):
        start = pl.multiple_of(cell * BIN, BIN)
        first = jnp.maximum(start - 1, 0)
        last = jnp.minimum(start + BIN, sizex - 1)
        slabs = [ref_ref[first].astype(jnp.float32)]
        slabs += [ref_ref[start + i].astype(jnp.float32) for i in range(BIN)]
        slabs += [ref_ref[last].astype(jnp.float32)]
        for i in range(BIN):
            base[start + i] = def_ref[start + i].astype(jnp.float32) - slabs[i + 1]
            grad_x[start + i] = slabs[i + 2] - slabs[i]
        return carry

    lax.fori_loop(0, cells_x, prepare, 0)

    slab_row = lax.broadcasted_iota(jnp.int32, (sizey, sizez), 0)

    def slope_y(cell, carry):
        start = pl.multiple_of(cell * BIN, BIN)
        for i in range(BIN):
            slab = ref_ref[start + i].astype(jnp.float32)
            above = jnp.where(slab_row == sizey - 1, 0.0, pltpu.roll(slab, sizey - 1, 0))
            below = jnp.where(slab_row == 0, 0.0, pltpu.roll(slab, 1, 0))
            grad_y[pl.ds(pl.multiple_of((start + i) * sizey, sizey), sizey)] = above - below
        return carry

    lax.fori_loop(0, cells_x, slope_y, 0, unroll=2)

    for dz in z_steps:
        guarded(0, dz, lambda dz=dz: z_copy(-dz if nz > 2 else dz).wait_recv())

    row = lax.broadcasted_iota(jnp.int32, (sizez, sizez), 0)
    column = lax.broadcasted_iota(jnp.int32, (sizez, sizez), 1)
    inner = jnp.where(row == column + 1, 1.0, 0.0) - jnp.where(row + 1 == column, 1.0, 0.0)
    from_low = jnp.where(
        jnp.logical_and(jnp.logical_and(row == sizez - 1, column == 0), me[2] > 0), -1.0, 0.0
    )
    from_high = jnp.where(
        jnp.logical_and(jnp.logical_and(row == 0, column == sizez - 1), me[2] < nz - 1), 1.0, 0.0
    )
    outer = [from_low + from_high] if nz == 2 else [from_low, from_high]
    across = jnp.concatenate([inner] + outer, axis=0).astype(half)

    def slope_z(cell, carry):
        start = pl.multiple_of(cell * BIN, BIN)
        sideways = [ref_ref[pl.ds(start, BIN)].reshape(BIN * sizey, sizez)]
        sideways += [zhalo[i, pl.ds(start, BIN)].reshape(BIN * sizey, sizez) for i in range(len(z_steps))]
        slope = jnp.dot(jnp.concatenate(sideways, axis=1), across, preferred_element_type=jnp.float32)
        grad_z[pl.ds(start, BIN)] = slope.reshape(BIN, sizey, sizez)
        return carry

    lax.fori_loop(0, cells_x, slope_z, 0, unroll=8)

    def gather(tiles, q):
        height = tiles[0].shape[0]
        group = lax.broadcasted_iota(jnp.int32, (height, 128), 1) // cells_x
        out = []
        for t in range(nx // groups):
            value = tiles[t * groups + (-q) % groups]
            for g in range(1, groups):
                value = jnp.where(group == g, tiles[t * groups + (g - q) % groups], value)
            out.append(pltpu.roll(value, (groups - q) * cells_x, 1) if q else value)
        return out[0] if len(out) == 1 else jnp.concatenate(out, axis=1)

    blank = jnp.zeros((SLOT - deep, across_x), jnp.float32)

    def split_store(target, k, y, value, count):
        padded = jnp.concatenate([value, blank], axis=0)
        for i, part in enumerate(pieces(padded, count)):
            target[pl.ds((4 * k + y) * SLOT, SLOT), pl.ds(i * across_x, across_x)] = part

    bottom = deep - cells_z
    foot_row = lax.broadcasted_iota(jnp.int32, (bottom, across_x), 0)

    def unpack(slot):
        for i in range(nx):
            if slot < 2:
                foot[slot, i, 0, pl.ds(0, 1)] = rims[1, slot, i, 0]
                foot[slot, i, 0, pl.ds(bottom - 1, 1)] = rims[0, slot, i, 0]
            for r in range(2):
                foot[slot, i, 1, pl.ds(r, 1)] = rims[1, slot, i, 1 + r]
                foot[slot, i, 1, pl.ds(bottom - 2 + r, 1)] = rims[0, slot, i, 1 + r]
            if slot > 0:
                foot[slot, i, 2, pl.ds(0, 1)] = rims[1, slot, i, 3]
                foot[slot, i, 2, pl.ds(bottom - 1, 1)] = rims[0, slot, i, 3]
        halves = [mail[slot, i, pl.ds(cells_z, quarter)] for i in range(nx)]
        feet = [foot[slot, i, 1] for i in range(nx)]
        for y in range(2):
            cline[2 * slot + y] = jnp.concatenate(
                [
                    gather(halves, 2 * y), gather(halves, 2 * y + 1),
                    jnp.where(foot_row < bottom // 2, gather(feet, 2 * y), gather(feet, 2 * y + 1)),
                ],
                axis=0,
            )
        for y, first, which, order in ((1, 0, 0, (0, 1, 2, 3)), (0, 3 * quarter, 2, (3, 0, 1, 2))):
            line = {(0, 1): 0, (1, 0): 1, (1, 1): 2, (2, 0): 3}.get((slot, y))
            if line is None:
                continue
            tiles = [
                jnp.concatenate([mail[slot, i, pl.ds(first, cells_z)], foot[slot, i, which]], axis=0)
                for i in range(nx)
            ]
            for k in range(3):
                value = gather(tiles, order[k])
                dline[k, line] = value
                split_store(dsplit, k, line, value, 3)
            fline[line] = gather(tiles, order[3])

    settle(0, False)
    grad_x[0] = ref_ref[1].astype(jnp.float32) - jnp.where(me[0] > 0, xhalo[0].astype(jnp.float32), 0.0)
    grad_x[sizex - 1] = (
        jnp.where(me[0] < nx - 1, xhalo[1].astype(jnp.float32), 0.0) - ref_ref[sizex - 2].astype(jnp.float32)
    )
    unpack(1)
    settle(-1, False)
    settle(1, False)
    unpack(0)
    unpack(2)
    kept = across_lanes(sections["pick"][...], dsplit[...])
    lane = lax.broadcasted_iota(jnp.int32, (deep, across_x), 1)
    for y in range(4):
        c = cline[y + 1]
        slopes = [
            (
                jnp.where(lane == across_x - 1, 0.0, pltpu.roll(c, across_x - 1, 1))
                - jnp.where(lane == 0, 0.0, pltpu.roll(c, 1, 1))
            ) * 0.5,
            (cline[y + 2] - cline[y]) * 0.5,
            (pltpu.roll(c, deep - 1, 0) - pltpu.roll(c, 1, 0)) * 0.5,
        ]
        mismatch = fline[y] - c - (
            slopes[0] * dline[0, y] + slopes[1] * dline[1, y] + slopes[2] * dline[2, y]
        )
        for k in range(3):
            split_store(rsplit, k, y, slopes[k] * mismatch, 2)
    step = across_lanes(sections["solve"][...], rsplit[...])
    new = kept + (step[:rows] + step[rows:])
    new_ref[...] = new
    parts = [
        jnp.concatenate(pieces(new[:, 4 * SLOT * k : 4 * SLOT * (k + 1)], 2), axis=1) for k in range(3)
    ]
    along = jnp.dot(jnp.concatenate(parts, axis=0), sections["prolong"][...], preferred_element_type=jnp.float32)
    for k in range(3):
        for s in range(4):
            lines[k, s] = along[rows * k : rows * (k + 1), sizez * s : sizez * (s + 1)]

    for step in (-1, 1):
        guarded(step, 0, lambda step=step: y_copy(-step).wait_recv())
    for at, side in ((0, 0), (sizey - 1, 1)):
        edge = pl.ds(at, sizex, stride=sizey)
        plane = yhalo[side].astype(jnp.float32)
        grad_y[edge, :] = grad_y[edge, :] + plane if side else grad_y[edge, :] - plane
    for dy in (0, -1, 1):
        settle(dy, True)


def combine(
    chunks,
    new_in, lines, base, grad_x, grad_y, grad_z,
    new_hbm, out_hbm,
    out, turned, new_sem, out_sem,
):
    sizex, sizey, sizez = base.shape
    cells_x = sizex // BIN
    span = sizex // chunks
    keep_new = pltpu.make_async_copy(turned, new_hbm, new_sem.at[0])
    cells_z = sizez // BIN
    before_row = new_in.shape[0] - 1

    third = lax.broadcasted_iota(jnp.int32, (8, sizez), 0).astype(jnp.float32)
    offset_y = (third + 0.5) / 8.0 - 0.5
    weight_low = jnp.maximum(-offset_y, 0.0)
    weight_high = jnp.maximum(offset_y, 0.0)
    weight_mid = 1.0 - jnp.abs(offset_y)

    def plane(at):
        planes = []
        for k in range(3):
            row_of = [lines[k, s, pl.ds(at, 1), :] for s in range(4)]
            planes.append(
                jnp.concatenate(
                    [
                        weight_low * row_of[c] + weight_mid * row_of[c + 1] + weight_high * row_of[c + 2]
                        for c in range(2)
                    ],
                    axis=0,
                )
            )
        return planes

    def residual(cell, carry):
        now, rise = carry
        later = plane(cell + 1)
        climb = [(b - a) * 0.125 for a, b in zip(now, later)]
        start = pl.multiple_of(cell * BIN, BIN)
        for i in range(BIN):
            if i == 0:
                field = [n - 3.5 * r for n, r in zip(now, rise)]
            elif i == BIN // 2:
                field = [n + 0.5 * c for n, c in zip(now, climb)]
            else:
                field = [f + d for f, d in zip(field, rise if i < BIN // 2 else climb)]
            total = base[start + i]
            at_y = pl.ds(pl.multiple_of((start + i) * sizey, sizey), sizey)
            total = total - grad_x[start + i] * field[0]
            total = total - grad_y[at_y] * field[1]
            total = total - grad_z[start + i] * field[2]
            out[start + i] = total.astype(jnp.bfloat16)
        return (later, climb)

    def store(c):
        slabs = pl.ds(c * span, span)
        return pltpu.make_async_copy(out.at[slabs], out_hbm.at[slabs], out_sem.at[c])

    before, now = plane(before_row), plane(0)
    state = (now, [(b - a) * 0.125 for a, b in zip(before, now)])
    for c in range(chunks):
        each = cells_x // chunks
        state = lax.fori_loop(c * each, (c + 1) * each, residual, state)
        store(c).start()
        if c == 0:
            for k in range(3):
                flipped = new_in[:cells_x, 4 * SLOT * k : 4 * SLOT * (k + 1)].T
                for y in range(2):
                    turned[k, y] = flipped[SLOT * (y + 1) : SLOT * (y + 1) + cells_z]
            keep_new.start()
    for c in range(chunks):
        store(c).wait()
    keep_new.wait()


def on_device(counts, ref_image, def_image, displacement):
    nx, ny, nz = counts
    sizex, sizey, sizez = ref_image.shape
    cells_x, cells_z = sizex // BIN, sizez // BIN
    rows, deep, across_x = cells_x + 16, cells_z + 8, nx * cells_x
    solve, pick = solve_tables(nx, cells_x, rows)
    binning, prolong = lane_tables(cells_z, sizez, deep, 4)
    parts_of, at = {}, 0
    for name, part in (("prolong", prolong), ("solve", solve), ("pick", pick), ("bin", binning)):
        parts_of[name] = (at, part.shape[-2], part.shape[-1])
        at += part.shape[-2]
    table = np.zeros((nx, at, max(width for _, _, width in parts_of.values())), half)
    for name, part in (("prolong", prolong), ("solve", solve), ("pick", pick), ("bin", binning)):
        row, height, width = parts_of[name]
        table[:, row : row + height, :width] = part
    lanes = 1 if nz == 2 else 3
    sides = 1 if nz == 2 else 2
    dma = pltpu.SemaphoreType.DMA
    vmem, anywhere = pl.BlockSpec(memory_space=pltpu.VMEM), pl.BlockSpec(memory_space=pl.ANY)
    shape = jax.ShapeDtypeStruct
    image = ref_image.shape
    coarse = jnp.transpose(displacement, (0, 2, 3, 1))
    constants = (table,)
    f32 = jnp.float32
    held = pl.pallas_call(
        functools.partial(exchange, counts, 4, parts_of),
        out_shape=(
            shape((rows, 12 * SLOT), f32),
            shape((3, 4, rows, sizez), f32),
            shape(image, f32),
            shape(image, f32),
            shape((sizex * sizey, sizez), f32),
            shape(image, f32),
        ),
        in_specs=[pl.BlockSpec(memory_space=pltpu.HBM)] * 4,
        out_specs=(vmem,) * 6,
        scratch_shapes=[
            pltpu.VMEM((sides,) + image, half),
            pltpu.VMEM((2,) + image, half),
            pltpu.VMEM(coarse.shape, f32),
            pltpu.VMEM(table.shape[1:], half),
            pltpu.VMEM((4, cells_x * 8, sizez), f32),
            pltpu.VMEM((8 * cells_x, 3 * sizez), half),
            pltpu.VMEM((3, nx, 5 * cells_z // 2, 128), f32),
            pltpu.VMEM((2, 3, nx, 4, 1, 128), f32),
            pltpu.VMEM((2, 4, 1, 128), f32),
            pltpu.VMEM((3, nx, 3, deep - cells_z, 128), f32),
            pltpu.VMEM((3, 4, deep, across_x), f32),
            pltpu.VMEM((6, deep, across_x), f32),
            pltpu.VMEM((4, deep, across_x), f32),
            pltpu.VMEM((12 * SLOT, 3 * across_x), half),
            pltpu.VMEM((12 * SLOT, 2 * across_x), half),
            pltpu.VMEM((2, sizey, sizez), half),
            pltpu.VMEM((2, sizex, sizez), f32),
            pltpu.VMEM((2, sizex, sizez), half),
            pltpu.VMEM((2, sizex, sizez), half),
            dma((2,)), dma((4,)), dma((3, lanes)), dma((3, lanes)), dma((2,)), dma((sides,)),
        ],
        compiler_params=pltpu.CompilerParams(
            collective_id=0, has_side_effects=True, vmem_limit_bytes=24 << 20
        ),
    )(*[pltpu.with_memory_space_constraint(jnp.asarray(x), pltpu.HBM) for x in (ref_image, def_image, coarse) + constants])
    chunks = 4
    new, residual = pl.pallas_call(
        functools.partial(combine, chunks),
        out_shape=(shape(coarse.shape, f32), shape(image, half)),
        in_specs=[vmem] * 6,
        out_specs=(anywhere, anywhere),
        scratch_shapes=[pltpu.VMEM(image, half), pltpu.VMEM(coarse.shape, f32), dma((1,)), dma((chunks,))],
        compiler_params=pltpu.CompilerParams(vmem_limit_bytes=16 << 20),
    )(*held)
    return jnp.transpose(new, (0, 3, 1, 2)), residual


def solution(mesh):
    counts = tuple(mesh.shape[axis] for axis in ("gx", "gy", "gz"))
    return jax.shard_map(
        functools.partial(on_device, counts),
        mesh=mesh,
        in_specs=(P("gx", "gy", "gz"), P("gx", "gy", "gz"), P(None, "gx", "gy", "gz")),
        out_specs=(P(None, "gx", "gy", "gz"), P("gx", "gy", "gz")),
        check_vma=False,
    )
```

```python
import functools

import jax
import jax.numpy as jnp
import numpy as np
from jax import lax
from jax.experimental import pallas as pl
from jax.experimental.pallas import tpu as pltpu
from jax.sharding import PartitionSpec as P

stiffness = 64.0
BIN = 8
SLOT = 32
PITCH = 24
MESH = pl.DeviceIdType.MESH
half = jnp.bfloat16


def solve_tables(devices, cells, rows):
    lines = devices * cells
    theta = np.arccosh((1.0 + 2.0 * stiffness) / (2.0 * stiffness))
    index = np.arange(lines)
    low = np.minimum(index[:, None], index[None, :])
    high = np.maximum(index[:, None], index[None, :])
    a, b, c = (low + 1) * theta, (lines - high) * theta, (lines + 1) * theta
    inverse = (
        np.exp(a + b - c) * (1 - np.exp(-2 * a)) * (1 - np.exp(-2 * b)) / (1 - np.exp(-2 * c))
        / (2.0 * stiffness * np.sinh(theta))
    )
    solve = np.zeros((devices, 2 * rows, 2 * lines), np.float32)
    for me in range(devices):
        first = me * cells
        for row, x in [(r, first + r) for r in range(cells + 1)] + [(rows - 1, first - 1)]:
            if x < 0 or x >= lines:
                continue
            top = inverse[x].astype(half).astype(np.float64)
            solve[me, row, :lines] = top
            solve[me, row, lines:] = top
            solve[me, rows + row, :lines] = inverse[x] - top
    return solve.astype(half)


def lane_tables(cells_z, size_z, deep, slots):
    binning = np.repeat(np.eye(cells_z, dtype=np.float32), BIN, axis=1) / 32.0
    prolong = np.zeros((slots * SLOT, slots * size_z), np.float32)
    for slot in range(slots):
        for fine in range(size_z):
            cell, offset = fine // BIN, (fine % BIN + 0.5) / BIN - 0.5
            other = (cell + (1 if offset >= 0 else -1)) % deep
            prolong[slot * SLOT + cell, slot * size_z + fine] = 0.5 * (1.0 - abs(offset))
            prolong[slot * SLOT + other, slot * size_z + fine] = 0.5 * abs(offset)
    return np.tile(binning, (1, 3)).astype(half), np.tile(prolong, (2, 1)).astype(half)


def pieces(value, count):
    parts = []
    for i in range(count):
        part = value.astype(half)
        parts.append(part)
        if i < count - 1:
            value = value - part.astype(jnp.float32)
    return parts


def across_lanes(a, b):
    return lax.dot_general(a, b, (((1,), (1,)), ((), ())), preferred_element_type=jnp.float32)


def exchange(
    counts, chunks, parts_of,
    ref_hbm, def_hbm, disp_hbm, table_hbm,
    new_ref, lines, base, grad_x, grad_y, grad_z,
    zhalo, image_ref, disp_ref, table_ref,
    binned, stack, mail, rims, own_rim, foot, dline, cline, fline, kept, rsplit,
    xhalo, yrows, ysend, yhalo,
    load_sem, image_sem, mail_send, mail_recv, y_recv, z_recv,
):
    nx, ny, nz = counts
    ref_ref, def_ref = image_ref.at[0], image_ref.at[1]
    sizex, sizey, sizez = def_ref.shape
    cells_x, cells_z = sizex // BIN, sizez // BIN
    groups = 128 // cells_x
    across_x = nx * cells_x
    deep = dline.shape[2]
    rows = new_ref.shape[0]
    me = (lax.axis_index("gx"), lax.axis_index("gy"), lax.axis_index("gz"))
    turn = lax.rem(me[0], groups)

    def device(j, dy, dz, mirrored=False):
        gz = me[2] + dz if nz > 2 or dz == 0 else 1 - me[2]
        gx = lax.rem(2 * nx - 1 - me[0] - j, nx) if mirrored else lax.rem(me[0] + j, nx)
        return {"gx": gx, "gy": me[1] + dy, "gz": gz}

    def guarded(dy, dz, act):
        tests = []
        for at, step, count in ((me[1], dy, ny), (me[2], dz if nz > 2 else 0, nz)):
            if step:
                tests.append(at > 0 if step < 0 else at < count - 1)
        if tests:
            pl.when(functools.reduce(jnp.logical_and, tests))(act)
        else:
            act()

    z_steps = (1,) if nz == 2 else (1, -1)

    def side_out(dz):
        return me[2] if nz == 2 else (0 if dz > 0 else 1)

    def lane_of(dz):
        return 0 if nz == 2 or dz == 0 else (1 if dz > 0 else 2)

    sections = {}
    for name, (row, height, width) in parts_of.items():
        sections[name] = table_ref.at[pl.ds(row, height), pl.ds(0, width)]
    load_disp = pltpu.make_async_copy(disp_hbm, disp_ref, load_sem.at[0])
    load_table = pltpu.make_async_copy(table_hbm.at[me[0]], table_ref, load_sem.at[1])
    span = sizex // chunks
    for c in range(chunks):
        for i, hbm in enumerate((ref_hbm, def_hbm)):
            pltpu.make_async_copy(
                hbm.at[pl.ds(c * span, span)], image_ref.at[i, pl.ds(c * span, span)], image_sem.at[c]
            ).start()
    barrier = pltpu.get_barrier_semaphore()
    for dy in (-1, 1, 0):

        def greet(dy=dy):
            for j in range(nx):
                for dz in (0,) + z_steps:
                    if (j, dy, dz) != (0, 0, 0):

                        def hail(j=j, dz=dz):
                            pl.semaphore_signal(barrier, inc=1, device_id=device(j, dy, dz, dy != 0), device_id_type=MESH)

                        guarded(0, dz, hail)

        guarded(dy, 0, greet)

    load_disp.start()
    load_table.start()

    def clear(test, *parts):
        @pl.when(test)
        def _():
            for part in parts:
                part[...] = jnp.zeros(part.shape, part.dtype)

    low_y, high_y = me[1] == 0, me[1] == ny - 1
    low_z, high_z = me[2] == 0, me[2] == nz - 1
    clear(low_y, yhalo.at[0], mail.at[0], rims.at[:, 0])
    clear(high_y, yhalo.at[1], mail.at[2], rims.at[:, 2])
    clear(low_z, rims.at[0])
    clear(high_z, rims.at[1])
    if nz > 2:
        clear(low_z, zhalo.at[0])
        clear(high_z, zhalo.at[1])
    foot[...] = jnp.zeros(foot.shape, jnp.float32)
    kept[...] = jnp.zeros(kept.shape, jnp.float32)

    reach = [
        1 + (at > 0).astype(jnp.int32) + (at < count - 1).astype(jnp.int32)
        for at, count in zip(me, counts)
    ]
    expect = nx * reach[1] * (2 if nz == 2 else reach[2]) - 1

    def remote(src, dst, send, recv, to):
        return pltpu.make_async_remote_copy(
            src_ref=src, dst_ref=dst, send_sem=send, recv_sem=recv, device_id=to, device_id_type=MESH
        )

    body = pl.ds(0, cells_z)
    quarter = cells_z // 2
    part_rows = {0: (0, 5 * quarter), 1: (0, 3 * quarter), -1: (2 * quarter, 3 * quarter)}
    part_rims = {0: (0, 4), 1: (0, 3), -1: (1, 3)}

    def mail_copy(j, dy):
        where = pl.ds(*part_rows[dy])
        return remote(
            mail.at[1, me[0], where], mail.at[1 - dy, me[0], where],
            mail_send.at[1 + dy, 0], mail_recv.at[1 - dy, 0], device(j, dy, 0, dy != 0),
        )

    def rim_copy(j, dy, dz):
        side, where = side_out(dz), pl.ds(*part_rims[dy])
        return remote(
            own_rim.at[side, where], rims.at[side, 1 - dy, me[0], where],
            mail_send.at[1 + dy, lane_of(dz)], mail_recv.at[1 - dy, lane_of(dz)], device(j, dy, dz, dy != 0),
        )

    unit = 128 * 4
    plane_bytes = {"x": 2 * sizey * sizez, "y": 2 * sizex * sizez, "z": 2 * sizex * sizey * sizez}

    def settle(dy, sent):
        def one(dz_of, bytes_of):
            lane = lane_of(dz_of if sent else -dz_of)
            ref = grad_y.at[pl.ds(0, bytes_of // unit)]
            copy = remote(ref, ref, mail_send.at[1 + dy, lane], mail_recv.at[1 + dy, lane], device(1, 0, 0))
            copy.wait_send() if sent else copy.wait_recv()

        flat = (nx if dy else nx - 1) * part_rows[dy][1] * unit
        rim = nx * part_rims[dy][1] * unit
        if dy == 0:
            flat += 2 * plane_bytes["x"]
            rim += plane_bytes["z"] if sent else 0
        elif sent:
            flat += plane_bytes["y"]
        if nz == 2:
            guarded(dy, 0, lambda: one(0, flat + rim))
        else:

            def act():
                one(0, flat)
                for dz in z_steps:
                    guarded(0, dz, lambda dz=dz: one(dz, rim))

            guarded(dy, 0, act)

    def bin_cell(cell, carry):
        total = [None, None]
        for i in range(BIN):
            x = cell * BIN + i
            slabs = (ref_ref[x].astype(jnp.float32), def_ref[x].astype(jnp.float32))
            yrows[0, pl.ds(x, 1), :] = slabs[0][:1]
            yrows[1, pl.ds(x, 1), :] = slabs[0][sizey - 1 :]
            total = [s if t is None else t + s for t, s in zip(total, slabs)]
        for image in range(2):
            for y in range(2):
                binned[2 * image + y, pl.ds(cell, 1), :] = jnp.sum(
                    total[image][8 * y : 8 * y + 8], axis=0, keepdims=True
                )
        return carry

    def bin_chunk(c):
        both = image_ref.at[:, pl.ds(c * span, span)]
        pltpu.make_async_copy(both, both, image_sem.at[c]).wait()
        each = cells_x // chunks
        lax.fori_loop(c * each, (c + 1) * each, bin_cell, 0, unroll=2)

    for c in range(chunks):
        bin_chunk(c)

    load_table.wait()
    for q, spots in enumerate(((0, 1), (2, 3), (4, 6), (5, 7))):
        for i, part in enumerate(pieces(binned[q], 3)):
            for spot in spots:
                at = (lax.rem(turn + spot, groups) + spot // groups * groups) * cells_x
                stack[pl.ds(pl.multiple_of(at, cells_x), cells_x), pl.ds(i * sizez, sizez)] = part
    sums = across_lanes(sections["bin"][...], stack[...])
    load_disp.wait()
    lane = lax.broadcasted_iota(jnp.int32, (cells_z, 128), 1)
    held = lax.rem(lane // cells_x + groups - turn, groups)
    empty = jnp.zeros((cells_z, cells_x), jnp.float32)

    def turned_tile(row):
        return pltpu.roll(jnp.concatenate(row, axis=1), turn * cells_x, 1)

    upper = turned_tile([disp_ref[0, 1], disp_ref[1, 1], disp_ref[2, 1], empty])
    lower = turned_tile([disp_ref[1, 0], disp_ref[2, 0], empty, disp_ref[0, 0]])
    upper = jnp.where(held == 3, sums[:, 128:], upper)
    lower = jnp.where(held == 2, sums[:, 128:], lower)
    middle = jnp.where(held[:quarter] % 2 == 0, sums[:quarter, :128], sums[quarter:, :128])
    mail[1, me[0], pl.ds(0, cells_z)] = upper
    mail[1, me[0], pl.ds(cells_z, quarter)] = middle
    mail[1, me[0], pl.ds(cells_z + quarter, cells_z)] = lower
    for side, rows_out in (
        (0, (upper[cells_z - 1 :], middle[quarter - 2 : quarter - 1], middle[quarter - 1 :], lower[cells_z - 1 :])),
        (1, (upper[:1], middle[:1], middle[1:2], lower[:1])),
    ):
        for i, row_out in enumerate(rows_out):
            own_rim[side, i] = row_out
    pl.semaphore_wait(barrier, expect)
    for dy in (-1, 1, 0):

        def act(dy=dy):
            for j in range(nx):
                if j or dy:
                    mail_copy(j, dy).start()
                for dz in z_steps:
                    guarded(0, dz, lambda j=j, dz=dz: rim_copy(j, dy, dz).start())

        guarded(dy, 0, act)

    def x_copy(step):
        side = 0 if step > 0 else 1
        return remote(
            ref_ref.at[pl.ds(sizex - 1 if step > 0 else 0, 1)], xhalo.at[pl.ds(side, 1)],
            mail_send.at[1, 0], mail_recv.at[1, 0], device(1 if step > 0 else nx - 1, 0, 0),
        )

    def y_copy(step):
        side = 1 if step > 0 else 0
        return remote(
            ysend.at[side], yhalo.at[1 - side], mail_send.at[1 + step, 0], y_recv.at[1 - side], device(0, step, 0)
        )

    def z_copy(dz):
        i = 0 if dz > 0 else 1
        return remote(ref_ref, zhalo.at[i], mail_send.at[1, lane_of(dz)], z_recv.at[i], device(0, 0, dz))

    ysend[...] = yrows[...].astype(half)
    for step in (-1, 1):
        guarded(step, 0, lambda step=step: y_copy(step).start())
        x_copy(step).start()
    for dz in z_steps:
        guarded(0, dz, lambda dz=dz: z_copy(dz).start())

    def prepare(cell, carry):
        start = pl.multiple_of(cell * BIN, BIN)
        first = jnp.maximum(start - 1, 0)
        last = jnp.minimum(start + BIN, sizex - 1)
        slabs = [ref_ref[first].astype(jnp.float32)]
        slabs += [ref_ref[start + i].astype(jnp.float32) for i in range(BIN)]
        slabs += [ref_ref[last].astype(jnp.float32)]
        for i in range(BIN):
            base[start + i] = def_ref[start + i].astype(jnp.float32) - slabs[i + 1]
            grad_x[start + i] = slabs[i + 2] - slabs[i]
        return carry

    lax.fori_loop(0, cells_x, prepare, 0)

    slab_row = lax.broadcasted_iota(jnp.int32, (sizey, sizez), 0)

    def slope_y(cell, carry):
        start = pl.multiple_of(cell * BIN, BIN)
        for i in range(BIN):
            slab = ref_ref[start + i].astype(jnp.float32)
            above = jnp.where(slab_row == sizey - 1, 0.0, pltpu.roll(slab, sizey - 1, 0))
            below = jnp.where(slab_row == 0, 0.0, pltpu.roll(slab, 1, 0))
            grad_y[pl.ds(pl.multiple_of((start + i) * PITCH, 8), sizey)] = above - below
        return carry

    lax.fori_loop(0, cells_x, slope_y, 0, unroll=2)

    for dz in z_steps:
        guarded(0, dz, lambda dz=dz: z_copy(-dz if nz > 2 else dz).wait_recv())

    row = lax.broadcasted_iota(jnp.int32, (sizez, sizez), 0)
    column = lax.broadcasted_iota(jnp.int32, (sizez, sizez), 1)
    inner = jnp.where(row == column + 1, 1.0, 0.0) - jnp.where(row + 1 == column, 1.0, 0.0)
    from_low = jnp.where(
        jnp.logical_and(jnp.logical_and(row == sizez - 1, column == 0), me[2] > 0), -1.0, 0.0
    )
    from_high = jnp.where(
        jnp.logical_and(jnp.logical_and(row == 0, column == sizez - 1), me[2] < nz - 1), 1.0, 0.0
    )
    outer = [from_low + from_high] if nz == 2 else [from_low, from_high]
    across = jnp.concatenate([inner] + outer, axis=0).astype(half)

    def slope_z(cell, carry):
        start = pl.multiple_of(cell * BIN, BIN)
        sideways = [ref_ref[pl.ds(start, BIN)].reshape(BIN * sizey, sizez)]
        sideways += [zhalo[i, pl.ds(start, BIN)].reshape(BIN * sizey, sizez) for i in range(len(z_steps))]
        slope = jnp.dot(jnp.concatenate(sideways, axis=1), across, preferred_element_type=jnp.float32)
        grad_z[pl.ds(start, BIN)] = slope.reshape(BIN, sizey, sizez)
        return carry

    lax.fori_loop(0, cells_x, slope_z, 0, unroll=8)

    def gather(tiles, q):
        height = tiles[0].shape[0]
        group = lax.broadcasted_iota(jnp.int32, (height, 128), 1) // cells_x
        out = []
        for t in range(nx // groups):
            value = tiles[t * groups + (-q) % groups]
            for g in range(1, groups):
                value = jnp.where(group == g, tiles[t * groups + (g - q) % groups], value)
            out.append(pltpu.roll(value, (groups - q) * cells_x, 1) if q else value)
        return out[0] if len(out) == 1 else jnp.concatenate(out, axis=1)

    blank = jnp.zeros((SLOT - deep, across_x), jnp.float32)

    def split_store(target, k, y, value, count):
        padded = jnp.concatenate([value, blank], axis=0)
        for i, part in enumerate(pieces(padded, count)):
            target[pl.ds((4 * k + y) * SLOT, SLOT), pl.ds(i * across_x, across_x)] = part

    bottom = deep - cells_z
    foot_row = lax.broadcasted_iota(jnp.int32, (bottom, across_x), 0)

    def unpack(slot):
        for i in range(nx):
            if slot < 2:
                foot[slot, i, 0, pl.ds(0, 1)] = rims[1, slot, i, 0]
                foot[slot, i, 0, pl.ds(bottom - 1, 1)] = rims[0, slot, i, 0]
            for r in range(2):
                foot[slot, i, 1, pl.ds(r, 1)] = rims[1, slot, i, 1 + r]
                foot[slot, i, 1, pl.ds(bottom - 2 + r, 1)] = rims[0, slot, i, 1 + r]
            if slot > 0:
                foot[slot, i, 2, pl.ds(0, 1)] = rims[1, slot, i, 3]
                foot[slot, i, 2, pl.ds(bottom - 1, 1)] = rims[0, slot, i, 3]
        halves = [mail[slot, i, pl.ds(cells_z, quarter)] for i in range(nx)]
        feet = [foot[slot, i, 1] for i in range(nx)]
        for y in range(2):
            cline[2 * slot + y] = jnp.concatenate(
                [
                    gather(halves, 2 * y), gather(halves, 2 * y + 1),
                    jnp.where(foot_row < bottom // 2, gather(feet, 2 * y), gather(feet, 2 * y + 1)),
                ],
                axis=0,
            )
        for y, first, which, order in ((1, 0, 0, (0, 1, 2, 3)), (0, 3 * quarter, 2, (3, 0, 1, 2))):
            line = {(0, 1): 0, (1, 0): 1, (1, 1): 2, (2, 0): 3}.get((slot, y))
            if line is None:
                continue
            tiles = [
                jnp.concatenate([mail[slot, i, pl.ds(first, cells_z)], foot[slot, i, which]], axis=0)
                for i in range(nx)
            ]
            for k in range(3):
                value = gather(tiles, order[k])
                dline[k, line] = value
                kept[k, pl.ds(SLOT * line, deep)] = value
            fline[line] = gather(tiles, order[3])

    settle(0, False)
    grad_x[0] = ref_ref[1].astype(jnp.float32) - jnp.where(me[0] > 0, xhalo[0].astype(jnp.float32), 0.0)
    grad_x[sizex - 1] = (
        jnp.where(me[0] < nx - 1, xhalo[1].astype(jnp.float32), 0.0) - ref_ref[sizex - 2].astype(jnp.float32)
    )
    unpack(1)
    settle(-1, False)
    settle(1, False)
    unpack(0)
    unpack(2)
    lane = lax.broadcasted_iota(jnp.int32, (deep, across_x), 1)
    for y in range(4):
        c = cline[y + 1]
        slopes = [
            (
                jnp.where(lane == across_x - 1, 0.0, pltpu.roll(c, across_x - 1, 1))
                - jnp.where(lane == 0, 0.0, pltpu.roll(c, 1, 1))
            ) * 0.5,
            (cline[y + 2] - cline[y]) * 0.5,
            (pltpu.roll(c, deep - 1, 0) - pltpu.roll(c, 1, 0)) * 0.5,
        ]
        mismatch = fline[y] - c - (
            slopes[0] * dline[0, y] + slopes[1] * dline[1, y] + slopes[2] * dline[2, y]
        )
        for k in range(3):
            split_store(rsplit, k, y, slopes[k] * mismatch, 2)
    wide = 4 * SLOT
    out_row = lax.broadcasted_iota(jnp.int32, (rows, wide), 0)
    real = jnp.logical_and(
        jnp.logical_or(out_row != cells_x, me[0] < nx - 1), jnp.logical_or(out_row != rows - 1, me[0] > 0)
    )

    def shifted(k):
        near = pltpu.roll(kept[k], across_x - me[0] * cells_x, 1)
        head, tail = near[:, :128].T, near[:, across_x - 128 :].T
        return jnp.where(real, jnp.concatenate([head[: rows - 8], tail[120:]], axis=0), 0.0)

    for k in range(3):
        span_k = pl.ds(wide * k, wide)
        step = across_lanes(sections["solve"][...], rsplit[span_k, :])
        new = shifted(k) + (step[:rows] + step[rows:])
        new_ref[:, span_k] = new
        along = jnp.dot(
            jnp.concatenate(pieces(new, 2), axis=1), sections["prolong"][...], preferred_element_type=jnp.float32
        )
        for s in range(4):
            lines[k, s] = along[:, sizez * s : sizez * (s + 1)]

    for step in (-1, 1):
        guarded(step, 0, lambda step=step: y_copy(-step).wait_recv())
    for at, side in ((0, 0), (sizey - 1, 1)):
        edge = pl.ds(at, sizex, stride=PITCH)
        plane = yhalo[side].astype(jnp.float32)
        grad_y[edge, :] = grad_y[edge, :] + plane if side else grad_y[edge, :] - plane
    for dy in (0, -1, 1):
        settle(dy, True)


def combine(
    chunks,
    new_in, lines, base, grad_x, grad_y, grad_z,
    new_hbm, out_hbm,
    out, turned, new_sem, out_sem,
):
    sizex, sizey, sizez = base.shape
    cells_x = sizex // BIN
    span = sizex // chunks
    keep_new = pltpu.make_async_copy(turned, new_hbm, new_sem.at[0])
    cells_z = sizez // BIN
    before_row = new_in.shape[0] - 1

    third = lax.broadcasted_iota(jnp.int32, (8, sizez), 0).astype(jnp.float32)
    offset_y = (third + 0.5) / 8.0 - 0.5
    weight_low = jnp.maximum(-offset_y, 0.0)
    weight_high = jnp.maximum(offset_y, 0.0)
    weight_mid = 1.0 - jnp.abs(offset_y)

    def plane(at):
        planes = []
        for k in range(3):
            row_of = [lines[k, s, pl.ds(at, 1), :] for s in range(4)]
            planes.append(
                jnp.concatenate(
                    [
                        weight_low * row_of[c] + weight_mid * row_of[c + 1] + weight_high * row_of[c + 2]
                        for c in range(2)
                    ],
                    axis=0,
                )
            )
        return planes

    def residual(cell, carry):
        now, rise = carry
        later = plane(cell + 1)
        climb = [(b - a) * 0.125 for a, b in zip(now, later)]
        start = pl.multiple_of(cell * BIN, BIN)
        for i in range(BIN):
            if i == 0:
                field = [n - 3.5 * r for n, r in zip(now, rise)]
            elif i == BIN // 2:
                field = [n + 0.5 * c for n, c in zip(now, climb)]
            else:
                field = [f + d for f, d in zip(field, rise if i < BIN // 2 else climb)]
            total = base[start + i]
            at_y = pl.ds(pl.multiple_of((start + i) * PITCH, 8), sizey)
            total = total - grad_x[start + i] * field[0]
            total = total - grad_y[at_y] * field[1]
            total = total - grad_z[start + i] * field[2]
            out[start + i] = total.astype(jnp.bfloat16)
        return (later, climb)

    def store(c):
        slabs = pl.ds(c * span, span)
        return pltpu.make_async_copy(out.at[slabs], out_hbm.at[slabs], out_sem.at[c])

    before, now = plane(before_row), plane(0)
    state = (now, [(b - a) * 0.125 for a, b in zip(before, now)])
    for c in range(chunks):
        each = cells_x // chunks
        state = lax.fori_loop(c * each, (c + 1) * each, residual, state, unroll=4)
        store(c).start()
        if c == 0:
            for k in range(3):
                flipped = new_in[:cells_x, 4 * SLOT * k : 4 * SLOT * (k + 1)].T
                for y in range(2):
                    turned[k, y] = flipped[SLOT * (y + 1) : SLOT * (y + 1) + cells_z]
            keep_new.start()
    for c in range(chunks):
        store(c).wait()
    keep_new.wait()


def on_device(counts, ref_image, def_image, displacement):
    nx, ny, nz = counts
    sizex, sizey, sizez = ref_image.shape
    cells_x, cells_z = sizex // BIN, sizez // BIN
    rows, deep, across_x = cells_x + 16, cells_z + 8, nx * cells_x
    solve = solve_tables(nx, cells_x, rows)
    binning, prolong = lane_tables(cells_z, sizez, deep, 4)
    parts_of, at = {}, 0
    for name, part in (("prolong", prolong), ("solve", solve), ("bin", binning)):
        parts_of[name] = (at, part.shape[-2], part.shape[-1])
        at += part.shape[-2]
    table = np.zeros((nx, at, max(width for _, _, width in parts_of.values())), half)
    for name, part in (("prolong", prolong), ("solve", solve), ("bin", binning)):
        row, height, width = parts_of[name]
        table[:, row : row + height, :width] = part
    lanes = 1 if nz == 2 else 3
    sides = 1 if nz == 2 else 2
    dma = pltpu.SemaphoreType.DMA
    vmem, anywhere = pl.BlockSpec(memory_space=pltpu.VMEM), pl.BlockSpec(memory_space=pl.ANY)
    shape = jax.ShapeDtypeStruct
    image = ref_image.shape
    coarse = jnp.transpose(displacement, (0, 2, 3, 1))
    constants = (table,)
    f32 = jnp.float32
    held = pl.pallas_call(
        functools.partial(exchange, counts, 4, parts_of),
        out_shape=(
            shape((rows, 12 * SLOT), f32),
            shape((3, 4, rows, sizez), f32),
            shape(image, f32),
            shape(image, f32),
            shape((sizex * PITCH, sizez), f32),
            shape(image, f32),
        ),
        in_specs=[pl.BlockSpec(memory_space=pltpu.HBM)] * 4,
        out_specs=(vmem,) * 6,
        scratch_shapes=[
            pltpu.VMEM((sides,) + image, half),
            pltpu.VMEM((2,) + image, half),
            pltpu.VMEM(coarse.shape, f32),
            pltpu.VMEM(table.shape[1:], half),
            pltpu.VMEM((4, cells_x, sizez), f32),
            pltpu.VMEM((8 * cells_x, 3 * sizez), half),
            pltpu.VMEM((3, nx, 5 * cells_z // 2, 128), f32),
            pltpu.VMEM((2, 3, nx, 4, 1, 128), f32),
            pltpu.VMEM((2, 4, 1, 128), f32),
            pltpu.VMEM((3, nx, 3, deep - cells_z, 128), f32),
            pltpu.VMEM((3, 4, deep, across_x), f32),
            pltpu.VMEM((6, deep, across_x), f32),
            pltpu.VMEM((4, deep, across_x), f32),
            pltpu.VMEM((3, 4 * SLOT, across_x), f32),
            pltpu.VMEM((12 * SLOT, 2 * across_x), half),
            pltpu.VMEM((2, sizey, sizez), half),
            pltpu.VMEM((2, sizex, sizez), f32),
            pltpu.VMEM((2, sizex, sizez), half),
            pltpu.VMEM((2, sizex, sizez), half),
            dma((2,)), dma((4,)), dma((3, lanes)), dma((3, lanes)), dma((2,)), dma((sides,)),
        ],
        compiler_params=pltpu.CompilerParams(
            collective_id=0, has_side_effects=True, vmem_limit_bytes=24 << 20
        ),
    )(*[pltpu.with_memory_space_constraint(jnp.asarray(x), pltpu.HBM) for x in (ref_image, def_image, coarse) + constants])
    chunks = 8
    new, residual = pl.pallas_call(
        functools.partial(combine, chunks),
        out_shape=(shape(coarse.shape, f32), shape(image, half)),
        in_specs=[vmem] * 6,
        out_specs=(anywhere, anywhere),
        scratch_shapes=[pltpu.VMEM(image, half), pltpu.VMEM(coarse.shape, f32), dma((1,)), dma((chunks,))],
        compiler_params=pltpu.CompilerParams(vmem_limit_bytes=16 << 20),
    )(*held)
    return jnp.transpose(new, (0, 3, 1, 2)), residual


def solution(mesh):
    counts = tuple(mesh.shape[axis] for axis in ("gx", "gy", "gz"))
    return jax.shard_map(
        functools.partial(on_device, counts),
        mesh=mesh,
        in_specs=(P("gx", "gy", "gz"), P("gx", "gy", "gz"), P(None, "gx", "gy", "gz")),
        out_specs=(P(None, "gx", "gy", "gz"), P("gx", "gy", "gz")),
        check_vma=False,
    )
```

```python
import functools

import jax
import jax.numpy as jnp
import numpy as np
from jax import lax
from jax.experimental import pallas as pl
from jax.experimental.pallas import tpu as pltpu
from jax.sharding import PartitionSpec as P

stiffness = 64.0
BIN = 8
SLOT = 32
PITCH = 24
MESH = pl.DeviceIdType.MESH
half = jnp.bfloat16


def solve_tables(devices, cells, rows):
    lines = devices * cells
    theta = np.arccosh((1.0 + 2.0 * stiffness) / (2.0 * stiffness))
    index = np.arange(lines)
    low = np.minimum(index[:, None], index[None, :])
    high = np.maximum(index[:, None], index[None, :])
    a, b, c = (low + 1) * theta, (lines - high) * theta, (lines + 1) * theta
    inverse = (
        np.exp(a + b - c) * (1 - np.exp(-2 * a)) * (1 - np.exp(-2 * b)) / (1 - np.exp(-2 * c))
        / (2.0 * stiffness * np.sinh(theta))
    )
    pick = np.zeros((devices, rows, 2 * lines), np.float32)
    solve = np.zeros((devices, 2 * rows, 2 * lines), np.float32)
    for me in range(devices):
        first = me * cells
        for row, x in [(r, first + r) for r in range(cells + 1)] + [(rows - 1, first - 1)]:
            if x < 0 or x >= lines:
                continue
            top = inverse[x].astype(half).astype(np.float64)
            solve[me, row, :lines] = top
            solve[me, row, lines:] = top
            solve[me, rows + row, :lines] = inverse[x] - top
            pick[me, row, x::lines] = 1.0
    return solve.astype(half), pick.astype(half)


def lane_tables(cells_z, size_z, deep, slots):
    binning = np.repeat(np.eye(cells_z, dtype=np.float32), BIN, axis=1) / 32.0
    prolong = np.zeros((slots * SLOT, slots * size_z), np.float32)
    for slot in range(slots):
        for fine in range(size_z):
            cell, offset = fine // BIN, (fine % BIN + 0.5) / BIN - 0.5
            other = (cell + (1 if offset >= 0 else -1)) % deep
            prolong[slot * SLOT + cell, slot * size_z + fine] = 0.5 * (1.0 - abs(offset))
            prolong[slot * SLOT + other, slot * size_z + fine] = 0.5 * abs(offset)
    return np.tile(binning, (1, 3)).astype(half), np.tile(prolong, (2, 1)).astype(half)


def pieces(value, count):
    parts = []
    for i in range(count):
        part = value.astype(half)
        parts.append(part)
        if i < count - 1:
            value = value - part.astype(jnp.float32)
    return parts


def across_lanes(a, b):
    return lax.dot_general(a, b, (((1,), (1,)), ((), ())), preferred_element_type=jnp.float32)


def exchange(
    counts, chunks, parts_of,
    ref_hbm, def_hbm, disp_hbm, table_hbm,
    new_ref, planes, base, grad_x, grad_y, grad_z,
    zhalo, lines, image_ref, disp_ref, table_ref,
    binned, stack, mail, rims, own_rim, foot, dline, cline, fline, sline, kept, rsplit,
    xhalo, yrows, ysend, yhalo,
    load_sem, image_sem, mail_send, mail_recv, y_recv, z_recv,
):
    nx, ny, nz = counts
    ref_ref, def_ref = image_ref.at[0], image_ref.at[1]
    sizex, sizey, sizez = def_ref.shape
    cells_x, cells_z = sizex // BIN, sizez // BIN
    groups = 128 // cells_x
    across_x = nx * cells_x
    deep = dline.shape[2]
    rows = new_ref.shape[0]
    me = (lax.axis_index("gx"), lax.axis_index("gy"), lax.axis_index("gz"))
    turn = lax.rem(me[0], groups)

    def device(j, dy, dz, mirrored=False):
        gz = me[2] + dz if nz > 2 or dz == 0 else 1 - me[2]
        gx = lax.rem(2 * nx - 1 - me[0] - j, nx) if mirrored else lax.rem(me[0] + j, nx)
        return {"gx": gx, "gy": me[1] + dy, "gz": gz}

    def guarded(dy, dz, act):
        tests = []
        for at, step, count in ((me[1], dy, ny), (me[2], dz if nz > 2 else 0, nz)):
            if step:
                tests.append(at > 0 if step < 0 else at < count - 1)
        if tests:
            pl.when(functools.reduce(jnp.logical_and, tests))(act)
        else:
            act()

    z_steps = (1,) if nz == 2 else (1, -1)

    def side_out(dz):
        return me[2] if nz == 2 else (0 if dz > 0 else 1)

    def lane_of(dz):
        return 0 if nz == 2 or dz == 0 else (1 if dz > 0 else 2)

    sections = {}
    for name, (row, height, width) in parts_of.items():
        sections[name] = table_ref.at[pl.ds(row, height), pl.ds(0, width)]
    load_disp = pltpu.make_async_copy(disp_hbm, disp_ref, load_sem.at[0])
    load_table = pltpu.make_async_copy(table_hbm.at[me[0]], table_ref, load_sem.at[1])
    span = sizex // chunks
    for c in range(chunks):
        for i, hbm in enumerate((ref_hbm, def_hbm)):
            pltpu.make_async_copy(
                hbm.at[pl.ds(c * span, span)], image_ref.at[i, pl.ds(c * span, span)], image_sem.at[c]
            ).start()
    barrier = pltpu.get_barrier_semaphore()
    for dy in (-1, 1, 0):

        def greet(dy=dy):
            for j in range(nx):
                for dz in (0,) + z_steps:
                    if (j, dy, dz) != (0, 0, 0):

                        def hail(j=j, dz=dz):
                            pl.semaphore_signal(barrier, inc=1, device_id=device(j, dy, dz, dy != 0), device_id_type=MESH)

                        guarded(0, dz, hail)

        guarded(dy, 0, greet)

    load_disp.start()
    load_table.start()

    def clear(test, *parts):
        @pl.when(test)
        def _():
            for part in parts:
                part[...] = jnp.zeros(part.shape, part.dtype)

    low_y, high_y = me[1] == 0, me[1] == ny - 1
    low_z, high_z = me[2] == 0, me[2] == nz - 1
    clear(low_y, yhalo.at[0], mail.at[0], rims.at[:, 0])
    clear(high_y, yhalo.at[1], mail.at[2], rims.at[:, 2])
    clear(low_z, rims.at[0])
    clear(high_z, rims.at[1])
    if nz > 2:
        clear(low_z, zhalo.at[0])
        clear(high_z, zhalo.at[1])
    foot[...] = jnp.zeros(foot.shape, jnp.float32)

    reach = [
        1 + (at > 0).astype(jnp.int32) + (at < count - 1).astype(jnp.int32)
        for at, count in zip(me, counts)
    ]
    expect = nx * reach[1] * (2 if nz == 2 else reach[2]) - 1

    def remote(src, dst, send, recv, to):
        return pltpu.make_async_remote_copy(
            src_ref=src, dst_ref=dst, send_sem=send, recv_sem=recv, device_id=to, device_id_type=MESH
        )

    body = pl.ds(0, cells_z)
    quarter = cells_z // 2
    part_rows = {0: (0, 5 * quarter), 1: (0, 3 * quarter), -1: (2 * quarter, 3 * quarter)}
    part_rims = {0: (0, 4), 1: (0, 3), -1: (1, 3)}

    def mail_copy(j, dy):
        where = pl.ds(*part_rows[dy])
        return remote(
            mail.at[1, me[0], where], mail.at[1 - dy, me[0], where],
            mail_send.at[0], mail_recv.at[abs(dy), 0], device(j, dy, 0, dy != 0),
        )

    def rim_copy(j, dy, dz):
        side, where = side_out(dz), pl.ds(*part_rims[dy])
        return remote(
            own_rim.at[side, where], rims.at[side, 1 - dy, me[0], where],
            mail_send.at[lane_of(dz)], mail_recv.at[abs(dy), lane_of(dz)], device(j, dy, dz, dy != 0),
        )

    unit = 128 * 4
    plane_bytes = {"x": 2 * sizey * sizez, "y": 2 * sizex * sizez, "z": 2 * sizex * sizey * sizez}

    def drain(bytes_of, send, recv, sent):
        ref = grad_y.at[pl.ds(0, bytes_of // unit)]
        copy = remote(ref, ref, send, recv, device(1, 0, 0))
        copy.wait_send() if sent else copy.wait_recv()

    inner_y = jnp.logical_and(me[1] > 0, me[1] < ny - 1)

    def sides(act):
        pl.when(inner_y)(lambda: act(2))
        pl.when(jnp.logical_not(inner_y))(lambda: act(1))

    def near_bytes(rim):
        return nx * part_rims[0][1] * unit if rim else (nx - 1) * part_rows[0][1] * unit + 2 * plane_bytes["x"]

    def far_bytes(rim):
        return nx * (part_rims if rim else part_rows)[1][1] * unit

    def settle_near():
        if nz == 2:
            drain(near_bytes(False) + near_bytes(True), mail_send.at[0], mail_recv.at[0, 0], False)
        else:
            drain(near_bytes(False), mail_send.at[0], mail_recv.at[0, 0], False)
            for dz in z_steps:
                guarded(0, dz, lambda dz=dz: drain(near_bytes(True), mail_send.at[0], mail_recv.at[0, lane_of(-dz)], False))

    def settle_far():
        def act(count):
            if nz == 2:
                drain(count * (far_bytes(False) + far_bytes(True)), mail_send.at[0], mail_recv.at[1, 0], False)
            else:
                drain(count * far_bytes(False), mail_send.at[0], mail_recv.at[1, 0], False)
                for dz in z_steps:
                    guarded(
                        0, dz, lambda dz=dz: drain(count * far_bytes(True), mail_send.at[0], mail_recv.at[1, lane_of(-dz)], False)
                    )

        sides(act)

    def settle_sent():
        def act(count):
            flat = near_bytes(False) + count * (far_bytes(False) + plane_bytes["y"])
            rim = near_bytes(True) + count * far_bytes(True) + plane_bytes["z"]
            if nz == 2:
                drain(flat + rim, mail_send.at[0], mail_recv.at[0, 0], True)
            else:
                drain(flat, mail_send.at[0], mail_recv.at[0, 0], True)
                for dz in z_steps:
                    guarded(0, dz, lambda dz=dz: drain(rim, mail_send.at[lane_of(dz)], mail_recv.at[0, 0], True))

        sides(act)

    def bin_cell(cell, carry):
        total = [None, None]
        for i in range(BIN):
            x = cell * BIN + i
            slabs = (ref_ref[x].astype(jnp.float32), def_ref[x].astype(jnp.float32))
            yrows[0, pl.ds(x, 1), :] = slabs[0][:1]
            yrows[1, pl.ds(x, 1), :] = slabs[0][sizey - 1 :]
            total = [s if t is None else t + s for t, s in zip(total, slabs)]
        for image in range(2):
            for y in range(2):
                binned[2 * image + y, pl.ds(cell, 1), :] = jnp.sum(
                    total[image][8 * y : 8 * y + 8], axis=0, keepdims=True
                )
        return carry

    def bin_chunk(c):
        both = image_ref.at[:, pl.ds(c * span, span)]
        pltpu.make_async_copy(both, both, image_sem.at[c]).wait()
        each = cells_x // chunks
        lax.fori_loop(c * each, (c + 1) * each, bin_cell, 0, unroll=2)

    for c in range(chunks):
        bin_chunk(c)

    load_table.wait()
    for q, spots in enumerate(((0, 1), (2, 3), (4, 6), (5, 7))):
        for i, part in enumerate(pieces(binned[q], 3)):
            for spot in spots:
                at = (lax.rem(turn + spot, groups) + spot // groups * groups) * cells_x
                stack[pl.ds(pl.multiple_of(at, cells_x), cells_x), pl.ds(i * sizez, sizez)] = part
    sums = across_lanes(sections["bin"][...], stack[...])
    load_disp.wait()
    lane = lax.broadcasted_iota(jnp.int32, (cells_z, 128), 1)
    held = lax.rem(lane // cells_x + groups - turn, groups)
    empty = jnp.zeros((cells_z, cells_x), jnp.float32)

    def turned_tile(row):
        return pltpu.roll(jnp.concatenate(row, axis=1), turn * cells_x, 1)

    upper = turned_tile([disp_ref[0, 1], disp_ref[1, 1], disp_ref[2, 1], empty])
    lower = turned_tile([disp_ref[1, 0], disp_ref[2, 0], empty, disp_ref[0, 0]])
    upper = jnp.where(held == 3, sums[:, 128:], upper)
    lower = jnp.where(held == 2, sums[:, 128:], lower)
    middle = jnp.where(held[:quarter] % 2 == 0, sums[:quarter, :128], sums[quarter:, :128])
    mail[1, me[0], pl.ds(0, cells_z)] = upper
    mail[1, me[0], pl.ds(cells_z, quarter)] = middle
    mail[1, me[0], pl.ds(cells_z + quarter, cells_z)] = lower
    for side, rows_out in (
        (0, (upper[cells_z - 1 :], middle[quarter - 2 : quarter - 1], middle[quarter - 1 :], lower[cells_z - 1 :])),
        (1, (upper[:1], middle[:1], middle[1:2], lower[:1])),
    ):
        for i, row_out in enumerate(rows_out):
            own_rim[side, i] = row_out
    ysend[...] = yrows[...].astype(half)
    pl.semaphore_wait(barrier, expect)
    for dy in (-1, 1, 0):

        def act(dy=dy):
            for j in range(nx):
                if j or dy:
                    mail_copy(j, dy).start()
                for dz in z_steps:
                    guarded(0, dz, lambda j=j, dz=dz: rim_copy(j, dy, dz).start())

        guarded(dy, 0, act)

    def x_copy(step):
        side = 0 if step > 0 else 1
        return remote(
            ref_ref.at[pl.ds(sizex - 1 if step > 0 else 0, 1)], xhalo.at[pl.ds(side, 1)],
            mail_send.at[0], mail_recv.at[0, 0], device(1 if step > 0 else nx - 1, 0, 0),
        )

    def y_copy(step):
        side = 1 if step > 0 else 0
        return remote(
            ysend.at[side], yhalo.at[1 - side], mail_send.at[0], y_recv.at[0], device(0, step, 0)
        )

    def z_copy(dz):
        i = 0 if dz > 0 else 1
        return remote(ref_ref, zhalo.at[i], mail_send.at[lane_of(dz)], z_recv.at[i], device(0, 0, dz))

    for step in (-1, 1):
        guarded(step, 0, lambda step=step: y_copy(step).start())
        x_copy(step).start()
    for dz in z_steps:
        guarded(0, dz, lambda dz=dz: z_copy(dz).start())

    def prepare(cell, carry):
        start = pl.multiple_of(cell * BIN, BIN)
        first = jnp.maximum(start - 1, 0)
        last = jnp.minimum(start + BIN, sizex - 1)
        slabs = [ref_ref[first].astype(jnp.float32)]
        slabs += [ref_ref[start + i].astype(jnp.float32) for i in range(BIN)]
        slabs += [ref_ref[last].astype(jnp.float32)]
        for i in range(BIN):
            base[start + i] = def_ref[start + i].astype(jnp.float32) - slabs[i + 1]
            grad_x[start + i] = slabs[i + 2] - slabs[i]
        return carry

    lax.fori_loop(0, cells_x, prepare, 0)

    slab_row = lax.broadcasted_iota(jnp.int32, (sizey, sizez), 0)

    def slope_y(cell, carry):
        start = pl.multiple_of(cell * BIN, BIN)
        for i in range(BIN):
            slab = ref_ref[start + i].astype(jnp.float32)
            above = jnp.where(slab_row == sizey - 1, 0.0, pltpu.roll(slab, sizey - 1, 0))
            below = jnp.where(slab_row == 0, 0.0, pltpu.roll(slab, 1, 0))
            grad_y[pl.ds(pl.multiple_of((start + i) * PITCH, 8), sizey)] = above - below
        return carry

    lax.fori_loop(0, cells_x, slope_y, 0, unroll=2)

    for dz in z_steps:
        guarded(0, dz, lambda dz=dz: z_copy(-dz if nz > 2 else dz).wait_recv())

    row = lax.broadcasted_iota(jnp.int32, (sizez, sizez), 0)
    column = lax.broadcasted_iota(jnp.int32, (sizez, sizez), 1)
    inner = jnp.where(row == column + 1, 1.0, 0.0) - jnp.where(row + 1 == column, 1.0, 0.0)
    from_low = jnp.where(
        jnp.logical_and(jnp.logical_and(row == sizez - 1, column == 0), me[2] > 0), -1.0, 0.0
    )
    from_high = jnp.where(
        jnp.logical_and(jnp.logical_and(row == 0, column == sizez - 1), me[2] < nz - 1), 1.0, 0.0
    )
    outer = [from_low + from_high] if nz == 2 else [from_low, from_high]
    across = jnp.concatenate([inner] + outer, axis=0).astype(half)

    def slope_z(cell, carry):
        start = pl.multiple_of(cell * BIN, BIN)
        sideways = [ref_ref[pl.ds(start, BIN)].reshape(BIN * sizey, sizez)]
        sideways += [zhalo[i, pl.ds(start, BIN)].reshape(BIN * sizey, sizez) for i in range(len(z_steps))]
        slope = jnp.dot(jnp.concatenate(sideways, axis=1), across, preferred_element_type=jnp.float32)
        grad_z[pl.ds(start, BIN)] = slope.reshape(BIN, sizey, sizez)
        return carry

    lax.fori_loop(0, cells_x, slope_z, 0, unroll=8)

    def gather(tiles, q, shift=0):
        height = tiles[0].shape[0]
        group = lax.broadcasted_iota(jnp.int32, (height, 128), 1) // cells_x
        out = []
        for t in range(nx // groups):
            value = tiles[t * groups + (-q) % groups]
            for g in range(1, groups):
                value = jnp.where(group == g, tiles[t * groups + (g - q) % groups], value)
            turn_by = (-q * cells_x - (shift if nx == groups else 0)) % 128
            out.append(pltpu.roll(value, turn_by, 1) if turn_by else value)
        if len(out) == 1:
            return out[0]
        whole = jnp.concatenate(out, axis=1)
        return pltpu.roll(whole, -shift % across_x, 1) if shift else whole

    blank = jnp.zeros((SLOT - deep, across_x), jnp.float32)

    def split_store(target, k, y, value, count):
        padded = jnp.concatenate([value, blank], axis=0)
        for i, part in enumerate(pieces(padded, count)):
            target[pl.ds((4 * k + y) * SLOT, SLOT), pl.ds(i * across_x, across_x)] = part

    bottom = deep - cells_z
    lane = lax.broadcasted_iota(jnp.int32, (deep, across_x), 1)
    foot_row = lax.broadcasted_iota(jnp.int32, (bottom, across_x), 0)

    def unpack(slot):
        for i in range(nx):
            if slot < 2:
                foot[slot, i, 0, pl.ds(0, 1)] = rims[1, slot, i, 0]
                foot[slot, i, 0, pl.ds(bottom - 1, 1)] = rims[0, slot, i, 0]
            for r in range(2):
                foot[slot, i, 1, pl.ds(r, 1)] = rims[1, slot, i, 1 + r]
                foot[slot, i, 1, pl.ds(bottom - 2 + r, 1)] = rims[0, slot, i, 1 + r]
            if slot > 0:
                foot[slot, i, 2, pl.ds(0, 1)] = rims[1, slot, i, 3]
                foot[slot, i, 2, pl.ds(bottom - 1, 1)] = rims[0, slot, i, 3]
        halves = [mail[slot, i, pl.ds(cells_z, quarter)] for i in range(nx)]
        feet = [foot[slot, i, 1] for i in range(nx)]
        def sums_of(y, shift):
            return jnp.concatenate(
                [
                    gather(halves, 2 * y, shift), gather(halves, 2 * y + 1, shift),
                    jnp.where(foot_row < bottom // 2, gather(feet, 2 * y, shift), gather(feet, 2 * y + 1, shift)),
                ],
                axis=0,
            )

        for y, first, which, order in ((0, 3 * quarter, 2, (3, 0, 1, 2)), (1, 0, 0, (0, 1, 2, 3))):
            c = sums_of(y, 0)
            cline[2 * slot + y] = c
            line = {(0, 1): 0, (1, 0): 1, (1, 1): 2, (2, 0): 3}.get((slot, y))
            if line is None:
                continue
            tiles = [
                jnp.concatenate([mail[slot, i, pl.ds(first, cells_z)], foot[slot, i, which]], axis=0)
                for i in range(nx)
            ]
            moved = [gather(tiles, order[k]) for k in range(3)]
            for k in range(3):
                split_store(kept, k, line, moved[k], 2)
            slope_0 = (
                jnp.where(lane == across_x - 1, 0.0, sums_of(y, 1)) - jnp.where(lane == 0, 0.0, sums_of(y, -1))
            ) * 0.5
            slope_2 = (pltpu.roll(c, deep - 1, 0) - pltpu.roll(c, 1, 0)) * 0.5
            sline[line, 0] = slope_0
            sline[line, 1] = slope_2
            dline[0, line] = moved[1]
            fline[line] = gather(tiles, order[3]) - c - (slope_0 * moved[0] + slope_2 * moved[2])

    settle_near()
    grad_x[0] = ref_ref[1].astype(jnp.float32) - jnp.where(me[0] > 0, xhalo[0].astype(jnp.float32), 0.0)
    grad_x[sizex - 1] = (
        jnp.where(me[0] < nx - 1, xhalo[1].astype(jnp.float32), 0.0) - ref_ref[sizex - 2].astype(jnp.float32)
    )
    unpack(1)
    settle_far()
    unpack(0)
    unpack(2)
    picked = [
        across_lanes(sections["pick"][...], kept[pl.ds(4 * SLOT * k, 4 * SLOT), :]) for k in range(3)
    ]
    for y in range(4):
        slope_1 = (cline[y + 2] - cline[y]) * 0.5
        mismatch = fline[y] - slope_1 * dline[0, y]
        for k, slope in enumerate((sline[y, 0], slope_1, sline[y, 1])):
            split_store(rsplit, k, y, slope * mismatch, 2)
    wide = 4 * SLOT
    for k in range(3):
        span_k = pl.ds(wide * k, wide)
        step = across_lanes(sections["solve"][...], rsplit[span_k, :])
        new = picked[k] + (step[:rows] + step[rows:])
        new_ref[:, span_k] = new
        along = jnp.dot(
            jnp.concatenate(pieces(new, 2), axis=1), sections["prolong"][...], preferred_element_type=jnp.float32
        )
        for s in range(4):
            lines[k, s] = along[:, sizez * s : sizez * (s + 1)]

    third = lax.broadcasted_iota(jnp.int32, (8, sizez), 0).astype(jnp.float32)
    offset_y = (third + 0.5) / 8.0 - 0.5
    weight_low = jnp.maximum(-offset_y, 0.0)
    weight_high = jnp.maximum(offset_y, 0.0)
    weight_mid = 1.0 - jnp.abs(offset_y)

    def plane(at):
        planes = []
        for k in range(3):
            row_of = [lines[k, s, pl.ds(at, 1), :] for s in range(4)]
            planes.append(
                jnp.concatenate(
                    [
                        weight_low * row_of[c] + weight_mid * row_of[c + 1] + weight_high * row_of[c + 2]
                        for c in range(2)
                    ],
                    axis=0,
                )
            )
        return planes

    def interpolate(cell, carry):
        for k, value in enumerate(plane(cell)):
            planes[cell + 1, k] = value
        return carry

    for k, value in enumerate(plane(rows - 1)):
        planes[0, k] = value
    lax.fori_loop(0, cells_x + 1, interpolate, 0, unroll=3)

    sides(lambda count: drain(count * plane_bytes["y"], mail_send.at[0], y_recv.at[0], False))
    for at, side in ((0, 0), (sizey - 1, 1)):
        edge = pl.ds(at, sizex, stride=PITCH)
        plane = yhalo[side].astype(jnp.float32)
        grad_y[edge, :] = grad_y[edge, :] + plane if side else grad_y[edge, :] - plane
    settle_sent()


def combine(
    chunks,
    new_in, planes, base, grad_x, grad_y, grad_z,
    new_hbm, out_hbm,
    out, turned, new_sem, out_sem,
):
    sizex, sizey, sizez = base.shape
    cells_x = sizex // BIN
    span = sizex // chunks
    keep_new = pltpu.make_async_copy(turned, new_hbm, new_sem.at[0])
    cells_z = sizez // BIN

    def residual(cell, carry):
        now, rise = carry
        later = [planes[cell + 2, k] for k in range(3)]
        climb = [(b - a) * 0.125 for a, b in zip(now, later)]
        start = pl.multiple_of(cell * BIN, BIN)
        for i in range(BIN):
            if i == 0:
                field = [n - 3.5 * r for n, r in zip(now, rise)]
            elif i == BIN // 2:
                field = [n + 0.5 * c for n, c in zip(now, climb)]
            else:
                field = [f + d for f, d in zip(field, rise if i < BIN // 2 else climb)]
            total = base[start + i]
            at_y = pl.ds(pl.multiple_of((start + i) * PITCH, 8), sizey)
            total = total - grad_x[start + i] * field[0]
            total = total - grad_y[at_y] * field[1]
            total = total - grad_z[start + i] * field[2]
            out[start + i] = total.astype(jnp.bfloat16)
        return (later, climb)

    def store(c):
        slabs = pl.ds(c * span, span)
        return pltpu.make_async_copy(out.at[slabs], out_hbm.at[slabs], out_sem.at[0])

    before, now = ([planes[i, k] for k in range(3)] for i in range(2))
    state = (now, [(b - a) * 0.125 for a, b in zip(before, now)])
    for c in range(chunks):
        each = cells_x // chunks
        state = lax.fori_loop(c * each, (c + 1) * each, residual, state, unroll=4)
        store(c).start()
        if c == 0:
            for k in range(3):
                flipped = new_in[:cells_x, 4 * SLOT * k : 4 * SLOT * (k + 1)].T
                for y in range(2):
                    turned[k, y] = flipped[SLOT * (y + 1) : SLOT * (y + 1) + cells_z]
            keep_new.start()
    pltpu.make_async_copy(out, out_hbm, out_sem.at[0]).wait()
    keep_new.wait()


def on_device(counts, ref_image, def_image, displacement):
    nx, ny, nz = counts
    sizex, sizey, sizez = ref_image.shape
    cells_x, cells_z = sizex // BIN, sizez // BIN
    rows, deep, across_x = cells_x + 16, cells_z + 8, nx * cells_x
    solve, pick = solve_tables(nx, cells_x, rows)
    binning, prolong = lane_tables(cells_z, sizez, deep, 4)
    parts_of, at = {}, 0
    for name, part in (("prolong", prolong), ("solve", solve), ("pick", pick), ("bin", binning)):
        parts_of[name] = (at, part.shape[-2], part.shape[-1])
        at += part.shape[-2]
    table = np.zeros((nx, at, max(width for _, _, width in parts_of.values())), half)
    for name, part in (("prolong", prolong), ("solve", solve), ("pick", pick), ("bin", binning)):
        row, height, width = parts_of[name]
        table[:, row : row + height, :width] = part
    lanes = 1 if nz == 2 else 3
    sides = 1 if nz == 2 else 2
    dma = pltpu.SemaphoreType.DMA
    vmem, anywhere = pl.BlockSpec(memory_space=pltpu.VMEM), pl.BlockSpec(memory_space=pl.ANY)
    shape = jax.ShapeDtypeStruct
    image = ref_image.shape
    coarse = jnp.transpose(displacement, (0, 2, 3, 1))
    constants = (table,)
    f32 = jnp.float32
    held = pl.pallas_call(
        functools.partial(exchange, counts, 4, parts_of),
        out_shape=(
            shape((rows, 12 * SLOT), f32),
            shape((cells_x + 2, 3, sizey, sizez), f32),
            shape(image, f32),
            shape(image, f32),
            shape((sizex * PITCH, sizez), f32),
            shape(image, f32),
        ),
        in_specs=[pl.BlockSpec(memory_space=pltpu.HBM)] * 4,
        out_specs=(vmem,) * 6,
        scratch_shapes=[
            pltpu.VMEM((sides,) + image, half),
            pltpu.VMEM((3, 4, rows, sizez), f32),
            pltpu.VMEM((2,) + image, half),
            pltpu.VMEM(coarse.shape, f32),
            pltpu.VMEM(table.shape[1:], half),
            pltpu.VMEM((4, cells_x, sizez), f32),
            pltpu.VMEM((8 * cells_x, 3 * sizez), half),
            pltpu.VMEM((3, nx, 5 * cells_z // 2, 128), f32),
            pltpu.VMEM((2, 3, nx, 4, 1, 128), f32),
            pltpu.VMEM((2, 4, 1, 128), f32),
            pltpu.VMEM((3, nx, 3, deep - cells_z, 128), f32),
            pltpu.VMEM((1, 4, deep, across_x), f32),
            pltpu.VMEM((6, deep, across_x), f32),
            pltpu.VMEM((4, deep, across_x), f32),
            pltpu.VMEM((4, 2, deep, across_x), f32),
            pltpu.VMEM((12 * SLOT, 2 * across_x), half),
            pltpu.VMEM((12 * SLOT, 2 * across_x), half),
            pltpu.VMEM((2, sizey, sizez), half),
            pltpu.VMEM((2, sizex, sizez), f32),
            pltpu.VMEM((2, sizex, sizez), half),
            pltpu.VMEM((2, sizex, sizez), half),
            dma((2,)), dma((4,)), dma((lanes,)), dma((2, lanes)), dma((1,)), dma((sides,)),
        ],
        compiler_params=pltpu.CompilerParams(
            collective_id=0, has_side_effects=True, vmem_limit_bytes=24 << 20
        ),
    )(*[pltpu.with_memory_space_constraint(jnp.asarray(x), pltpu.HBM) for x in (ref_image, def_image, coarse) + constants])
    chunks = 8
    new, residual = pl.pallas_call(
        functools.partial(combine, chunks),
        out_shape=(shape(coarse.shape, f32), shape(image, half)),
        in_specs=[vmem] * 6,
        out_specs=(anywhere, anywhere),
        scratch_shapes=[pltpu.VMEM(image, half), pltpu.VMEM(coarse.shape, f32), dma((1,)), dma((1,))],
        compiler_params=pltpu.CompilerParams(vmem_limit_bytes=16 << 20),
    )(*held)
    return jnp.transpose(new, (0, 3, 1, 2)), residual


def solution(mesh):
    counts = tuple(mesh.shape[axis] for axis in ("gx", "gy", "gz"))
    return jax.shard_map(
        functools.partial(on_device, counts),
        mesh=mesh,
        in_specs=(P("gx", "gy", "gz"), P("gx", "gy", "gz"), P(None, "gx", "gy", "gz")),
        out_specs=(P(None, "gx", "gy", "gz"), P("gx", "gy", "gz")),
        check_vma=False,
    )
```

```python
import functools

import jax
import jax.numpy as jnp
import numpy as np
from jax import lax
from jax.experimental import pallas as pl
from jax.experimental.pallas import tpu as pltpu
from jax.sharding import PartitionSpec as P

stiffness = 64.0
BIN = 8
SLOT = 32
PITCH = 24
MESH = pl.DeviceIdType.MESH
half = jnp.bfloat16


def solve_tables(devices, cells, rows):
    lines = devices * cells
    theta = np.arccosh((1.0 + 2.0 * stiffness) / (2.0 * stiffness))
    index = np.arange(lines)
    low = np.minimum(index[:, None], index[None, :])
    high = np.maximum(index[:, None], index[None, :])
    a, b, c = (low + 1) * theta, (lines - high) * theta, (lines + 1) * theta
    inverse = (
        np.exp(a + b - c) * (1 - np.exp(-2 * a)) * (1 - np.exp(-2 * b)) / (1 - np.exp(-2 * c))
        / (2.0 * stiffness * np.sinh(theta))
    )
    pick = np.zeros((devices, rows, 2 * lines), np.float32)
    solve = np.zeros((devices, 2 * rows, 2 * lines), np.float32)
    for me in range(devices):
        first = me * cells
        for row, x in [(r, first + r) for r in range(cells + 1)] + [(rows - 1, first - 1)]:
            if x < 0 or x >= lines:
                continue
            top = inverse[x].astype(half).astype(np.float64)
            solve[me, row, :lines] = top
            solve[me, row, lines:] = top
            solve[me, rows + row, :lines] = inverse[x] - top
            pick[me, row, x::lines] = 1.0
    return solve.astype(half), pick.astype(half)


def lane_tables(cells_z, size_z, deep, slots):
    binning = np.repeat(np.eye(cells_z, dtype=np.float32), BIN, axis=1) / 32.0
    prolong = np.zeros((slots * SLOT, slots * size_z), np.float32)
    for slot in range(slots):
        for fine in range(size_z):
            cell, offset = fine // BIN, (fine % BIN + 0.5) / BIN - 0.5
            other = (cell + (1 if offset >= 0 else -1)) % deep
            prolong[slot * SLOT + cell, slot * size_z + fine] = 0.5 * (1.0 - abs(offset))
            prolong[slot * SLOT + other, slot * size_z + fine] = 0.5 * abs(offset)
    return np.tile(binning, (1, 3)).astype(half), np.tile(prolong, (2, 1)).astype(half)


def pieces(value, count):
    parts = []
    for i in range(count):
        part = value.astype(half)
        parts.append(part)
        if i < count - 1:
            value = value - part.astype(jnp.float32)
    return parts


def across_lanes(a, b):
    return lax.dot_general(a, b, (((1,), (1,)), ((), ())), preferred_element_type=jnp.float32)


def exchange(
    counts, chunks, parts_of,
    ref_hbm, def_hbm, disp_hbm, table_hbm,
    new_ref, planes, base, grad_x, grad_y, grad_z,
    zhalo, lines, image_ref, disp_ref, table_ref,
    binned, stack, mail, rims, own_rim, foot, dline, cline, fline, sline, kept, rsplit,
    xhalo, yrows, ysend, yhalo,
    load_sem, image_sem, mail_send, mail_recv, y_recv, z_recv,
):
    nx, ny, nz = counts
    ref_ref, def_ref = image_ref.at[0], image_ref.at[1]
    sizex, sizey, sizez = def_ref.shape
    cells_x, cells_z = sizex // BIN, sizez // BIN
    groups = 128 // cells_x
    across_x = nx * cells_x
    deep = dline.shape[2]
    rows = new_ref.shape[0]
    me = (lax.axis_index("gx"), lax.axis_index("gy"), lax.axis_index("gz"))
    turn = lax.rem(me[0], groups)

    def device(j, dy, dz, mirrored=False):
        gz = me[2] + dz if nz > 2 or dz == 0 else 1 - me[2]
        gx = lax.rem(2 * nx - 1 - me[0] - j, nx) if mirrored else lax.rem(me[0] + j, nx)
        return {"gx": gx, "gy": me[1] + dy, "gz": gz}

    def guarded(dy, dz, act):
        tests = []
        for at, step, count in ((me[1], dy, ny), (me[2], dz if nz > 2 else 0, nz)):
            if step:
                tests.append(at > 0 if step < 0 else at < count - 1)
        if tests:
            pl.when(functools.reduce(jnp.logical_and, tests))(act)
        else:
            act()

    z_steps = (1,) if nz == 2 else (1, -1)

    def side_out(dz):
        return me[2] if nz == 2 else (0 if dz > 0 else 1)

    def lane_of(dz):
        return 0 if nz == 2 or dz == 0 else (1 if dz > 0 else 2)

    sections = {}
    for name, (row, height, width) in parts_of.items():
        sections[name] = table_ref.at[pl.ds(row, height), pl.ds(0, width)]
    load_disp = pltpu.make_async_copy(disp_hbm, disp_ref, load_sem.at[0])
    load_table = pltpu.make_async_copy(table_hbm.at[me[0]], table_ref, load_sem.at[1])
    span = sizex // chunks
    for c in range(chunks):
        for i, hbm in enumerate((ref_hbm, def_hbm)):
            pltpu.make_async_copy(
                hbm.at[pl.ds(c * span, span)], image_ref.at[i, pl.ds(c * span, span)], image_sem.at[c]
            ).start()
    barrier = pltpu.get_barrier_semaphore()
    for dy in (-1, 1, 0):

        def greet(dy=dy):
            for j in range(nx):
                for dz in (0,) + z_steps:
                    if (j, dy, dz) != (0, 0, 0):

                        def hail(j=j, dz=dz):
                            pl.semaphore_signal(barrier, inc=1, device_id=device(j, dy, dz, dy != 0), device_id_type=MESH)

                        guarded(0, dz, hail)

        guarded(dy, 0, greet)

    load_disp.start()
    load_table.start()

    def clear(test, *parts):
        @pl.when(test)
        def _():
            for part in parts:
                part[...] = jnp.zeros(part.shape, part.dtype)

    low_y, high_y = me[1] == 0, me[1] == ny - 1
    low_z, high_z = me[2] == 0, me[2] == nz - 1
    clear(low_y, yhalo.at[0], mail.at[0], rims.at[:, 0])
    clear(high_y, yhalo.at[1], mail.at[2], rims.at[:, 2])
    clear(low_z, rims.at[0])
    clear(high_z, rims.at[1])
    if nz > 2:
        clear(low_z, zhalo.at[0])
        clear(high_z, zhalo.at[1])
    foot[...] = jnp.zeros(foot.shape, jnp.float32)

    reach = [
        1 + (at > 0).astype(jnp.int32) + (at < count - 1).astype(jnp.int32)
        for at, count in zip(me, counts)
    ]
    expect = nx * reach[1] * (2 if nz == 2 else reach[2]) - 1

    def remote(src, dst, send, recv, to):
        return pltpu.make_async_remote_copy(
            src_ref=src, dst_ref=dst, send_sem=send, recv_sem=recv, device_id=to, device_id_type=MESH
        )

    body = pl.ds(0, cells_z)
    quarter = cells_z // 2
    part_rows = {0: (0, 5 * quarter), 1: (0, 3 * quarter), -1: (2 * quarter, 3 * quarter)}
    part_rims = {0: (0, 4), 1: (0, 3), -1: (1, 3)}

    def mail_copy(j, dy):
        where = pl.ds(*part_rows[dy])
        return remote(
            mail.at[1, me[0], where], mail.at[1 - dy, me[0], where],
            mail_send.at[0], mail_recv.at[abs(dy), 0], device(j, dy, 0, dy != 0),
        )

    def rim_copy(j, dy, dz):
        side, where = side_out(dz), pl.ds(*part_rims[dy])
        return remote(
            own_rim.at[side, where], rims.at[side, 1 - dy, me[0], where],
            mail_send.at[lane_of(dz)], mail_recv.at[abs(dy), lane_of(dz)], device(j, dy, dz, dy != 0),
        )

    unit = 128 * 4
    plane_bytes = {"x": 2 * sizey * sizez, "y": 2 * sizex * sizez, "z": 2 * sizex * sizey * sizez}

    def drain(bytes_of, send, recv, sent):
        ref = grad_y.at[pl.ds(0, bytes_of // unit)]
        copy = remote(ref, ref, send, recv, device(1, 0, 0))
        copy.wait_send() if sent else copy.wait_recv()

    inner_y = jnp.logical_and(me[1] > 0, me[1] < ny - 1)

    def sides(act):
        pl.when(inner_y)(lambda: act(2))
        pl.when(jnp.logical_not(inner_y))(lambda: act(1))

    def near_bytes(rim):
        return nx * part_rims[0][1] * unit if rim else (nx - 1) * part_rows[0][1] * unit + 2 * plane_bytes["x"]

    def far_bytes(rim):
        return nx * (part_rims if rim else part_rows)[1][1] * unit

    def settle_near():
        if nz == 2:
            drain(near_bytes(False) + near_bytes(True), mail_send.at[0], mail_recv.at[0, 0], False)
        else:
            drain(near_bytes(False), mail_send.at[0], mail_recv.at[0, 0], False)
            for dz in z_steps:
                guarded(0, dz, lambda dz=dz: drain(near_bytes(True), mail_send.at[0], mail_recv.at[0, lane_of(-dz)], False))

    def settle_far():
        def act(count):
            if nz == 2:
                drain(count * (far_bytes(False) + far_bytes(True)), mail_send.at[0], mail_recv.at[1, 0], False)
            else:
                drain(count * far_bytes(False), mail_send.at[0], mail_recv.at[1, 0], False)
                for dz in z_steps:
                    guarded(
                        0, dz, lambda dz=dz: drain(count * far_bytes(True), mail_send.at[0], mail_recv.at[1, lane_of(-dz)], False)
                    )

        sides(act)

    def settle_sent():
        def act(count):
            flat = near_bytes(False) + count * (far_bytes(False) + plane_bytes["y"])
            rim = near_bytes(True) + count * far_bytes(True) + plane_bytes["z"]
            if nz == 2:
                drain(flat + rim, mail_send.at[0], mail_recv.at[0, 0], True)
            else:
                drain(flat, mail_send.at[0], mail_recv.at[0, 0], True)
                for dz in z_steps:
                    guarded(0, dz, lambda dz=dz: drain(rim, mail_send.at[lane_of(dz)], mail_recv.at[0, 0], True))

        sides(act)

    def bin_cell(cell, carry):
        total = [None, None]
        for i in range(BIN):
            x = cell * BIN + i
            slabs = (ref_ref[x].astype(jnp.float32), def_ref[x].astype(jnp.float32))
            yrows[0, pl.ds(x, 1), :] = slabs[0][:1]
            yrows[1, pl.ds(x, 1), :] = slabs[0][sizey - 1 :]
            total = [s if t is None else t + s for t, s in zip(total, slabs)]
        for image in range(2):
            for y in range(2):
                binned[2 * image + y, pl.ds(cell, 1), :] = jnp.sum(
                    total[image][8 * y : 8 * y + 8], axis=0, keepdims=True
                )
        return carry

    def bin_chunk(c):
        both = image_ref.at[:, pl.ds(c * span, span)]
        pltpu.make_async_copy(both, both, image_sem.at[c]).wait()
        each = cells_x // chunks
        lax.fori_loop(c * each, (c + 1) * each, bin_cell, 0, unroll=2)

    for c in range(chunks):
        bin_chunk(c)

    load_table.wait()
    for q, spots in enumerate(((0, 1), (2, 3), (4, 6), (5, 7))):
        for i, part in enumerate(pieces(binned[q], 3)):
            for spot in spots:
                at = (lax.rem(turn + spot, groups) + spot // groups * groups) * cells_x
                stack[pl.ds(pl.multiple_of(at, cells_x), cells_x), pl.ds(i * sizez, sizez)] = part
    sums = across_lanes(sections["bin"][...], stack[...])
    load_disp.wait()
    lane = lax.broadcasted_iota(jnp.int32, (cells_z, 128), 1)
    held = lax.rem(lane // cells_x + groups - turn, groups)
    empty = jnp.zeros((cells_z, cells_x), jnp.float32)

    def turned_tile(row):
        return pltpu.roll(jnp.concatenate(row, axis=1), turn * cells_x, 1)

    upper = turned_tile([disp_ref[0, 1], disp_ref[1, 1], disp_ref[2, 1], empty])
    lower = turned_tile([disp_ref[1, 0], disp_ref[2, 0], empty, disp_ref[0, 0]])
    upper = jnp.where(held == 3, sums[:, 128:], upper)
    lower = jnp.where(held == 2, sums[:, 128:], lower)
    middle = jnp.where(held[:quarter] % 2 == 0, sums[:quarter, :128], sums[quarter:, :128])
    mail[1, me[0], pl.ds(0, cells_z)] = upper
    mail[1, me[0], pl.ds(cells_z, quarter)] = middle
    mail[1, me[0], pl.ds(cells_z + quarter, cells_z)] = lower
    for side, rows_out in (
        (0, (upper[cells_z - 1 :], middle[quarter - 2 : quarter - 1], middle[quarter - 1 :], lower[cells_z - 1 :])),
        (1, (upper[:1], middle[:1], middle[1:2], lower[:1])),
    ):
        for i, row_out in enumerate(rows_out):
            own_rim[side, i] = row_out
    ysend[...] = yrows[...].astype(half)
    pl.semaphore_wait(barrier, expect)
    for dy in (-1, 1, 0):

        def act(dy=dy):
            for j in range(nx):
                if j or dy:
                    mail_copy(j, dy).start()
                for dz in z_steps:
                    guarded(0, dz, lambda j=j, dz=dz: rim_copy(j, dy, dz).start())

        guarded(dy, 0, act)

    def x_copy(step):
        side = 0 if step > 0 else 1
        return remote(
            ref_ref.at[pl.ds(sizex - 1 if step > 0 else 0, 1)], xhalo.at[pl.ds(side, 1)],
            mail_send.at[0], mail_recv.at[0, 0], device(1 if step > 0 else nx - 1, 0, 0),
        )

    def y_copy(step):
        side = 1 if step > 0 else 0
        return remote(
            ysend.at[side], yhalo.at[1 - side], mail_send.at[0], y_recv.at[0], device(0, step, 0)
        )

    def z_copy(dz):
        i = 0 if dz > 0 else 1
        return remote(ref_ref, zhalo.at[i], mail_send.at[lane_of(dz)], z_recv.at[i], device(0, 0, dz))

    for step in (-1, 1):
        guarded(step, 0, lambda step=step: y_copy(step).start())
        x_copy(step).start()
    for dz in z_steps:
        guarded(0, dz, lambda dz=dz: z_copy(dz).start())

    def prepare(cell, carry):
        start = pl.multiple_of(cell * BIN, BIN)
        first = jnp.maximum(start - 1, 0)
        last = jnp.minimum(start + BIN, sizex - 1)
        slabs = [ref_ref[first].astype(jnp.float32)]
        slabs += [ref_ref[start + i].astype(jnp.float32) for i in range(BIN)]
        slabs += [ref_ref[last].astype(jnp.float32)]
        for i in range(BIN):
            base[start + i] = def_ref[start + i].astype(jnp.float32) - slabs[i + 1]
            grad_x[start + i] = slabs[i + 2] - slabs[i]
        return carry

    lax.fori_loop(0, cells_x, prepare, 0)

    slab_row = lax.broadcasted_iota(jnp.int32, (sizey, sizez), 0)

    def slope_y(cell, carry):
        start = pl.multiple_of(cell * BIN, BIN)
        for i in range(BIN):
            slab = ref_ref[start + i].astype(jnp.float32)
            above = jnp.where(slab_row == sizey - 1, 0.0, pltpu.roll(slab, sizey - 1, 0))
            below = jnp.where(slab_row == 0, 0.0, pltpu.roll(slab, 1, 0))
            grad_y[pl.ds(pl.multiple_of((start + i) * PITCH, 8), sizey)] = above - below
        return carry

    lax.fori_loop(0, cells_x, slope_y, 0, unroll=2)

    for dz in z_steps:
        guarded(0, dz, lambda dz=dz: z_copy(-dz if nz > 2 else dz).wait_recv())

    row = lax.broadcasted_iota(jnp.int32, (sizez, sizez), 0)
    column = lax.broadcasted_iota(jnp.int32, (sizez, sizez), 1)
    inner = jnp.where(row == column + 1, 1.0, 0.0) - jnp.where(row + 1 == column, 1.0, 0.0)
    from_low = jnp.where(
        jnp.logical_and(jnp.logical_and(row == sizez - 1, column == 0), me[2] > 0), -1.0, 0.0
    )
    from_high = jnp.where(
        jnp.logical_and(jnp.logical_and(row == 0, column == sizez - 1), me[2] < nz - 1), 1.0, 0.0
    )
    outer = [from_low + from_high] if nz == 2 else [from_low, from_high]
    across = jnp.concatenate([inner] + outer, axis=0).astype(half)

    def slope_z(cell, carry):
        start = pl.multiple_of(cell * BIN, BIN)
        sideways = [ref_ref[pl.ds(start, BIN)].reshape(BIN * sizey, sizez)]
        sideways += [zhalo[i, pl.ds(start, BIN)].reshape(BIN * sizey, sizez) for i in range(len(z_steps))]
        slope = jnp.dot(jnp.concatenate(sideways, axis=1), across, preferred_element_type=jnp.float32)
        grad_z[pl.ds(start, BIN)] = slope.reshape(BIN, sizey, sizez)
        return carry

    lax.fori_loop(0, cells_x, slope_z, 0, unroll=8)

    def gather(tiles, q, shift=0):
        height = tiles[0].shape[0]
        group = lax.broadcasted_iota(jnp.int32, (height, 128), 1) // cells_x
        out = []
        for t in range(nx // groups):
            value = tiles[t * groups + (-q) % groups]
            for g in range(1, groups):
                value = jnp.where(group == g, tiles[t * groups + (g - q) % groups], value)
            turn_by = (-q * cells_x - (shift if nx == groups else 0)) % 128
            out.append(pltpu.roll(value, turn_by, 1) if turn_by else value)
        if len(out) == 1:
            return out[0]
        whole = jnp.concatenate(out, axis=1)
        return pltpu.roll(whole, -shift % across_x, 1) if shift else whole

    blank = jnp.zeros((SLOT - deep, across_x), jnp.float32)

    def split_store(target, k, y, value, count):
        padded = jnp.concatenate([value, blank], axis=0)
        for i, part in enumerate(pieces(padded, count)):
            target[pl.ds((4 * k + y) * SLOT, SLOT), pl.ds(i * across_x, across_x)] = part

    bottom = deep - cells_z
    lane = lax.broadcasted_iota(jnp.int32, (deep, across_x), 1)
    foot_row = lax.broadcasted_iota(jnp.int32, (bottom, across_x), 0)

    def unpack(slot):
        for i in range(nx):
            if slot < 2:
                foot[slot, i, 0, pl.ds(0, 1)] = rims[1, slot, i, 0]
                foot[slot, i, 0, pl.ds(bottom - 1, 1)] = rims[0, slot, i, 0]
            for r in range(2):
                foot[slot, i, 1, pl.ds(r, 1)] = rims[1, slot, i, 1 + r]
                foot[slot, i, 1, pl.ds(bottom - 2 + r, 1)] = rims[0, slot, i, 1 + r]
            if slot > 0:
                foot[slot, i, 2, pl.ds(0, 1)] = rims[1, slot, i, 3]
                foot[slot, i, 2, pl.ds(bottom - 1, 1)] = rims[0, slot, i, 3]
        halves = [mail[slot, i, pl.ds(cells_z, quarter)] for i in range(nx)]
        feet = [foot[slot, i, 1] for i in range(nx)]
        def sums_of(y, shift):
            return jnp.concatenate(
                [
                    gather(halves, 2 * y, shift), gather(halves, 2 * y + 1, shift),
                    jnp.where(foot_row < bottom // 2, gather(feet, 2 * y, shift), gather(feet, 2 * y + 1, shift)),
                ],
                axis=0,
            )

        for y, first, which, order in ((0, 3 * quarter, 2, (3, 0, 1, 2)), (1, 0, 0, (0, 1, 2, 3))):
            c = sums_of(y, 0)
            cline[2 * slot + y] = c
            line = {(0, 1): 0, (1, 0): 1, (1, 1): 2, (2, 0): 3}.get((slot, y))
            if line is None:
                continue
            tiles = [
                jnp.concatenate([mail[slot, i, pl.ds(first, cells_z)], foot[slot, i, which]], axis=0)
                for i in range(nx)
            ]
            moved = [gather(tiles, order[k]) for k in range(3)]
            for k in range(3):
                split_store(kept, k, line, moved[k], 2)
            slope_0 = (
                jnp.where(lane == across_x - 1, 0.0, sums_of(y, 1)) - jnp.where(lane == 0, 0.0, sums_of(y, -1))
            ) * 0.5
            slope_2 = (pltpu.roll(c, deep - 1, 0) - pltpu.roll(c, 1, 0)) * 0.5
            sline[line, 0] = slope_0
            sline[line, 1] = slope_2
            dline[0, line] = moved[1]
            fline[line] = gather(tiles, order[3]) - c - (slope_0 * moved[0] + slope_2 * moved[2])

    settle_near()
    grad_x[0] = ref_ref[1].astype(jnp.float32) - jnp.where(me[0] > 0, xhalo[0].astype(jnp.float32), 0.0)
    grad_x[sizex - 1] = (
        jnp.where(me[0] < nx - 1, xhalo[1].astype(jnp.float32), 0.0) - ref_ref[sizex - 2].astype(jnp.float32)
    )
    unpack(1)
    settle_far()
    unpack(0)
    unpack(2)
    picked = [
        across_lanes(sections["pick"][...], kept[pl.ds(4 * SLOT * k, 4 * SLOT), :]) for k in range(3)
    ]
    for y in range(4):
        slope_1 = (cline[y + 2] - cline[y]) * 0.5
        mismatch = fline[y] - slope_1 * dline[0, y]
        for k, slope in enumerate((sline[y, 0], slope_1, sline[y, 1])):
            split_store(rsplit, k, y, slope * mismatch, 2)
    wide = 4 * SLOT
    parts = []
    for k in range(3):
        span_k = pl.ds(wide * k, wide)
        step = across_lanes(sections["solve"][...], rsplit[span_k, :])
        new = picked[k] + (step[:rows] + step[rows:])
        new_ref[:, span_k] = new
        parts.append(jnp.concatenate(pieces(new, 2), axis=1))
    along = jnp.dot(jnp.concatenate(parts, axis=0), sections["prolong"][...], preferred_element_type=jnp.float32)
    for k in range(3):
        for s in range(4):
            lines[k, s] = along[rows * k : rows * (k + 1), sizez * s : sizez * (s + 1)]

    third = lax.broadcasted_iota(jnp.int32, (8, sizez), 0).astype(jnp.float32)
    offset_y = (third + 0.5) / 8.0 - 0.5
    weight_low = jnp.maximum(-offset_y, 0.0)
    weight_high = jnp.maximum(offset_y, 0.0)
    weight_mid = 1.0 - jnp.abs(offset_y)

    def plane(at):
        planes = []
        for k in range(3):
            row_of = [lines[k, s, pl.ds(at, 1), :] for s in range(4)]
            planes.append(
                jnp.concatenate(
                    [
                        weight_low * row_of[c] + weight_mid * row_of[c + 1] + weight_high * row_of[c + 2]
                        for c in range(2)
                    ],
                    axis=0,
                )
            )
        return planes

    def interpolate(cell, carry):
        for k, value in enumerate(plane(cell)):
            planes[cell + 1, k] = value
        return carry

    for k, value in enumerate(plane(rows - 1)):
        planes[0, k] = value
    lax.fori_loop(0, cells_x + 1, interpolate, 0, unroll=3)

    sides(lambda count: drain(count * plane_bytes["y"], mail_send.at[0], y_recv.at[0], False))
    for at, side in ((0, 0), (sizey - 1, 1)):
        edge = pl.ds(at, sizex, stride=PITCH)
        plane = yhalo[side].astype(jnp.float32)
        grad_y[edge, :] = grad_y[edge, :] + plane if side else grad_y[edge, :] - plane
    settle_sent()


def combine(
    chunks,
    new_in, planes, base, grad_x, grad_y, grad_z,
    new_hbm, out_hbm,
    out, turned, new_sem, out_sem,
):
    sizex, sizey, sizez = base.shape
    cells_x = sizex // BIN
    span = sizex // chunks
    keep_new = pltpu.make_async_copy(turned, new_hbm, new_sem.at[0])
    cells_z = sizez // BIN

    def residual(cell, carry):
        now, rise = carry
        later = [planes[cell + 2, k] for k in range(3)]
        climb = [(b - a) * 0.125 for a, b in zip(now, later)]
        start = pl.multiple_of(cell * BIN, BIN)
        for i in range(BIN):
            if i == 0:
                field = [n - 3.5 * r for n, r in zip(now, rise)]
            elif i == BIN // 2:
                field = [n + 0.5 * c for n, c in zip(now, climb)]
            else:
                field = [f + d for f, d in zip(field, rise if i < BIN // 2 else climb)]
            total = base[start + i]
            at_y = pl.ds(pl.multiple_of((start + i) * PITCH, 8), sizey)
            total = total - grad_x[start + i] * field[0]
            total = total - grad_y[at_y] * field[1]
            total = total - grad_z[start + i] * field[2]
            out[start + i] = total.astype(jnp.bfloat16)
        return (later, climb)

    def store(c):
        slabs = pl.ds(c * span, span)
        return pltpu.make_async_copy(out.at[slabs], out_hbm.at[slabs], out_sem.at[0])

    before, now = ([planes[i, k] for k in range(3)] for i in range(2))
    state = (now, [(b - a) * 0.125 for a, b in zip(before, now)])
    for c in range(chunks):
        each = cells_x // chunks
        state = lax.fori_loop(c * each, (c + 1) * each, residual, state, unroll=2)
        store(c).start()
        if c == 0:
            for k in range(3):
                flipped = new_in[:cells_x, 4 * SLOT * k : 4 * SLOT * (k + 1)].T
                for y in range(2):
                    turned[k, y] = flipped[SLOT * (y + 1) : SLOT * (y + 1) + cells_z]
            keep_new.start()
    pltpu.make_async_copy(out, out_hbm, out_sem.at[0]).wait()
    keep_new.wait()


def on_device(counts, ref_image, def_image, displacement):
    nx, ny, nz = counts
    sizex, sizey, sizez = ref_image.shape
    cells_x, cells_z = sizex // BIN, sizez // BIN
    rows, deep, across_x = cells_x + 16, cells_z + 8, nx * cells_x
    solve, pick = solve_tables(nx, cells_x, rows)
    binning, prolong = lane_tables(cells_z, sizez, deep, 4)
    parts_of, at = {}, 0
    for name, part in (("prolong", prolong), ("solve", solve), ("pick", pick), ("bin", binning)):
        parts_of[name] = (at, part.shape[-2], part.shape[-1])
        at += part.shape[-2]
    table = np.zeros((nx, at, max(width for _, _, width in parts_of.values())), half)
    for name, part in (("prolong", prolong), ("solve", solve), ("pick", pick), ("bin", binning)):
        row, height, width = parts_of[name]
        table[:, row : row + height, :width] = part
    lanes = 1 if nz == 2 else 3
    sides = 1 if nz == 2 else 2
    dma = pltpu.SemaphoreType.DMA
    vmem, anywhere = pl.BlockSpec(memory_space=pltpu.VMEM), pl.BlockSpec(memory_space=pl.ANY)
    shape = jax.ShapeDtypeStruct
    image = ref_image.shape
    coarse = jnp.transpose(displacement, (0, 2, 3, 1))
    constants = (table,)
    f32 = jnp.float32
    held = pl.pallas_call(
        functools.partial(exchange, counts, 4, parts_of),
        out_shape=(
            shape((rows, 12 * SLOT), f32),
            shape((cells_x + 2, 3, sizey, sizez), f32),
            shape(image, f32),
            shape(image, f32),
            shape((sizex * PITCH, sizez), f32),
            shape(image, f32),
        ),
        in_specs=[pl.BlockSpec(memory_space=pltpu.HBM)] * 4,
        out_specs=(vmem,) * 6,
        scratch_shapes=[
            pltpu.VMEM((sides,) + image, half),
            pltpu.VMEM((3, 4, rows, sizez), f32),
            pltpu.VMEM((2,) + image, half),
            pltpu.VMEM(coarse.shape, f32),
            pltpu.VMEM(table.shape[1:], half),
            pltpu.VMEM((4, cells_x, sizez), f32),
            pltpu.VMEM((8 * cells_x, 3 * sizez), half),
            pltpu.VMEM((3, nx, 5 * cells_z // 2, 128), f32),
            pltpu.VMEM((2, 3, nx, 4, 1, 128), f32),
            pltpu.VMEM((2, 4, 1, 128), f32),
            pltpu.VMEM((3, nx, 3, deep - cells_z, 128), f32),
            pltpu.VMEM((1, 4, deep, across_x), f32),
            pltpu.VMEM((6, deep, across_x), f32),
            pltpu.VMEM((4, deep, across_x), f32),
            pltpu.VMEM((4, 2, deep, across_x), f32),
            pltpu.VMEM((12 * SLOT, 2 * across_x), half),
            pltpu.VMEM((12 * SLOT, 2 * across_x), half),
            pltpu.VMEM((2, sizey, sizez), half),
            pltpu.VMEM((2, sizex, sizez), f32),
            pltpu.VMEM((2, sizex, sizez), half),
            pltpu.VMEM((2, sizex, sizez), half),
            dma((2,)), dma((4,)), dma((lanes,)), dma((2, lanes)), dma((1,)), dma((sides,)),
        ],
        compiler_params=pltpu.CompilerParams(
            collective_id=0, has_side_effects=True, vmem_limit_bytes=24 << 20
        ),
    )(*[pltpu.with_memory_space_constraint(jnp.asarray(x), pltpu.HBM) for x in (ref_image, def_image, coarse) + constants])
    chunks = 16
    new, residual = pl.pallas_call(
        functools.partial(combine, chunks),
        out_shape=(shape(coarse.shape, f32), shape(image, half)),
        in_specs=[vmem] * 6,
        out_specs=(anywhere, anywhere),
        scratch_shapes=[pltpu.VMEM(image, half), pltpu.VMEM(coarse.shape, f32), dma((1,)), dma((1,))],
        compiler_params=pltpu.CompilerParams(vmem_limit_bytes=16 << 20),
    )(*held)
    return jnp.transpose(new, (0, 3, 1, 2)), residual


def solution(mesh):
    counts = tuple(mesh.shape[axis] for axis in ("gx", "gy", "gz"))
    return jax.shard_map(
        functools.partial(on_device, counts),
        mesh=mesh,
        in_specs=(P("gx", "gy", "gz"), P("gx", "gy", "gz"), P(None, "gx", "gy", "gz")),
        out_specs=(P(None, "gx", "gy", "gz"), P("gx", "gy", "gz")),
        check_vma=False,
    )
```

```python
import functools

import jax
import jax.numpy as jnp
import numpy as np
from jax import lax
from jax.experimental import pallas as pl
from jax.experimental.pallas import tpu as pltpu
from jax.sharding import PartitionSpec as P

stiffness = 64.0
BIN = 8
SLOT = 32
PITCH = 24
MESH = pl.DeviceIdType.MESH
half = jnp.bfloat16


def solve_tables(devices, cells, rows):
    lines = devices * cells
    theta = np.arccosh((1.0 + 2.0 * stiffness) / (2.0 * stiffness))
    index = np.arange(lines)
    low = np.minimum(index[:, None], index[None, :])
    high = np.maximum(index[:, None], index[None, :])
    a, b, c = (low + 1) * theta, (lines - high) * theta, (lines + 1) * theta
    inverse = (
        np.exp(a + b - c) * (1 - np.exp(-2 * a)) * (1 - np.exp(-2 * b)) / (1 - np.exp(-2 * c))
        / (2.0 * stiffness * np.sinh(theta))
    )
    pick = np.zeros((devices, rows, 2 * lines), np.float32)
    solve = np.zeros((devices, 2 * rows, 2 * lines), np.float32)
    for me in range(devices):
        first = me * cells
        for row, x in [(r, first + r) for r in range(cells + 1)] + [(rows - 1, first - 1)]:
            if x < 0 or x >= lines:
                continue
            top = inverse[x].astype(half).astype(np.float64)
            solve[me, row, :lines] = top
            solve[me, row, lines:] = top
            solve[me, rows + row, :lines] = inverse[x] - top
            pick[me, row, x::lines] = 1.0
    return solve.astype(half), pick.astype(half)


def lane_tables(cells_z, size_z, deep, slots):
    binning = np.repeat(np.eye(cells_z, dtype=np.float32), BIN, axis=1) / 32.0
    prolong = np.zeros((slots * SLOT, slots * size_z), np.float32)
    for slot in range(slots):
        for fine in range(size_z):
            cell, offset = fine // BIN, (fine % BIN + 0.5) / BIN - 0.5
            other = (cell + (1 if offset >= 0 else -1)) % deep
            prolong[slot * SLOT + cell, slot * size_z + fine] = 0.5 * (1.0 - abs(offset))
            prolong[slot * SLOT + other, slot * size_z + fine] = 0.5 * abs(offset)
    return np.tile(binning, (1, 3)).astype(half), np.tile(prolong, (2, 1)).astype(half)


def pieces(value, count):
    parts = []
    for i in range(count):
        part = value.astype(half)
        parts.append(part)
        if i < count - 1:
            value = value - part.astype(jnp.float32)
    return parts


def across_lanes(a, b):
    return lax.dot_general(a, b, (((1,), (1,)), ((), ())), preferred_element_type=jnp.float32)


def exchange(
    counts, chunks, parts_of,
    ref_hbm, def_hbm, disp_hbm, table_hbm,
    new_ref, planes, base, grad_x, grad_y, grad_z,
    zhalo, lines, image_ref, disp_ref, table_ref,
    binned, stack, mail, rims, own_rim, foot, dline, cline, fline, sline, kept, rsplit,
    xhalo, yrows, ysend, yhalo,
    load_sem, image_sem, mail_send, mail_recv, y_recv, z_recv,
):
    nx, ny, nz = counts
    ref_ref, def_ref = image_ref.at[0], image_ref.at[1]
    sizex, sizey, sizez = def_ref.shape
    cells_x, cells_z = sizex // BIN, sizez // BIN
    groups = 128 // cells_x
    across_x = nx * cells_x
    deep = dline.shape[2]
    rows = new_ref.shape[0]
    me = (lax.axis_index("gx"), lax.axis_index("gy"), lax.axis_index("gz"))
    turn = lax.rem(me[0], groups)

    def device(j, dy, dz, mirrored=False):
        gz = me[2] + dz if nz > 2 or dz == 0 else 1 - me[2]
        gx = lax.rem(2 * nx - 1 - me[0] - j, nx) if mirrored else lax.rem(me[0] + j, nx)
        return {"gx": gx, "gy": me[1] + dy, "gz": gz}

    def guarded(dy, dz, act):
        tests = []
        for at, step, count in ((me[1], dy, ny), (me[2], dz if nz > 2 else 0, nz)):
            if step:
                tests.append(at > 0 if step < 0 else at < count - 1)
        if tests:
            pl.when(functools.reduce(jnp.logical_and, tests))(act)
        else:
            act()

    z_steps = (1,) if nz == 2 else (1, -1)

    def side_out(dz):
        return me[2] if nz == 2 else (0 if dz > 0 else 1)

    def lane_of(dz):
        return 0 if nz == 2 or dz == 0 else (1 if dz > 0 else 2)

    sections = {}
    for name, (row, height, width) in parts_of.items():
        sections[name] = table_ref.at[pl.ds(row, height), pl.ds(0, width)]
    load_disp = pltpu.make_async_copy(disp_hbm, disp_ref, load_sem.at[0])
    load_table = pltpu.make_async_copy(table_hbm.at[me[0]], table_ref, load_sem.at[1])
    span = sizex // chunks
    for c in range(chunks):
        for i, hbm in enumerate((ref_hbm, def_hbm)):
            pltpu.make_async_copy(
                hbm.at[pl.ds(c * span, span)], image_ref.at[i, pl.ds(c * span, span)], image_sem.at[c]
            ).start()
    barrier = pltpu.get_barrier_semaphore()
    for dy in (-1, 1, 0):

        def greet(dy=dy):
            for j in range(nx):
                for dz in (0,) + z_steps:
                    if (j, dy, dz) != (0, 0, 0):

                        def hail(j=j, dz=dz):
                            pl.semaphore_signal(barrier, inc=1, device_id=device(j, dy, dz, dy != 0), device_id_type=MESH)

                        guarded(0, dz, hail)

        guarded(dy, 0, greet)

    load_disp.start()
    load_table.start()

    def clear(test, *parts):
        @pl.when(test)
        def _():
            for part in parts:
                part[...] = jnp.zeros(part.shape, part.dtype)

    low_y, high_y = me[1] == 0, me[1] == ny - 1
    low_z, high_z = me[2] == 0, me[2] == nz - 1
    clear(low_y, yhalo.at[0], mail.at[0], rims.at[:, 0])
    clear(high_y, yhalo.at[1], mail.at[2], rims.at[:, 2])
    clear(low_z, rims.at[0])
    clear(high_z, rims.at[1])
    if nz > 2:
        clear(low_z, zhalo.at[0])
        clear(high_z, zhalo.at[1])
    foot[...] = jnp.zeros(foot.shape, jnp.float32)

    reach = [
        1 + (at > 0).astype(jnp.int32) + (at < count - 1).astype(jnp.int32)
        for at, count in zip(me, counts)
    ]
    expect = nx * reach[1] * (2 if nz == 2 else reach[2]) - 1

    def remote(src, dst, send, recv, to):
        return pltpu.make_async_remote_copy(
            src_ref=src, dst_ref=dst, send_sem=send, recv_sem=recv, device_id=to, device_id_type=MESH
        )

    body = pl.ds(0, cells_z)
    quarter = cells_z // 2
    part_rows = {0: (0, 5 * quarter), 1: (0, 3 * quarter), -1: (2 * quarter, 3 * quarter)}
    part_rims = {0: (0, 4), 1: (0, 3), -1: (1, 3)}

    def mail_copy(j, dy):
        where = pl.ds(*part_rows[dy])
        return remote(
            mail.at[1, me[0], where], mail.at[1 - dy, me[0], where],
            mail_send.at[0], mail_recv.at[abs(dy), 0], device(j, dy, 0, dy != 0),
        )

    def rim_copy(j, dy, dz):
        side, where = side_out(dz), pl.ds(*part_rims[dy])
        return remote(
            own_rim.at[side, where], rims.at[side, 1 - dy, me[0], where],
            mail_send.at[lane_of(dz)], mail_recv.at[abs(dy), lane_of(dz)], device(j, dy, dz, dy != 0),
        )

    unit = 128 * 4
    plane_bytes = {"x": 2 * sizey * sizez, "y": 2 * sizex * sizez, "z": 2 * sizex * sizey * sizez}

    def drain(bytes_of, send, recv, sent):
        ref = grad_y.at[pl.ds(0, bytes_of // unit)]
        copy = remote(ref, ref, send, recv, device(1, 0, 0))
        copy.wait_send() if sent else copy.wait_recv()

    inner_y = jnp.logical_and(me[1] > 0, me[1] < ny - 1)

    def sides(act):
        pl.when(inner_y)(lambda: act(2))
        pl.when(jnp.logical_not(inner_y))(lambda: act(1))

    def near_bytes(rim):
        return nx * part_rims[0][1] * unit if rim else (nx - 1) * part_rows[0][1] * unit + 2 * plane_bytes["x"]

    def far_bytes(rim):
        return nx * (part_rims if rim else part_rows)[1][1] * unit

    def settle_near():
        if nz == 2:
            drain(near_bytes(False) + near_bytes(True), mail_send.at[0], mail_recv.at[0, 0], False)
        else:
            drain(near_bytes(False), mail_send.at[0], mail_recv.at[0, 0], False)
            for dz in z_steps:
                guarded(0, dz, lambda dz=dz: drain(near_bytes(True), mail_send.at[0], mail_recv.at[0, lane_of(-dz)], False))

    def settle_far():
        def act(count):
            if nz == 2:
                drain(count * (far_bytes(False) + far_bytes(True)), mail_send.at[0], mail_recv.at[1, 0], False)
            else:
                drain(count * far_bytes(False), mail_send.at[0], mail_recv.at[1, 0], False)
                for dz in z_steps:
                    guarded(
                        0, dz, lambda dz=dz: drain(count * far_bytes(True), mail_send.at[0], mail_recv.at[1, lane_of(-dz)], False)
                    )

        sides(act)

    def settle_sent():
        def act(count):
            flat = near_bytes(False) + count * (far_bytes(False) + plane_bytes["y"])
            rim = near_bytes(True) + count * far_bytes(True) + plane_bytes["z"]
            if nz == 2:
                drain(flat + rim, mail_send.at[0], mail_recv.at[0, 0], True)
            else:
                drain(flat, mail_send.at[0], mail_recv.at[0, 0], True)
                for dz in z_steps:
                    guarded(0, dz, lambda dz=dz: drain(rim, mail_send.at[lane_of(dz)], mail_recv.at[0, 0], True))

        sides(act)

    def bin_cell(cell, carry):
        total = [None, None]
        for i in range(BIN):
            x = cell * BIN + i
            slabs = (ref_ref[x].astype(jnp.float32), def_ref[x].astype(jnp.float32))
            yrows[0, pl.ds(x, 1), :] = slabs[0][:1]
            yrows[1, pl.ds(x, 1), :] = slabs[0][sizey - 1 :]
            total = [s if t is None else t + s for t, s in zip(total, slabs)]
        for image in range(2):
            for y in range(2):
                binned[2 * image + y, pl.ds(cell, 1), :] = jnp.sum(
                    total[image][8 * y : 8 * y + 8], axis=0, keepdims=True
                )
        return carry

    def bin_chunk(c):
        both = image_ref.at[:, pl.ds(c * span, span)]
        pltpu.make_async_copy(both, both, image_sem.at[c]).wait()
        each = cells_x // chunks
        lax.fori_loop(c * each, (c + 1) * each, bin_cell, 0, unroll=2)

    for c in range(chunks):
        bin_chunk(c)

    load_table.wait()
    for q, spots in enumerate(((0, 1), (2, 3), (4, 6), (5, 7))):
        for i, part in enumerate(pieces(binned[q], 3)):
            for spot in spots:
                at = (lax.rem(turn + spot, groups) + spot // groups * groups) * cells_x
                stack[pl.ds(pl.multiple_of(at, cells_x), cells_x), pl.ds(i * sizez, sizez)] = part
    sums = across_lanes(sections["bin"][...], stack[...])
    load_disp.wait()
    lane = lax.broadcasted_iota(jnp.int32, (cells_z, 128), 1)
    held = lax.rem(lane // cells_x + groups - turn, groups)
    empty = jnp.zeros((cells_z, cells_x), jnp.float32)

    def turned_tile(row):
        return pltpu.roll(jnp.concatenate(row, axis=1), turn * cells_x, 1)

    upper = turned_tile([disp_ref[0, 1], disp_ref[1, 1], disp_ref[2, 1], empty])
    lower = turned_tile([disp_ref[1, 0], disp_ref[2, 0], empty, disp_ref[0, 0]])
    upper = jnp.where(held == 3, sums[:, 128:], upper)
    lower = jnp.where(held == 2, sums[:, 128:], lower)
    middle = jnp.where(held[:quarter] % 2 == 0, sums[:quarter, :128], sums[quarter:, :128])
    mail[1, me[0], pl.ds(0, cells_z)] = upper
    mail[1, me[0], pl.ds(cells_z, quarter)] = middle
    mail[1, me[0], pl.ds(cells_z + quarter, cells_z)] = lower
    for side, rows_out in (
        (0, (upper[cells_z - 1 :], middle[quarter - 2 : quarter - 1], middle[quarter - 1 :], lower[cells_z - 1 :])),
        (1, (upper[:1], middle[:1], middle[1:2], lower[:1])),
    ):
        for i, row_out in enumerate(rows_out):
            own_rim[side, i] = row_out
    ysend[...] = yrows[...].astype(half)
    pl.semaphore_wait(barrier, expect)
    for dy in (-1, 1, 0):

        def act(dy=dy):
            for j in range(nx):
                if j or dy:
                    mail_copy(j, dy).start()
                for dz in z_steps:
                    guarded(0, dz, lambda j=j, dz=dz: rim_copy(j, dy, dz).start())

        guarded(dy, 0, act)

    def x_copy(step):
        side = 0 if step > 0 else 1
        return remote(
            ref_ref.at[pl.ds(sizex - 1 if step > 0 else 0, 1)], xhalo.at[pl.ds(side, 1)],
            mail_send.at[0], mail_recv.at[0, 0], device(1 if step > 0 else nx - 1, 0, 0),
        )

    def y_copy(step):
        side = 1 if step > 0 else 0
        return remote(
            ysend.at[side], yhalo.at[1 - side], mail_send.at[0], y_recv.at[0], device(0, step, 0)
        )

    def z_copy(dz):
        i = 0 if dz > 0 else 1
        return remote(ref_ref, zhalo.at[i], mail_send.at[lane_of(dz)], z_recv.at[i], device(0, 0, dz))

    for step in (-1, 1):
        guarded(step, 0, lambda step=step: y_copy(step).start())
        x_copy(step).start()

    def prepare(cell, carry):
        start = pl.multiple_of(cell * BIN, BIN)
        first = jnp.maximum(start - 1, 0)
        last = jnp.minimum(start + BIN, sizex - 1)
        slabs = [ref_ref[first].astype(jnp.float32)]
        slabs += [ref_ref[start + i].astype(jnp.float32) for i in range(BIN)]
        slabs += [ref_ref[last].astype(jnp.float32)]
        for i in range(BIN):
            base[start + i] = def_ref[start + i].astype(jnp.float32) - slabs[i + 1]
            grad_x[start + i] = slabs[i + 2] - slabs[i]
        return carry

    lax.fori_loop(0, cells_x, prepare, 0)

    for dz in z_steps:
        guarded(0, dz, lambda dz=dz: z_copy(dz).start())

    slab_row = lax.broadcasted_iota(jnp.int32, (sizey, sizez), 0)

    def slope_y(cell, carry):
        start = pl.multiple_of(cell * BIN, BIN)
        for i in range(BIN):
            slab = ref_ref[start + i].astype(jnp.float32)
            above = jnp.where(slab_row == sizey - 1, 0.0, pltpu.roll(slab, sizey - 1, 0))
            below = jnp.where(slab_row == 0, 0.0, pltpu.roll(slab, 1, 0))
            grad_y[pl.ds(pl.multiple_of((start + i) * PITCH, 8), sizey)] = above - below
        return carry

    lax.fori_loop(0, cells_x, slope_y, 0, unroll=2)

    for dz in z_steps:
        guarded(0, dz, lambda dz=dz: z_copy(-dz if nz > 2 else dz).wait_recv())

    row = lax.broadcasted_iota(jnp.int32, (sizez, sizez), 0)
    column = lax.broadcasted_iota(jnp.int32, (sizez, sizez), 1)
    inner = jnp.where(row == column + 1, 1.0, 0.0) - jnp.where(row + 1 == column, 1.0, 0.0)
    from_low = jnp.where(
        jnp.logical_and(jnp.logical_and(row == sizez - 1, column == 0), me[2] > 0), -1.0, 0.0
    )
    from_high = jnp.where(
        jnp.logical_and(jnp.logical_and(row == 0, column == sizez - 1), me[2] < nz - 1), 1.0, 0.0
    )
    outer = [from_low + from_high] if nz == 2 else [from_low, from_high]
    across = jnp.concatenate([inner] + outer, axis=0).astype(half)

    def slope_z(cell, carry):
        start = pl.multiple_of(cell * BIN, BIN)
        sideways = [ref_ref[pl.ds(start, BIN)].reshape(BIN * sizey, sizez)]
        sideways += [zhalo[i, pl.ds(start, BIN)].reshape(BIN * sizey, sizez) for i in range(len(z_steps))]
        slope = jnp.dot(jnp.concatenate(sideways, axis=1), across, preferred_element_type=jnp.float32)
        grad_z[pl.ds(start, BIN)] = slope.reshape(BIN, sizey, sizez)
        return carry

    lax.fori_loop(0, cells_x, slope_z, 0, unroll=8)

    def gather(tiles, q, shift=0):
        height = tiles[0].shape[0]
        group = lax.broadcasted_iota(jnp.int32, (height, 128), 1) // cells_x
        out = []
        for t in range(nx // groups):
            value = tiles[t * groups + (-q) % groups]
            for g in range(1, groups):
                value = jnp.where(group == g, tiles[t * groups + (g - q) % groups], value)
            turn_by = (-q * cells_x - (shift if nx == groups else 0)) % 128
            out.append(pltpu.roll(value, turn_by, 1) if turn_by else value)
        if len(out) == 1:
            return out[0]
        whole = jnp.concatenate(out, axis=1)
        return pltpu.roll(whole, -shift % across_x, 1) if shift else whole

    blank = jnp.zeros((SLOT - deep, across_x), jnp.float32)

    def split_store(target, k, y, value, count):
        padded = jnp.concatenate([value, blank], axis=0)
        for i, part in enumerate(pieces(padded, count)):
            target[pl.ds((4 * k + y) * SLOT, SLOT), pl.ds(i * across_x, across_x)] = part

    bottom = deep - cells_z
    lane = lax.broadcasted_iota(jnp.int32, (deep, across_x), 1)
    foot_row = lax.broadcasted_iota(jnp.int32, (bottom, across_x), 0)

    def unpack(slot):
        for i in range(nx):
            if slot < 2:
                foot[slot, i, 0, pl.ds(0, 1)] = rims[1, slot, i, 0]
                foot[slot, i, 0, pl.ds(bottom - 1, 1)] = rims[0, slot, i, 0]
            for r in range(2):
                foot[slot, i, 1, pl.ds(r, 1)] = rims[1, slot, i, 1 + r]
                foot[slot, i, 1, pl.ds(bottom - 2 + r, 1)] = rims[0, slot, i, 1 + r]
            if slot > 0:
                foot[slot, i, 2, pl.ds(0, 1)] = rims[1, slot, i, 3]
                foot[slot, i, 2, pl.ds(bottom - 1, 1)] = rims[0, slot, i, 3]
        halves = [mail[slot, i, pl.ds(cells_z, quarter)] for i in range(nx)]
        feet = [foot[slot, i, 1] for i in range(nx)]
        def sums_of(y, shift):
            return jnp.concatenate(
                [
                    gather(halves, 2 * y, shift), gather(halves, 2 * y + 1, shift),
                    jnp.where(foot_row < bottom // 2, gather(feet, 2 * y, shift), gather(feet, 2 * y + 1, shift)),
                ],
                axis=0,
            )

        for y, first, which, order in ((0, 3 * quarter, 2, (3, 0, 1, 2)), (1, 0, 0, (0, 1, 2, 3))):
            c = sums_of(y, 0)
            cline[2 * slot + y] = c
            line = {(0, 1): 0, (1, 0): 1, (1, 1): 2, (2, 0): 3}.get((slot, y))
            if line is None:
                continue
            tiles = [
                jnp.concatenate([mail[slot, i, pl.ds(first, cells_z)], foot[slot, i, which]], axis=0)
                for i in range(nx)
            ]
            moved = [gather(tiles, order[k]) for k in range(3)]
            for k in range(3):
                split_store(kept, k, line, moved[k], 2)
            slope_0 = (
                jnp.where(lane == across_x - 1, 0.0, sums_of(y, 1)) - jnp.where(lane == 0, 0.0, sums_of(y, -1))
            ) * 0.5
            slope_2 = (pltpu.roll(c, deep - 1, 0) - pltpu.roll(c, 1, 0)) * 0.5
            sline[line, 0] = slope_0
            sline[line, 1] = slope_2
            dline[0, line] = moved[1]
            fline[line] = gather(tiles, order[3]) - c - (slope_0 * moved[0] + slope_2 * moved[2])

    settle_near()
    grad_x[0] = ref_ref[1].astype(jnp.float32) - jnp.where(me[0] > 0, xhalo[0].astype(jnp.float32), 0.0)
    grad_x[sizex - 1] = (
        jnp.where(me[0] < nx - 1, xhalo[1].astype(jnp.float32), 0.0) - ref_ref[sizex - 2].astype(jnp.float32)
    )
    unpack(1)
    settle_far()
    unpack(0)
    unpack(2)
    picked = [
        across_lanes(sections["pick"][...], kept[pl.ds(4 * SLOT * k, 4 * SLOT), :]) for k in range(3)
    ]
    for y in range(4):
        slope_1 = (cline[y + 2] - cline[y]) * 0.5
        mismatch = fline[y] - slope_1 * dline[0, y]
        for k, slope in enumerate((sline[y, 0], slope_1, sline[y, 1])):
            split_store(rsplit, k, y, slope * mismatch, 2)
    wide = 4 * SLOT
    parts = []
    for k in range(3):
        span_k = pl.ds(wide * k, wide)
        step = across_lanes(sections["solve"][...], rsplit[span_k, :])
        new = picked[k] + (step[:rows] + step[rows:])
        new_ref[:, span_k] = new
        parts.append(jnp.concatenate(pieces(new, 2), axis=1))
    along = jnp.dot(jnp.concatenate(parts, axis=0), sections["prolong"][...], preferred_element_type=jnp.float32)
    for k in range(3):
        for s in range(4):
            lines[k, s] = along[rows * k : rows * (k + 1), sizez * s : sizez * (s + 1)]

    third = lax.broadcasted_iota(jnp.int32, (8, sizez), 0).astype(jnp.float32)
    offset_y = (third + 0.5) / 8.0 - 0.5
    weight_low = jnp.maximum(-offset_y, 0.0)
    weight_high = jnp.maximum(offset_y, 0.0)
    weight_mid = 1.0 - jnp.abs(offset_y)

    def plane(at):
        planes = []
        for k in range(3):
            row_of = [lines[k, s, pl.ds(at, 1), :] for s in range(4)]
            planes.append(
                jnp.concatenate(
                    [
                        weight_low * row_of[c] + weight_mid * row_of[c + 1] + weight_high * row_of[c + 2]
                        for c in range(2)
                    ],
                    axis=0,
                )
            )
        return planes

    def interpolate(cell, carry):
        for k, value in enumerate(plane(cell)):
            planes[cell + 1, k] = value
        return carry

    for k, value in enumerate(plane(rows - 1)):
        planes[0, k] = value
    lax.fori_loop(0, cells_x + 1, interpolate, 0, unroll=3)

    sides(lambda count: drain(count * plane_bytes["y"], mail_send.at[0], y_recv.at[0], False))
    for at, side in ((0, 0), (sizey - 1, 1)):
        edge = pl.ds(at, sizex, stride=PITCH)
        plane = yhalo[side].astype(jnp.float32)
        grad_y[edge, :] = grad_y[edge, :] + plane if side else grad_y[edge, :] - plane
    settle_sent()


def combine(
    chunks,
    new_in, planes, base, grad_x, grad_y, grad_z,
    new_hbm, out_hbm,
    out, turned, new_sem, out_sem,
):
    sizex, sizey, sizez = base.shape
    cells_x = sizex // BIN
    span = sizex // chunks
    keep_new = pltpu.make_async_copy(turned, new_hbm, new_sem.at[0])
    cells_z = sizez // BIN

    def residual(cell, carry):
        now, rise = carry
        later = [planes[cell + 2, k] for k in range(3)]
        climb = [(b - a) * 0.125 for a, b in zip(now, later)]
        start = pl.multiple_of(cell * BIN, BIN)
        for i in range(BIN):
            if i == 0:
                field = [n - 3.5 * r for n, r in zip(now, rise)]
            elif i == BIN // 2:
                field = [n + 0.5 * c for n, c in zip(now, climb)]
            else:
                field = [f + d for f, d in zip(field, rise if i < BIN // 2 else climb)]
            total = base[start + i]
            at_y = pl.ds(pl.multiple_of((start + i) * PITCH, 8), sizey)
            total = total - grad_x[start + i] * field[0]
            total = total - grad_y[at_y] * field[1]
            total = total - grad_z[start + i] * field[2]
            out[start + i] = total.astype(jnp.bfloat16)
        return (later, climb)

    def store(c):
        slabs = pl.ds(c * span, span)
        return pltpu.make_async_copy(out.at[slabs], out_hbm.at[slabs], out_sem.at[0])

    before, now = ([planes[i, k] for k in range(3)] for i in range(2))
    state = (now, [(b - a) * 0.125 for a, b in zip(before, now)])
    for c in range(chunks):
        each = cells_x // chunks
        state = lax.fori_loop(c * each, (c + 1) * each, residual, state, unroll=2)
        store(c).start()
        if c == 0:
            for k in range(3):
                flipped = new_in[:cells_x, 4 * SLOT * k : 4 * SLOT * (k + 1)].T
                for y in range(2):
                    turned[k, y] = flipped[SLOT * (y + 1) : SLOT * (y + 1) + cells_z]
            keep_new.start()
    pltpu.make_async_copy(out, out_hbm, out_sem.at[0]).wait()
    keep_new.wait()


def on_device(counts, ref_image, def_image, displacement):
    nx, ny, nz = counts
    sizex, sizey, sizez = ref_image.shape
    cells_x, cells_z = sizex // BIN, sizez // BIN
    rows, deep, across_x = cells_x + 16, cells_z + 8, nx * cells_x
    solve, pick = solve_tables(nx, cells_x, rows)
    binning, prolong = lane_tables(cells_z, sizez, deep, 4)
    parts_of, at = {}, 0
    for name, part in (("prolong", prolong), ("solve", solve), ("pick", pick), ("bin", binning)):
        parts_of[name] = (at, part.shape[-2], part.shape[-1])
        at += part.shape[-2]
    table = np.zeros((nx, at, max(width for _, _, width in parts_of.values())), half)
    for name, part in (("prolong", prolong), ("solve", solve), ("pick", pick), ("bin", binning)):
        row, height, width = parts_of[name]
        table[:, row : row + height, :width] = part
    lanes = 1 if nz == 2 else 3
    sides = 1 if nz == 2 else 2
    dma = pltpu.SemaphoreType.DMA
    vmem, anywhere = pl.BlockSpec(memory_space=pltpu.VMEM), pl.BlockSpec(memory_space=pl.ANY)
    shape = jax.ShapeDtypeStruct
    image = ref_image.shape
    coarse = jnp.transpose(displacement, (0, 2, 3, 1))
    constants = (table,)
    f32 = jnp.float32
    held = pl.pallas_call(
        functools.partial(exchange, counts, 2, parts_of),
        out_shape=(
            shape((rows, 12 * SLOT), f32),
            shape((cells_x + 2, 3, sizey, sizez), f32),
            shape(image, f32),
            shape(image, f32),
            shape((sizex * PITCH, sizez), f32),
            shape(image, f32),
        ),
        in_specs=[pl.BlockSpec(memory_space=pltpu.HBM)] * 4,
        out_specs=(vmem,) * 6,
        scratch_shapes=[
            pltpu.VMEM((sides,) + image, half),
            pltpu.VMEM((3, 4, rows, sizez), f32),
            pltpu.VMEM((2,) + image, half),
            pltpu.VMEM(coarse.shape, f32),
            pltpu.VMEM(table.shape[1:], half),
            pltpu.VMEM((4, cells_x, sizez), f32),
            pltpu.VMEM((8 * cells_x, 3 * sizez), half),
            pltpu.VMEM((3, nx, 5 * cells_z // 2, 128), f32),
            pltpu.VMEM((2, 3, nx, 4, 1, 128), f32),
            pltpu.VMEM((2, 4, 1, 128), f32),
            pltpu.VMEM((3, nx, 3, deep - cells_z, 128), f32),
            pltpu.VMEM((1, 4, deep, across_x), f32),
            pltpu.VMEM((6, deep, across_x), f32),
            pltpu.VMEM((4, deep, across_x), f32),
            pltpu.VMEM((4, 2, deep, across_x), f32),
            pltpu.VMEM((12 * SLOT, 2 * across_x), half),
            pltpu.VMEM((12 * SLOT, 2 * across_x), half),
            pltpu.VMEM((2, sizey, sizez), half),
            pltpu.VMEM((2, sizex, sizez), f32),
            pltpu.VMEM((2, sizex, sizez), half),
            pltpu.VMEM((2, sizex, sizez), half),
            dma((2,)), dma((2,)), dma((lanes,)), dma((2, lanes)), dma((1,)), dma((sides,)),
        ],
        compiler_params=pltpu.CompilerParams(
            collective_id=0, has_side_effects=True, vmem_limit_bytes=24 << 20
        ),
    )(*[pltpu.with_memory_space_constraint(jnp.asarray(x), pltpu.HBM) for x in (ref_image, def_image, coarse) + constants])
    chunks = 16
    new, residual = pl.pallas_call(
        functools.partial(combine, chunks),
        out_shape=(shape(coarse.shape, f32), shape(image, half)),
        in_specs=[vmem] * 6,
        out_specs=(anywhere, anywhere),
        scratch_shapes=[pltpu.VMEM(image, half), pltpu.VMEM(coarse.shape, f32), dma((1,)), dma((1,))],
        compiler_params=pltpu.CompilerParams(vmem_limit_bytes=16 << 20),
    )(*held)
    return jnp.transpose(new, (0, 3, 1, 2)), residual


def solution(mesh):
    counts = tuple(mesh.shape[axis] for axis in ("gx", "gy", "gz"))
    return jax.shard_map(
        functools.partial(on_device, counts),
        mesh=mesh,
        in_specs=(P("gx", "gy", "gz"), P("gx", "gy", "gz"), P(None, "gx", "gy", "gz")),
        out_specs=(P(None, "gx", "gy", "gz"), P("gx", "gy", "gz")),
        check_vma=False,
    )
```
